32 devices in a mesh: dp: 4 (over y, x), fsdp: 8 (over z, core).
Axes of the slice: x: 2, y: 2, z: 4, core: 2. Of those that a mesh axis runs over, the one named last changes fastest.
Arguments:
- tokens: bfloat16 [32768, 768], P(('dp', 'fsdp')), may hold values from -11 to 11
- attention: bfloat16 [768, 3072], P(None, 'fsdp'), may hold values from -2 to 2
- attvector: bfloat16 [3840], P('fsdp'), may hold values from -2 to 2
- expand: bfloat16 [768, 3072], P(None, 'fsdp'), may hold values from -0.21875 to 0.21875
- contract: bfloat16 [3072, 768], P('fsdp'), may hold values from -0.109375 to 0.109375
- feedvector: bfloat16 [5376], P('fsdp'), may hold values from -2 to 2
- lengths: int32 [64], P(('dp', 'fsdp')), may hold values from 1 to 512, 19660 in all
- cotangent: bfloat16 [32768, 768], P(('dp', 'fsdp')), may hold values from -6 to 6
Outputs:
- layer_output: bfloat16 [32768, 768], P(('dp', 'fsdp'))
- input_grad: bfloat16 [32768, 768], P(('dp', 'fsdp'))
- attention_grad: float32 [768, 3072], P(None, 'fsdp')
- attvector_grad: float32 [3840], P('fsdp')
- expand_grad: float32 [768, 3072], P(None, 'fsdp')
- contract_grad: float32 [3072, 768], P('fsdp')
- feedvector_grad: float32 [5376], P('fsdp')
- root_squares: float32 [3], replicated
The draws below stay inside these ranges and needn't reach their ends.
Inputs may be any that keep to these rules, and one draw needn't show every extreme that they name: `lengths`: some row is full.
All inputs are finite; a program needn't handle non-finite values. No bound on the sum of `lengths` on one device may be relied on, other than what follows from the above.
Results may differ from the reference program's by a relative error of at most 0.015.
Values may be sent and summed in bfloat16 or wider, within the bound.
No kernel may reach another device: no remote copies, remote signals or barrier semaphores. Data moves between devices by JAX's collectives and lax.ppermute only.
A program may use at most 192 MiB of HBM per device.

```python
import math
import jax
import jax.numpy as jnp
import numpy as np
from jax import lax

D = 768
HEAD_DIM = 64
FF = 3072
SEQ_LEN = 512
ROWS = 64
TOKENS = 32768


def rough_normal(key, shape):
    return jnp.clip(jax.random.normal(key, shape, jnp.float32), -6.0, 6.0)


def draw_tokens(key, part):
    own_key = jax.random.fold_in(key, 101)
    place = jnp.arange(TOKENS, dtype=jnp.float32)[:, None] * (1.0 / TOKENS)
    factor = 1.0 + 0.732 * place
    return (rough_normal(own_key, (TOKENS, D)) * factor).astype(jnp.bfloat16)


def draw_attention(key, part):
    own_key = jax.random.fold_in(key, 202)
    column = jnp.arange(4 * D, dtype=jnp.int32)[None, :] // D
    factor = jnp.where(column < 3, 1.0, 3.0) * (1.0 / math.sqrt(D))
    return (rough_normal(own_key, (D, 4 * D)) * factor).astype(jnp.bfloat16)


def draw_attvector(key, part):
    first, second = jax.random.split(jax.random.fold_in(key, 303))
    segment = jnp.arange(5 * D, dtype=jnp.int32) // D
    shifts = 0.3 * rough_normal(first, (5 * D,))
    gains = jnp.exp(jax.random.uniform(second, (5 * D,), jnp.float32, -0.6931472, 0.6931472))
    return jnp.where(segment == 3, gains, shifts).astype(jnp.bfloat16)


def draw_feedvector(key, part):
    first, second = jax.random.split(jax.random.fold_in(key, 404))
    index = jnp.arange(FF + 3 * D, dtype=jnp.int32)
    shifts = 0.3 * rough_normal(first, (FF + 3 * D,))
    gains = jnp.exp(jax.random.uniform(second, (FF + 3 * D,), jnp.float32, -0.6931472, 0.6931472))
    chosen = (index >= FF + D) & (index < FF + 2 * D)
    return jnp.where(chosen, gains, shifts).astype(jnp.bfloat16)


def levels(stream_key, dims, cuts, smallest, top_value):
    loudness = 1.0
    for dim, blocks in cuts:
        steps = jax.random.uniform(jax.random.fold_in(jax.random.fold_in(stream_key, 6), dim), (blocks,), jnp.float32, smallest / len(cuts), top_value / len(cuts))
        loudness = loudness * jnp.repeat(jnp.exp(steps), dims[dim] // blocks).reshape((-1,) + (1,) * (len(dims) - 1 - dim))
    return loudness


def split_up(number_of, total, most, slope):
    portions = [(1 << 20) // math.isqrt(grade ** slope) + 1 for grade in range(2, number_of + 1)]
    surplus, counts = total - most - (number_of - 1), [1] * (number_of - 1)
    while surplus > 0:
        free = [i for i in range(number_of - 1) if counts[i] < most]
        mass, budget = sum([portions[i] for i in free]), surplus
        for i in free:
            addition = min(most - counts[i], max(1, budget * portions[i] // mass), surplus)
            counts[i] = counts[i] + addition
            surplus = surplus - addition
    return np.array([most] + counts)


def uneven_parts(stream_key, amount, total, most, lean):
    if amount == 2:
        one = jax.random.randint(stream_key, (), max(1, total - most), min(most, total - 1) + 1)
        return jnp.stack([one, total - one])
    sizes = jnp.asarray(split_up(amount, total, most, lean), jnp.int32)
    pairs = (amount - 1) // 2
    source_of, receiver = sizes[1:1 + 2 * pairs:2], sizes[2:2 + 2 * pairs:2]
    margin = jnp.minimum(source_of - 1, most - receiver)
    passed = jax.random.randint(jax.random.fold_in(stream_key, 1), (pairs,), 0, 1 << 20) % (margin + 1)
    sizes = sizes.at[1:1 + 2 * pairs:2].set(source_of - passed).at[2:2 + 2 * pairs:2].set(receiver + passed)
    return sizes[jax.random.permutation(jax.random.fold_in(stream_key, 2), amount)]


def normal_values(rng, shape, spread, most, cuts=(), held_as=jnp.bfloat16):
    loudness = levels(rng, shape, cuts, -0.22, 0.18) if cuts else 1.0
    array = jax.random.normal(rng, shape, jnp.float32) * spread * loudness
    return jnp.minimum(jnp.maximum(array, -most), most).astype(held_as)


def setup_inputs(seed: int = 0) -> dict:
    arg_keys = jax.random.split(jax.random.key(seed), 9)
    return {
        "tokens": draw_tokens(jax.random.fold_in(arg_keys[8], 71), 0),
        "attention": draw_attention(jax.random.fold_in(arg_keys[8], 71), 0),
        "attvector": draw_attvector(jax.random.fold_in(arg_keys[8], 71), 0),
        "expand": normal_values(arg_keys[3], (D, FF), D ** -0.5, 0.21875, ((1, 8),)),
        "contract": normal_values(arg_keys[4], (FF, D), FF ** -0.5, 0.109375, ((0, 8),)),
        "feedvector": draw_feedvector(jax.random.fold_in(arg_keys[8], 71), 0),
        "lengths": uneven_parts(arg_keys[6], ROWS, ROWS * SEQ_LEN * 3 // 5, SEQ_LEN, 0).astype(jnp.int32),
        "cotangent": normal_values(arg_keys[7], (TOKENS, D), 1.0, 6.0, ((0, 32),)),
    }


EPSILON = 1e-12
NEGATIVE = -1000000000.0

@jax.custom_vjp
def low(v):
    return lax.optimization_barrier(v.astype(jnp.bfloat16)).astype(jnp.float32)

@jax.custom_vjp
def low_back(v):
    return v

def low_keep(v):
    return (low(v), None)

def low_pass(kept, grad):
    return (grad,)

def back_keep(v):
    return (v, None)

def back_low(kept, grad):
    return (low(grad),)
low.defvjp(low_keep, low_pass)
low_back.defvjp(back_keep, back_low)

def product(left, right):
    return jnp.dot(left, right, precision=lax.Precision.HIGHEST)

def layer_norm(residual, scale_gain, shift_bias):
    centered = residual - lax.optimization_barrier(jnp.mean(residual, axis=-1, keepdims=True))
    inverse = lax.rsqrt(lax.optimization_barrier(jnp.mean(centered * centered, axis=-1, keepdims=True)) + EPSILON)
    return centered * inverse * scale_gain + shift_bias

def forward(tokens, attention, attvector, expand, contract, feedvector, lengths):
    model_width = tokens.shape[1]
    row_count = lengths.shape[0]
    positions = tokens.shape[0] // row_count
    head_count = model_width // HEAD_DIM
    query_bias = attvector[:model_width]
    value_bias = attvector[model_width:2 * model_width]
    output_bias = attvector[2 * model_width:3 * model_width]
    first_gain = attvector[3 * model_width:4 * model_width]
    first_shift = attvector[4 * model_width:]
    hidden_units = expand.shape[1]
    inner_bias = feedvector[:hidden_units]
    outer_bias = feedvector[hidden_units:hidden_units + model_width]
    second_gain = feedvector[hidden_units + model_width:hidden_units + 2 * model_width]
    second_shift = feedvector[hidden_units + 2 * model_width:]
    queries = low_back(low(product(tokens, attention[:, :model_width]) + query_bias))
    key_rows = low_back(low(product(tokens, attention[:, model_width:2 * model_width])))
    value_rows = low_back(low(product(tokens, attention[:, 2 * model_width:3 * model_width]) + value_bias))
    shape_four = (row_count, positions, head_count, HEAD_DIM)
    scores = jnp.einsum('rqhd,rkhd->rhqk', queries.reshape(shape_four), key_rows.reshape(shape_four), precision=lax.Precision.HIGHEST) * (1.0 / math.sqrt(HEAD_DIM))
    live_mask = jnp.arange(positions, dtype=jnp.int32)[None, :] < lengths[:, None]
    scores = low_back(jnp.where(live_mask[:, None, None, :], scores, NEGATIVE))
    softmax_low = low(jax.nn.softmax(scores, axis=-1))
    context = jnp.einsum('rhqk,rkhd->rqhd', softmax_low, value_rows.reshape(shape_four), precision=lax.Precision.HIGHEST).reshape(-1, model_width)
    context = low_back(low(context))
    branch_attn = low_back(product(context, attention[:, 3 * model_width:]) + output_bias)
    hidden = layer_norm(tokens + branch_attn, first_gain, first_shift)
    inner_act = low_back(product(low(hidden), expand) + inner_bias)
    branch_feed = low_back(product(low(jax.nn.gelu(inner_act, approximate=False)), contract) + outer_bias)
    result = layer_norm(hidden + branch_feed, second_gain, second_shift)
    return (result, (branch_attn, branch_feed))

def reference(tokens, attention, attvector, expand, contract, feedvector, lengths, cotangent):
    params = tuple((weight.astype(jnp.float32) for weight in (attention, attvector, expand, contract, feedvector)))
    model_width = tokens.shape[1]
    row_count = lengths.shape[0]
    positions = tokens.shape[0] // row_count
    group_rows = min(row_count, max(1, 4096 // positions))
    blocks = row_count // group_rows
    token_blocks = tokens.reshape(blocks, group_rows * positions, model_width)
    length_blocks = lengths.reshape(blocks, group_rows)
    cot_blocks = cotangent.reshape(blocks, group_rows * positions, model_width)

    def one_block(carried, block_item):
        gradients, squares = carried
        block_tokens, block_lengths, block_cot = block_item
        tokens_wide = block_tokens.astype(jnp.float32)

        def apply_layer(inputs, *weights):
            return forward(inputs, *weights, block_lengths)
        result, pullback, branches = jax.vjp(apply_layer, tokens_wide, *params, has_aux=True)
        pulled = pullback(block_cot.astype(jnp.float32))
        live_column = (jnp.arange(positions, dtype=jnp.int32)[None, :] < block_lengths[:, None]).reshape(-1, 1).astype(jnp.float32)
        sum_block = jnp.stack([jnp.sum(live_column * tokens_wide * tokens_wide), jnp.sum(live_column * branches[0] * branches[0]), jnp.sum(live_column * branches[1] * branches[1])])
        gradients = tuple((old + new for old, new in zip(gradients, pulled[1:])))
        return ((gradients, squares + sum_block), (result.astype(jnp.bfloat16), pulled[0].astype(jnp.bfloat16)))
    initial = (tuple((jnp.zeros_like(weight) for weight in params)), jnp.zeros((3,), jnp.float32))
    (gradients, squares), (outputs, input_grads) = lax.scan(one_block, initial, (token_blocks, length_blocks, cot_blocks))
    total_count = jnp.sum(lengths).astype(jnp.float32) * model_width
    root_squares = jnp.sqrt(squares / total_count)
    return (outputs.reshape(-1, model_width), input_grads.reshape(-1, model_width), gradients[0], gradients[1], gradients[2], gradients[3], gradients[4], root_squares)
```

```python
import math

import jax
import jax.numpy as jnp
from jax import lax
from jax.experimental import pallas as pl
from jax.experimental.pallas import tpu as pltpu
from jax.sharding import PartitionSpec as P

HEAD_DIM = 64
EPSILON = 1e-12
NEGATIVE = -1000000000.0
BF = jnp.bfloat16
F32 = jnp.float32
AXES = ("dp", "fsdp")


def norm_forward(residual, scale_gain, shift_bias):
    centered = residual - jnp.mean(residual, axis=-1, keepdims=True)
    inverse = lax.rsqrt(jnp.mean(centered * centered, axis=-1, keepdims=True) + EPSILON)
    normed = centered * inverse
    return (normed * scale_gain + shift_bias, normed, inverse)


def norm_backward(upstream, normed, inverse, scale_gain):
    gain_grad = jnp.sum(upstream * normed, axis=0)
    shift_grad = jnp.sum(upstream, axis=0)
    scaled = upstream * scale_gain
    mean_plain = jnp.mean(scaled, axis=-1, keepdims=True)
    mean_normed = jnp.mean(scaled * normed, axis=-1, keepdims=True)
    return (inverse * (scaled - mean_plain - normed * mean_normed), gain_grad, shift_grad)


def masked_scores(queries, key_rows, live_mask):
    scale_factor = 1.0 / math.sqrt(queries.shape[-1])
    scores = (
        jnp.einsum("qhd,khd->hqk", queries, key_rows, preferred_element_type=F32) * scale_factor
    )
    return jnp.where(live_mask[None, None, :], scores, NEGATIVE)


def attend(block_item):
    queries, key_rows, value_rows, live_mask = block_item
    scores = masked_scores(queries, key_rows, live_mask)
    peak_score = jnp.max(scores, axis=-1, keepdims=True)
    totals = jnp.sum(jnp.exp(scores - peak_score), axis=-1, keepdims=True)
    logsum = peak_score + jnp.log(totals)
    softmax_low = jnp.exp(scores - logsum).astype(BF)
    context = jnp.einsum("hqk,khd->qhd", softmax_low, value_rows, preferred_element_type=F32)
    return (context.astype(BF), logsum[..., 0])


def attend_back(block_item):
    queries, key_rows, value_rows, live_mask, logsum, context_grad = block_item
    scale_factor = 1.0 / math.sqrt(queries.shape[-1])
    scores = masked_scores(queries, key_rows, live_mask)
    softmax_wide = jnp.exp(scores - logsum[..., None])
    softmax_low = softmax_wide.astype(BF)
    value_grad = jnp.einsum("hqk,qhd->khd", softmax_low, context_grad, preferred_element_type=F32)
    weight_grad = jnp.einsum("qhd,khd->hqk", context_grad, value_rows, preferred_element_type=F32)
    row_total = jnp.sum(softmax_wide * weight_grad, axis=-1, keepdims=True)
    score_grad = (softmax_wide * (weight_grad - row_total)).astype(BF)
    query_grad = (
        jnp.einsum("hqk,khd->qhd", score_grad, key_rows, preferred_element_type=F32) * scale_factor
    )
    key_grad = (
        jnp.einsum("hqk,qhd->khd", score_grad, queries, preferred_element_type=F32) * scale_factor
    )
    return (query_grad.astype(BF), key_grad.astype(BF), value_grad.astype(BF))


def gelu_slope(inner_act):
    cumulative = 0.5 * (1.0 + lax.erf(inner_act * (1.0 / math.sqrt(2.0))))
    density = jnp.exp(-0.5 * inner_act * inner_act) * (1.0 / math.sqrt(2.0 * math.pi))
    return cumulative + inner_act * density


def column_sum(values):
    return jnp.sum(values, axis=0, dtype=F32)


def exchange(values, mask):
    size = lax.axis_size("dp") * lax.axis_size("fsdp")
    return lax.ppermute(values, AXES, [(i, i ^ mask) for i in range(size)])


class Places:
    def __init__(self):
        self.dp, self.fsdp = lax.axis_size("dp"), lax.axis_size("fsdp")
        self.zs = self.fsdp // 2
        self.my_dp, self.my_fsdp = lax.axis_index("dp"), lax.axis_index("fsdp")
        self.core_mask, self.dp_mask = 1, self.fsdp

    def z_mask(self, k):
        return 2 * k


def flip_axes(values, flips):
    for axis, bit in flips:
        values = jnp.where(bit == 1, jnp.flip(values, axis), values)
    return values


def bits_of(value, count):
    return [(value >> (count - 1 - i)) & 1 for i in range(count)]


def to_natural(values, places, with_dp):
    tail = values.shape[3 if with_dp else 2 :]
    zbits = places.zs.bit_length() - 1
    dbits = places.dp.bit_length() - 1 if with_dp else 0
    split = values.reshape((2,) + (2,) * dbits + (2,) * zbits + tail)
    flags = [places.my_fsdp & 1]
    flags += bits_of(places.my_dp, dbits) if with_dp else []
    flags += bits_of(places.my_fsdp >> 1, zbits)
    split = flip_axes(split, list(enumerate(flags)))
    lead = (2, places.dp, places.zs) if with_dp else (2, places.zs)
    whole = split.reshape(lead + tail)
    return jnp.moveaxis(whole, 2 if with_dp else 1, 0)


def to_exchange(values, places):
    moved = jnp.moveaxis(values, 0, 2)
    tail = moved.shape[3:]
    zbits, dbits = places.zs.bit_length() - 1, places.dp.bit_length() - 1
    split = moved.reshape((2,) + (2,) * dbits + (2,) * zbits + tail)
    flags = [places.my_fsdp & 1] + bits_of(places.my_dp, dbits) + bits_of(places.my_fsdp >> 1, zbits)
    split = flip_axes(split, list(enumerate(flags)))
    return split.reshape((2, places.dp, places.zs) + tail)


def gather_blocks(shard, places, extra=None):
    quarter = shard.shape[0] // places.dp
    mine = lax.dynamic_slice_in_dim(shard, places.my_dp * quarter, quarter, 0)
    if extra is not None:
        mine = jnp.concatenate([mine, extra], axis=0)
    over_z = [mine] + [exchange(mine, places.z_mask(k)) for k in range(1, places.zs)]
    extras = None
    if extra is not None:
        extras = jnp.concatenate([part[quarter:] for part in over_z], axis=0)
        over_z = [part[:quarter] for part in over_z]
    own = jnp.concatenate(over_z, axis=0)
    if places.dp == 4:
        half = own.shape[0] // 2
        one, two = exchange(own, places.dp_mask), exchange(own, 2 * places.dp_mask)
        three_a = exchange(one[:half], 2 * places.dp_mask)
        three_b = exchange(two[half:], places.dp_mask)
        parts = [own, one, two, three_a, three_b]
    else:
        parts = [own] + [exchange(own, m * places.dp_mask) for m in range(1, places.dp)]
    if extras is not None:
        parts.append(extras)
    ours = jnp.concatenate(parts, axis=0)
    theirs = exchange(ours, places.core_mask)
    rows = shard.shape[0] * places.zs
    whole = jnp.concatenate([ours[:rows], theirs[:rows]], axis=0)
    if extras is None:
        return whole, None
    return whole, jnp.stack([ours[rows:], theirs[rows:]])


def reduce_blocks(partial, places):
    rows, width = partial.shape
    half_rows = rows // 2
    quarter = half_rows // (places.dp * places.zs)

    def add(*parts):
        return sum(part.astype(F32) for part in parts)

    mine = add(partial[:half_rows], exchange(partial[half_rows:], places.core_mask)).astype(BF)
    block = half_rows // places.dp
    own = [mine[m * block : (m + 1) * block] for m in range(places.dp)]
    if places.dp == 4:
        half = block // 2
        three_a = exchange(own[3][:half], 2 * places.dp_mask)
        three_b = exchange(own[3][half:], places.dp_mask)
        one = jnp.concatenate([add(own[1][:half], three_a).astype(BF), own[1][half:]], axis=0)
        two = jnp.concatenate([own[2][:half], add(own[2][half:], three_b).astype(BF)], axis=0)
        got_one, got_two = exchange(one, places.dp_mask), exchange(two, 2 * places.dp_mask)
        summed = add(own[0], got_one, got_two).astype(BF)
    else:
        summed = add(own[0], *[exchange(own[m], m * places.dp_mask) for m in range(1, places.dp)]).astype(BF)
    pieces = [summed[k * quarter : (k + 1) * quarter] for k in range(places.zs)]
    final = add(pieces[0], *[exchange(pieces[k], places.z_mask(k)) for k in range(1, places.zs)]).astype(BF)
    stacked = jnp.stack([final] + [exchange(final, m * places.dp_mask) for m in range(1, places.dp)])
    dbits = places.dp.bit_length() - 1
    split = stacked.reshape((2,) * dbits + stacked.shape[1:])
    split = flip_axes(split, list(enumerate(bits_of(places.my_dp, dbits))))
    return split.reshape(places.dp * quarter, width).astype(F32)


def block_table(places):
    e = jnp.arange(2, dtype=jnp.int32)[:, None, None] ^ (places.my_fsdp & 1)
    m = jnp.arange(places.dp, dtype=jnp.int32)[None, :, None] ^ places.my_dp
    k = jnp.arange(places.zs, dtype=jnp.int32)[None, None, :] ^ (places.my_fsdp >> 1)
    return ((k * 2 + e) * places.dp + m).reshape(-1).astype(jnp.int32)


def reorder_kernel(table_ref, in_ref, out_ref, *, natural, size):
    def step(i, carry):
        here, there = pl.multiple_of(i * size, size), pl.multiple_of(table_ref[i] * size, size)
        if natural:
            out_ref[pl.ds(there, size), :] = in_ref[pl.ds(here, size), :]
        else:
            out_ref[pl.ds(here, size), :] = in_ref[pl.ds(there, size), :]
        return carry

    lax.fori_loop(0, in_ref.shape[0] // size, step, 0)


def reorder(values, places, natural):
    blocks = 2 * places.dp * places.zs
    size = values.shape[0] // blocks
    if size % 16:
        tail = values.shape[1:]
        if natural:
            return to_natural(values.reshape((2, places.dp, places.zs, size) + tail), places, True).reshape(values.shape)
        return to_exchange(values.reshape((places.zs, 2, places.dp, size) + tail), places).reshape(values.shape)
    import functools

    return pl.pallas_call(
        functools.partial(reorder_kernel, natural=natural, size=size),
        out_shape=jax.ShapeDtypeStruct(values.shape, values.dtype),
        in_specs=[pl.BlockSpec(memory_space=pltpu.SMEM), pl.BlockSpec(memory_space=pltpu.VMEM)],
        out_specs=pl.BlockSpec(memory_space=pltpu.VMEM),
        name="reorder",
    )(block_table(places), values)


def dot_nt(left, right):
    return lax.dot_general(left, right, (((1,), (1,)), ((), ())), preferred_element_type=F32)


def dot_nn(left, right):
    return jnp.dot(left, right, preferred_element_type=F32)


def dot_tn(left, right):
    return lax.dot_general(left, right, (((0,), (0,)), ((), ())), preferred_element_type=F32)


def per_device(tokens, attention, attvector, expand, contract, feedvector, lengths, cotangent):
    places = Places()
    width = tokens.shape[1]
    row_count = lengths.shape[0]
    positions = tokens.shape[0] // row_count
    head_count = width // HEAD_DIM
    fsdp = places.fsdp
    hidden = expand.shape[1] * fsdp
    att_len, feed_len = attvector.shape[0], feedvector.shape[0]

    extra_rows = 16
    vectors = jnp.concatenate([attvector, feedvector])
    extra = jnp.pad(vectors, (0, extra_rows * width - vectors.shape[0])).reshape(extra_rows, width)
    attn_blocks, extras = gather_blocks(attention.T, places, extra)
    expand_rows, _ = gather_blocks(expand.T, places)
    contract_rows, _ = gather_blocks(contract, places)
    attn_rows = reorder(attn_blocks, places, True)
    extras = extras.reshape(2, places.zs, extra_rows * width)[:, :, : vectors.shape[0]]
    vec_natural = to_natural(extras, places, False).reshape(fsdp, -1)
    attvec = vec_natural[:, :att_len].reshape(-1).astype(F32)
    feedvec = vec_natural[:, att_len:].reshape(-1).astype(F32)
    query_bias, value_bias, output_bias, first_gain, first_shift = (attvec[i * width : (i + 1) * width] for i in range(5))
    inner_natural = feedvec[:hidden]
    outer_bias, second_gain, second_shift = (feedvec[hidden + i * width : hidden + (i + 1) * width] for i in range(3))
    quarter = expand.shape[1] // places.dp
    inner_bias = to_exchange(inner_natural.reshape(places.zs, 2, places.dp, quarter), places).reshape(-1)

    tokens_wide = tokens.astype(F32)
    projected = dot_nt(tokens, attn_rows[: 3 * width])
    queries = (projected[:, :width] + query_bias).astype(BF)
    key_rows = projected[:, width : 2 * width].astype(BF)
    value_rows = (projected[:, 2 * width :] + value_bias).astype(BF)
    shape_four = (row_count, positions, head_count, HEAD_DIM)
    live_mask = jnp.arange(positions, dtype=jnp.int32)[None, :] < lengths[:, None]
    query_four = queries.reshape(shape_four)
    key_four = key_rows.reshape(shape_four)
    value_four = value_rows.reshape(shape_four)
    context, logsum = lax.map(attend, (query_four, key_four, value_four, live_mask))
    context_flat = context.reshape(-1, width)
    branch_attn = dot_nt(context_flat, attn_rows[3 * width :]) + output_bias
    hidden_state, normed_one, inverse_one = norm_forward(tokens_wide + branch_attn, first_gain, first_shift)
    hidden_low = hidden_state.astype(BF)
    inner_act = dot_nt(hidden_low, expand_rows) + inner_bias
    gelu_low = jax.nn.gelu(inner_act, approximate=False).astype(BF)
    branch_feed = dot_nn(gelu_low, contract_rows) + outer_bias
    result, normed_two, inverse_two = norm_forward(hidden_state + branch_feed, second_gain, second_shift)
    live_column = live_mask.reshape(-1, 1).astype(F32)
    scalars = jnp.stack(
        [
            jnp.sum(live_column * tokens_wide * tokens_wide),
            jnp.sum(live_column * branch_attn * branch_attn),
            jnp.sum(live_column * branch_feed * branch_feed),
            jnp.sum(lengths).astype(F32),
        ]
    )

    grad_two, second_gain_grad, second_shift_grad = norm_backward(
        cotangent.astype(F32), normed_two, inverse_two, second_gain
    )
    feed_out_grad = grad_two.astype(BF)
    outer_bias_grad = column_sum(feed_out_grad)
    contract_part = dot_tn(gelu_low, feed_out_grad).astype(BF)
    contract_sum = reduce_blocks(contract_part, places)
    inner_grad = (dot_nt(feed_out_grad, contract_rows) * gelu_slope(inner_act)).astype(BF)
    inner_bias_grad = column_sum(inner_grad)
    expand_part = dot_tn(inner_grad, hidden_low).astype(BF)
    expand_sum = reduce_blocks(expand_part, places)
    hidden_grad = grad_two + dot_nn(inner_grad, expand_rows)
    grad_one, first_gain_grad, first_shift_grad = norm_backward(hidden_grad, normed_one, inverse_one, first_gain)
    attn_out_grad = grad_one.astype(BF)
    output_bias_grad = column_sum(attn_out_grad)
    output_part = dot_tn(attn_out_grad, context_flat)
    context_grad = dot_nn(attn_out_grad, attn_rows[3 * width :]).astype(BF)
    query_grad, key_grad, value_grad = lax.map(
        attend_back,
        (query_four, key_four, value_four, live_mask, logsum, context_grad.reshape(shape_four)),
    )
    projected_grad = jnp.concatenate(
        [query_grad.reshape(-1, width), key_grad.reshape(-1, width), value_grad.reshape(-1, width)], axis=1
    )
    query_bias_grad = column_sum(projected_grad[:, :width])
    value_bias_grad = column_sum(projected_grad[:, 2 * width :])
    projection_part = dot_tn(projected_grad, tokens)
    attn_part = jnp.concatenate([projection_part.astype(BF), output_part.astype(BF)], axis=0)
    attn_sum = reduce_blocks(reorder(attn_part, places, False), places)
    input_grad = grad_one + dot_nn(projected_grad, attn_rows[: 3 * width])

    inner_bias_natural = to_natural(
        inner_bias_grad.reshape(2, places.dp, places.zs, quarter), places, True
    ).reshape(-1)
    vector_part = jnp.concatenate(
        [
            query_bias_grad, value_bias_grad, output_bias_grad, first_gain_grad, first_shift_grad,
            inner_bias_natural, outer_bias_grad, second_gain_grad, second_shift_grad, scalars,
        ]
    )
    count = vector_part.shape[0]
    small_rows = -(-count // (8 * width)) * 8
    vector_sum = jnp.pad(vector_part, (0, small_rows * width - count)).reshape(small_rows, width)
    step = 1
    while step < places.dp * fsdp:
        vector_sum = vector_sum + exchange(vector_sum, step)
        step *= 2
    vector_sum = vector_sum.reshape(-1)
    att_total, feed_total = att_len * fsdp, feed_len * fsdp
    att_sum = lax.dynamic_slice_in_dim(vector_sum[:att_total], places.my_fsdp * att_len, att_len, 0)
    feed_sum = lax.dynamic_slice_in_dim(vector_sum[att_total : att_total + feed_total], places.my_fsdp * feed_len, feed_len, 0)
    sums = vector_sum[att_total + feed_total : att_total + feed_total + 4]
    root_squares = jnp.sqrt(sums[:3] / (sums[3] * width))
    return (
        result.astype(BF),
        input_grad.astype(BF),
        attn_sum.T,
        att_sum,
        expand_sum.T,
        contract_sum,
        feed_sum,
        root_squares,
    )


def solution(mesh):
    return jax.shard_map(
        per_device,
        mesh=mesh,
        in_specs=(
            P(AXES, None),
            P(None, "fsdp"),
            P("fsdp"),
            P(None, "fsdp"),
            P("fsdp", None),
            P("fsdp"),
            P(AXES),
            P(AXES, None),
        ),
        out_specs=(
            P(AXES, None),
            P(AXES, None),
            P(None, "fsdp"),
            P("fsdp"),
            P(None, "fsdp"),
            P("fsdp", None),
            P("fsdp"),
            P(),
        ),
        check_vma=False,
    )
```

```python
import functools
import math

import jax
import jax.numpy as jnp
from jax import lax
from jax.experimental import pallas as pl
from jax.experimental.pallas import tpu as pltpu
from jax.sharding import PartitionSpec as P

HEAD_DIM = 64
EPSILON = 1e-12
NEGATIVE = -1000000000.0
BF = jnp.bfloat16
F32 = jnp.float32
AXES = ("dp", "fsdp")
LOG2E = 1.0 / math.log(2.0)
SCALE = 1.0 / math.sqrt(HEAD_DIM)
TILE = 256
PAIR = 2 * HEAD_DIM


def dot_nt(left, right, precision=None):
    return lax.dot_general(
        left, right, (((1,), (1,)), ((), ())), precision=precision, preferred_element_type=F32
    )


def dot_nn(left, right):
    return jnp.dot(left, right, preferred_element_type=F32)


def dot_tn(left, right):
    return lax.dot_general(left, right, (((0,), (0,)), ((), ())), preferred_element_type=F32)


def resident(shape, *index):
    index = index or (0,) * len(shape)
    return pl.BlockSpec(shape, lambda *_: index)


def call(kernel, name, flops, bytes_moved, **kwargs):
    cost = pl.CostEstimate(flops=flops, bytes_accessed=bytes_moved, transcendentals=0)
    return pl.pallas_call(kernel, name=name, cost_estimate=cost, **kwargs)


SMEM = pl.BlockSpec(memory_space=pltpu.SMEM)


def project_kernel(table_ref, bias_ref, token_ref, *refs, starts, size):
    pieces, (out_ref, rows_ref) = refs[:-2], refs[-2:]

    @pl.when(pl.program_id(0) == 0)
    def _():
        for piece, start in zip(pieces, starts):
            for i in range(piece.shape[0] // size):
                there = pl.multiple_of(table_ref[start + i] * size, size)
                rows_ref[pl.ds(there, size), :] = piece[i * size : (i + 1) * size, :]

    width = token_ref.shape[1]
    for j in range(3):
        part = dot_nt(token_ref[...], rows_ref[j * width : (j + 1) * width, :])
        if j == 0:
            part = part + bias_ref[0:1, :]
        if j == 2:
            part = part + bias_ref[1:2, :]
        out_ref[j] = part.astype(BF)


def project(tokens, bias, table, pieces, starts, size):
    count, width = tokens.shape
    total = sum(piece.shape[0] for piece in pieces)
    return call(
        functools.partial(project_kernel, starts=starts, size=size),
        "project",
        2 * count * width * 3 * width,
        2 * (4 * count * width + 2 * total * width),
        grid=(count // TILE,),
        in_specs=[SMEM, resident(bias.shape), pl.BlockSpec((TILE, width), lambda t: (t, 0))]
        + [resident(piece.shape) for piece in pieces],
        out_specs=[
            pl.BlockSpec((3, TILE, width), lambda t: (0, t, 0)),
            resident((total, width)),
        ],
        out_shape=[
            jax.ShapeDtypeStruct((3, count, width), BF),
            jax.ShapeDtypeStruct((total, width), BF),
        ],
    )(table, bias, tokens, *pieces)


def head_lanes(values, head):
    lane = lax.broadcasted_iota(jnp.int32, values.shape, 1)
    return jnp.where((lane >= HEAD_DIM) == (head == 1), values, jnp.zeros_like(values))


def scores_of(keys, queries, length, head):
    scores = dot_nt(keys, head_lanes(queries, head))
    place = lax.broadcasted_iota(jnp.int32, scores.shape, 0)
    return jnp.where(place < length, scores, NEGATIVE / SCALE)


def attend_kernel(length_ref, q_ref, k_ref, v_ref, out_ref, log_ref):
    length = length_ref[pl.program_id(0)]
    keys = k_ref[0]
    values_t = v_ref[0].T
    halves = []
    for head in range(2):
        scores = scores_of(keys, q_ref[0], length, head)
        peak = jnp.max(scores, axis=0, keepdims=True) * (SCALE * LOG2E)
        weights = jnp.exp2(scores * (SCALE * LOG2E) - peak)
        total = jnp.sum(weights, axis=0, keepdims=True)
        part = dot_nn(values_t[head * HEAD_DIM : (head + 1) * HEAD_DIM, :], weights.astype(BF))
        halves.append(part * (1.0 / total))
        log_ref[0, 0, head : head + 1, :] = peak + jnp.log2(total)
    out_ref[...] = jnp.concatenate(halves, axis=0).T.astype(BF)


def attend(projected, lengths, positions):
    _, count, width = projected.shape
    rows, pairs = count // positions, width // PAIR
    block = (1, positions, PAIR)
    flops = 4 * rows * pairs * 2 * positions * positions * HEAD_DIM
    return call(
        attend_kernel,
        "attend",
        2 * flops,
        8 * count * width,
        grid_spec=pltpu.PrefetchScalarGridSpec(
            num_scalar_prefetch=1,
            grid=(rows, pairs),
            in_specs=[pl.BlockSpec(block, lambda r, p, _, j=j: (j, r, p)) for j in range(3)],
            out_specs=[
                pl.BlockSpec((positions, PAIR), lambda r, p, _: (r, p)),
                pl.BlockSpec((1, 1, 2, positions), lambda r, p, _: (r, p, 0, 0)),
            ],
        ),
        out_shape=[
            jax.ShapeDtypeStruct((count, width), BF),
            jax.ShapeDtypeStruct((rows, pairs, 2, positions), F32),
        ],
    )(lengths, projected, projected, projected)


def attend_back_kernel(length_ref, q_ref, k_ref, v_ref, grad_ref, ctx_ref, log_ref, out_ref, sum_ref):
    length = length_ref[pl.program_id(0)]
    queries, keys, values, grad = q_ref[0], k_ref[0], v_ref[0], grad_ref[...]
    keys_t = keys.T
    product = grad.astype(F32) * ctx_ref[...].astype(F32)
    key_grad, value_grad, query_halves = None, None, []
    for head in range(2):
        scores = scores_of(keys, queries, length, head)
        wide = jnp.exp2(scores * (SCALE * LOG2E) - log_ref[0, 0, head : head + 1, :])
        grad_head = head_lanes(grad, head)
        value_part = dot_nn(wide.astype(BF), grad_head)
        weight_grad = dot_nt(values, grad_head)
        ones = head_lanes(jnp.ones((8, PAIR), F32), head)
        row_total = dot_nt(ones, product, lax.Precision.HIGHEST)[0:1, :]
        score_grad = (wide * (weight_grad - row_total)).astype(BF)
        key_part = dot_nn(score_grad, head_lanes(queries, head))
        query_halves.append(dot_nn(keys_t[head * HEAD_DIM : (head + 1) * HEAD_DIM, :], score_grad))
        value_grad = value_part if head == 0 else value_grad + value_part
        key_grad = key_part if head == 0 else key_grad + key_part
    query_low = (jnp.concatenate(query_halves, axis=0) * SCALE).astype(F32).T.astype(BF)
    value_low = value_grad.astype(BF)
    out_ref[0] = query_low
    out_ref[1] = (key_grad * SCALE).astype(BF)
    out_ref[2] = value_low
    sum_ref[0, 0:1, :] = jnp.sum(query_low.astype(F32), axis=0, keepdims=True)
    sum_ref[0, 1:2, :] = jnp.sum(value_low.astype(F32), axis=0, keepdims=True)


def attend_back(projected, lengths, context_grad, context, logs, positions):
    _, count, width = projected.shape
    rows, pairs = count // positions, width // PAIR
    block = (1, positions, PAIR)
    flat = pl.BlockSpec((positions, PAIR), lambda r, p, _: (r, p))
    flops = 10 * rows * pairs * 2 * positions * positions * HEAD_DIM
    return call(
        attend_back_kernel,
        "attend_back",
        2 * flops,
        16 * count * width,
        grid_spec=pltpu.PrefetchScalarGridSpec(
            num_scalar_prefetch=1,
            grid=(rows, pairs),
            in_specs=[pl.BlockSpec(block, lambda r, p, _, j=j: (j, r, p)) for j in range(3)]
            + [flat, flat, pl.BlockSpec((1, 1, 2, positions), lambda r, p, _: (r, p, 0, 0))],
            out_specs=[
                pl.BlockSpec((3, positions, PAIR), lambda r, p, _: (0, r, p)),
                pl.BlockSpec((1, 2, PAIR), lambda r, p, _: (r, 0, p)),
            ],
        ),
        out_shape=[
            jax.ShapeDtypeStruct((3, count, width), BF),
            jax.ShapeDtypeStruct((rows, 2, width), F32),
        ],
    )(lengths, projected, projected, projected, context_grad, context, logs)


def normalize(residual):
    centered = residual - jnp.mean(residual, axis=-1, keepdims=True)
    inverse = lax.rsqrt(jnp.mean(centered * centered, axis=-1, keepdims=True) + EPSILON)
    return centered * inverse, inverse


def norm_back(upstream, normed, inverse, gain):
    scaled = upstream * gain
    mean_plain = jnp.mean(scaled, axis=-1, keepdims=True)
    mean_normed = jnp.mean(scaled * normed, axis=-1, keepdims=True)
    return inverse * (scaled - mean_plain - normed * mean_normed)


def live_tile(length_ref, positions, shape):
    first = pl.program_id(0) * TILE
    place = lax.broadcasted_iota(jnp.int32, shape, 0) + first % positions
    return place < length_ref[first // positions]


def add_rows(ref, rows):
    @pl.when(pl.program_id(0) == 0)
    def _():
        ref[...] = jnp.zeros_like(ref)

    for i, row in enumerate(rows):
        ref[i : i + 1, :] += jnp.sum(row, axis=0, keepdims=True)


def middle_kernel(length_ref, vec_ref, ctx_ref, weight_ref, token_ref, n_ref, s_ref, low_ref, sum_ref, *, positions):
    branch = dot_nt(ctx_ref[...], weight_ref[...]) + vec_ref[0:1, :]
    tokens = token_ref[...].astype(F32)
    normed, inverse = normalize(tokens + branch)
    n_ref[...] = normed
    s_ref[...] = jnp.broadcast_to(inverse, s_ref.shape)
    low_ref[...] = (normed * vec_ref[1:2, :] + vec_ref[2:3, :]).astype(BF)
    live = live_tile(length_ref, positions, tokens.shape)
    add_rows(sum_ref, [jnp.where(live, tokens * tokens, 0.0), jnp.where(live, branch * branch, 0.0)])


def tiles(width):
    return pl.BlockSpec((TILE, width), lambda t: (t, 0))


def middle(lengths, vectors, context, attn_rows, tokens, positions):
    count, width = tokens.shape
    return call(
        functools.partial(middle_kernel, positions=positions),
        "middle",
        2 * count * width * width,
        count * width * 12,
        grid=(count // TILE,),
        in_specs=[SMEM, resident(vectors.shape), tiles(width), resident((width, width), 3, 0), tiles(width)],
        out_specs=[tiles(width), tiles(128), tiles(width), resident((8, width))],
        out_shape=[
            jax.ShapeDtypeStruct((count, width), F32),
            jax.ShapeDtypeStruct((count, 128), F32),
            jax.ShapeDtypeStruct((count, width), BF),
            jax.ShapeDtypeStruct((8, width), F32),
        ],
    )(lengths, vectors, context, attn_rows, tokens)


def gelu_parts(inner):
    cumulative = 0.5 * (1.0 + lax.erf(inner * (1.0 / math.sqrt(2.0))))
    density = jnp.exp2(inner * inner * (-0.5 * LOG2E)) * (1.0 / math.sqrt(2.0 * math.pi))
    return inner * cumulative, cumulative + inner * density


def expand_kernel(bias_ref, low_ref, *refs):
    pieces, (gelu_ref, slope_ref) = refs[:-2], refs[-2:]
    low, at = low_ref[...], 0
    for piece in pieces:
        size = piece.shape[0]
        inner = dot_nt(low, piece[...]) + bias_ref[0:1, at : at + size]
        gelu, slope = gelu_parts(inner)
        gelu_ref[:, at : at + size] = gelu.astype(BF)
        slope_ref[:, at : at + size] = slope.astype(BF)
        at += size


def picked(piece, width):
    array, start, size = piece
    return pl.BlockSpec((size, width), lambda *_, at=start // size: (at, 0))


def expand_call(low, bias, pieces):
    count, width = low.shape
    hidden = bias.shape[1]
    return call(
        expand_kernel,
        "expand_gelu",
        2 * count * width * hidden,
        count * hidden * 4,
        grid=(count // TILE,),
        in_specs=[resident(bias.shape), tiles(width)] + [picked(piece, width) for piece in pieces],
        out_specs=[tiles(hidden), tiles(hidden)],
        out_shape=[jax.ShapeDtypeStruct((count, hidden), BF)] * 2,
    )(bias, low, *[piece[0] for piece in pieces])


def contract_kernel(length_ref, vec_ref, gelu_ref, n_ref, cot_ref, *refs, positions):
    pieces, (out_ref, grad_ref, low_ref, sum_ref) = refs[:-4], refs[-4:]
    branch, at = vec_ref[3:4, :], 0
    for piece in pieces:
        size = piece.shape[0]
        branch = branch + dot_nn(gelu_ref[:, at : at + size], piece[...])
        at += size
    first = n_ref[...] * vec_ref[1:2, :] + vec_ref[2:3, :]
    normed, inverse = normalize(first + branch)
    out_ref[...] = (normed * vec_ref[4:5, :] + vec_ref[5:6, :]).astype(BF)
    upstream = cot_ref[...].astype(F32)
    grad = norm_back(upstream, normed, inverse, vec_ref[4:5, :])
    low = grad.astype(BF)
    grad_ref[...] = grad
    low_ref[...] = low
    live = live_tile(length_ref, positions, branch.shape)
    add_rows(
        sum_ref, [jnp.where(live, branch * branch, 0.0), low.astype(F32), upstream * normed, upstream]
    )


def contract_call(lengths, vectors, gelu, normed, cotangent, pieces, positions):
    count, width = cotangent.shape
    hidden = gelu.shape[1]
    return call(
        functools.partial(contract_kernel, positions=positions),
        "contract_norm",
        2 * count * width * hidden,
        count * hidden * 2 + count * width * 14,
        grid=(count // TILE,),
        in_specs=[SMEM, resident(vectors.shape), tiles(hidden), tiles(width), tiles(width)]
        + [picked(piece, width) for piece in pieces],
        out_specs=[tiles(width), tiles(width), tiles(width), resident((8, width))],
        out_shape=[
            jax.ShapeDtypeStruct((count, width), BF),
            jax.ShapeDtypeStruct((count, width), F32),
            jax.ShapeDtypeStruct((count, width), BF),
            jax.ShapeDtypeStruct((8, width), F32),
        ],
    )(lengths, vectors, gelu, normed, cotangent, *[piece[0] for piece in pieces])


def inner_kernel(low_ref, slope_ref, grad_ref, *refs, count):
    contracts, expands, (inner_ref, out_ref, sum_ref) = refs[:count], refs[count : 2 * count], refs[2 * count :]

    @pl.when(pl.program_id(0) == 0)
    def _():
        sum_ref[...] = jnp.zeros_like(sum_ref)

    low, total, at = low_ref[...], grad_ref[...], 0
    for contract, expand in zip(contracts, expands):
        span = slice(at, at + contract.shape[0])
        inner = (dot_nt(low, contract[...]) * slope_ref[:, span].astype(F32)).astype(BF)
        inner_ref[:, span] = inner
        sum_ref[0:1, span] += jnp.sum(inner.astype(F32), axis=0, keepdims=True)
        total = total + dot_nn(inner, expand[...])
        at += contract.shape[0]
    out_ref[...] = total


def inner_back(low, slope, grad, contracts, expands):
    count, width = low.shape
    hidden = slope.shape[1]
    return call(
        functools.partial(inner_kernel, count=len(contracts)),
        "inner_back",
        4 * count * width * hidden,
        count * hidden * 4 + count * width * 10,
        grid=(count // TILE,),
        in_specs=[tiles(width), tiles(hidden), tiles(width)]
        + [picked(piece, width) for piece in contracts + expands],
        out_specs=[tiles(hidden), tiles(width), resident((8, hidden))],
        out_shape=[
            jax.ShapeDtypeStruct((count, hidden), BF),
            jax.ShapeDtypeStruct((count, width), F32),
            jax.ShapeDtypeStruct((8, hidden), F32),
        ],
    )(low, slope, grad, *[piece[0] for piece in contracts + expands])


def feed_weights_kernel(inner_ref, gelu_ref, low_ref, grad_ref, out_ref):
    size = inner_ref.shape[1]
    out_ref[0:size, :] = dot_tn(inner_ref[...], low_ref[...]).astype(BF)
    out_ref[size:, :] = dot_tn(gelu_ref[...], grad_ref[...]).astype(BF)


def feed_weights(inner, gelu, low, grad, half, blocks):
    count, width = low.shape
    size = inner.shape[1] // (2 * blocks)
    columns = pl.BlockSpec((count, size), lambda i: (0, half * blocks + i))
    return call(
        feed_weights_kernel,
        "feed_weights",
        4 * count * width * size * blocks,
        count * size * blocks * 4 + blocks * size * width * 4,
        grid=(blocks,),
        in_specs=[columns, columns, resident((count, width)), resident((count, width))],
        out_specs=pl.BlockSpec((2 * size, width), lambda i: (i, 0)),
        out_shape=jax.ShapeDtypeStruct((blocks * 2 * size, width), BF),
    )(inner, gelu, low, grad)


def middle_back_kernel(vec_ref, hid_ref, n_ref, s_ref, weight_ref, grad_ref, low_ref, ctx_ref, sum_ref):
    upstream, normed = hid_ref[...], n_ref[...]
    grad = norm_back(upstream, normed, s_ref[:, 0:1], vec_ref[1:2, :])
    low = grad.astype(BF)
    grad_ref[...] = grad
    low_ref[...] = low
    ctx_ref[...] = dot_nn(low, weight_ref[...]).astype(BF)
    add_rows(sum_ref, [low.astype(F32), upstream * normed, upstream])


def middle_back(vectors, hidden_grad, normed, inverse, attn_rows):
    count, width = hidden_grad.shape
    return call(
        middle_back_kernel,
        "middle_back",
        2 * count * width * width,
        count * width * 16,
        grid=(count // TILE,),
        in_specs=[resident(vectors.shape), tiles(width), tiles(width), tiles(128), resident((width, width), 3, 0)],
        out_specs=[tiles(width), tiles(width), tiles(width), resident((8, width))],
        out_shape=[
            jax.ShapeDtypeStruct((count, width), F32),
            jax.ShapeDtypeStruct((count, width), BF),
            jax.ShapeDtypeStruct((count, width), BF),
            jax.ShapeDtypeStruct((8, width), F32),
        ],
    )(vectors, hidden_grad, normed, inverse, attn_rows)


def attn_weights_kernel(table_ref, qkv_ref, low_ref, token_ref, ctx_ref, out_ref, *, quarters):
    def put(result):
        size = result.shape[0] // quarters
        for d in range(quarters):
            out_ref[d ^ table_ref[1], 0] = result[d * size : (d + 1) * size, :]

    @pl.when(pl.program_id(0) < 3)
    def _():
        put(dot_tn(qkv_ref[0], token_ref[...]).astype(BF))

    @pl.when(pl.program_id(0) == 3)
    def _():
        put(dot_tn(low_ref[...], ctx_ref[...]).astype(BF))


def attn_weights(table, qkv_grad, out_grad, tokens, context):
    count, width = tokens.shape
    half = width // 2
    return call(
        functools.partial(attn_weights_kernel, quarters=4),
        "attn_weights",
        4 * 2 * count * width * half,
        count * width * 8 + width * width * 4,
        grid_spec=pltpu.PrefetchScalarGridSpec(
            num_scalar_prefetch=1,
            grid=(4,),
            in_specs=[
                pl.BlockSpec((1, count, half), lambda i, t: (jnp.minimum(i, 2), 0, t[0])),
                pl.BlockSpec((count, half), lambda i, t: (0, t[0])),
                resident((count, width)),
                resident((count, width)),
            ],
            out_specs=pl.BlockSpec((4, 1, half // 4, width), lambda i, t: (0, i ^ t[2], 0, 0)),
        ),
        out_shape=jax.ShapeDtypeStruct((4, 4, half // 4, width), BF),
    )(table, qkv_grad, out_grad, tokens, context)


def input_kernel(qkv_ref, weight_ref, grad_ref, out_ref):
    width = out_ref.shape[1]
    total = grad_ref[...]
    for j in range(3):
        total = total + dot_nn(qkv_ref[j], weight_ref[j * width : (j + 1) * width, :])
    out_ref[...] = total.astype(BF)


def input_back(qkv_grad, attn_rows, grad):
    count, width = grad.shape
    return call(
        input_kernel,
        "input_back",
        6 * count * width * width,
        count * width * 12 + width * width * 6,
        grid=(count // TILE,),
        in_specs=[
            pl.BlockSpec((3, TILE, width), lambda t: (0, t, 0)),
            resident((3 * width, width)),
            tiles(width),
        ],
        out_specs=tiles(width),
        out_shape=jax.ShapeDtypeStruct((count, width), BF),
    )(qkv_grad, attn_rows, grad)


def tie(*values):
    return lax.optimization_barrier(values)


def add(*parts):
    return sum(part.astype(F32) for part in parts)


class Links:
    def __init__(self):
        self.dp, self.fsdp = lax.axis_size("dp"), lax.axis_size("fsdp")
        self.paired = (self.dp, self.fsdp) == (4, 8)
        my_dp, my_fsdp = lax.axis_index("dp"), lax.axis_index("fsdp")
        if self.paired:
            self.my_dp, self.my_core, self.my_z = my_dp, my_fsdp & 1, my_fsdp >> 1
        else:
            zero = jnp.zeros((), jnp.int32)
            self.my_dp, self.my_core, self.my_z = zero, zero, zero
        self.my_fsdp = my_fsdp

    def swap(self, values, core=0, dp=0, z=0):
        mask = core + 2 * z + self.fsdp * dp
        pairs = [(i, i ^ mask) for i in range(self.dp * self.fsdp)]
        return lax.ppermute(values, AXES, pairs)

    def table(self):
        e = jnp.arange(2, dtype=jnp.int32)[:, None, None]
        m = jnp.arange(4, dtype=jnp.int32)[None, :, None]
        k = jnp.arange(4, dtype=jnp.int32)[None, None, :]
        if not self.paired:
            return jnp.arange(32, dtype=jnp.int32)
        e, m, k = e ^ self.my_core, m ^ self.my_dp, k ^ self.my_z
        return ((k * 2 + e) * 4 + m).reshape(-1).astype(jnp.int32)

    def flip(self, values, axis, index):
        shape = values.shape
        bits = shape[axis].bit_length() - 1
        split = values.reshape(shape[:axis] + (2,) * bits + shape[axis + 1 :])
        for i in range(bits):
            bit = (index >> (bits - 1 - i)) & 1
            split = jnp.where(bit == 1, jnp.flip(split, axis + i), split)
        return split.reshape(shape)

    def to_exchange(self, natural):
        if not self.paired:
            return natural
        moved = natural.transpose(1, 2, 0, 3)
        return self.flip(self.flip(self.flip(moved, 0, self.my_core), 1, self.my_dp), 2, self.my_z)

    def to_natural(self, exchanged):
        if not self.paired:
            return exchanged
        moved = self.flip(self.flip(self.flip(exchanged, 0, self.my_core), 1, self.my_dp), 2, self.my_z)
        return moved.transpose(2, 0, 1, 3)


def spread_z(links, mine):
    return [mine] + [links.swap(mine, z=k) for k in range(1, 4)]


def spread_plane(links, own):
    one, two = links.swap(own, dp=1), links.swap(own, dp=2)
    return one, two


def spread_corner(links, one, two):
    half = one.shape[0] // 2
    return links.swap(one[:half], dp=2), links.swap(two[half:], dp=1)


def gather_plain(attention, attvector, expand, contract, feedvector):
    def whole(shard):
        return lax.all_gather(shard, "fsdp", axis=0, tiled=True)

    rows = [whole(attention.T), whole(expand.T), whole(contract)]
    return rows, whole(attvector).astype(F32), whole(feedvector).astype(F32)


def reduce_paired(links, near, far):
    mine = add(near, links.swap(far, core=1)).astype(BF)
    block = mine.shape[0] // 4
    half = block // 2
    own = [mine[m * block : (m + 1) * block] for m in range(4)]
    three_a, three_b = links.swap(own[3][:half], dp=2), links.swap(own[3][half:], dp=1)
    one = jnp.concatenate([add(own[1][:half], three_a).astype(BF), own[1][half:]], axis=0)
    two = jnp.concatenate([own[2][:half], add(own[2][half:], three_b).astype(BF)], axis=0)
    summed = add(own[0], links.swap(one, dp=1), links.swap(two, dp=2)).astype(BF)
    return summed


def reduce_z(links, summed, size):
    summed = summed.reshape(-1, 4, size, summed.shape[-1])
    pieces = [summed[:, k].reshape(-1, summed.shape[-1]) for k in range(4)]
    return add(pieces[0], *[links.swap(pieces[k], z=k) for k in range(1, 4)]).astype(BF)


def share_plane(links, final):
    stacked = jnp.stack([final] + [links.swap(final, dp=m) for m in range(1, 4)])
    return links.flip(stacked, 0, links.my_dp)


def per_device(tokens, attention, attvector, expand, contract, feedvector, lengths, cotangent):
    links = Links()
    width = tokens.shape[1]
    positions = tokens.shape[0] // lengths.shape[0]
    hidden = expand.shape[1] * links.fsdp
    att_len, feed_len = attvector.shape[0], feedvector.shape[0]
    size = width // 8
    quad = 4 * size

    if links.paired:
        vectors = jnp.concatenate([attvector, feedvector])
        extra = jnp.pad(vectors, (0, 16 * width - vectors.shape[0])).reshape(16, width)

        def quarter(shard):
            return lax.dynamic_slice_in_dim(shard, links.my_dp * size, size, 0)

        attn_z = spread_z(links, jnp.concatenate([quarter(attention.T), extra], axis=0))
        feed_mine = jnp.concatenate([quarter(expand.T), quarter(contract)], axis=0)
        feed_mine, *attn_z = tie(feed_mine, *attn_z)
        attn_own = jnp.concatenate([part[:size] for part in attn_z], axis=0)
        extras = jnp.concatenate([part[size:] for part in attn_z], axis=0)
        attn_one, attn_two = spread_plane(links, attn_own)
        feed_z = spread_z(links, feed_mine)
        attn_three = spread_corner(links, attn_one, attn_two)
        attn_near = [attn_own, attn_one, attn_two, *attn_three]
        attn_far = [links.swap(part, core=1) for part in attn_near]
        extras = jnp.stack([extras, links.swap(extras, core=1)])
        attn_pieces = attn_near + attn_far
        attn_starts = [0, 4, 8, 12, 14, 16, 20, 24, 28, 30]
        extras = extras.reshape(2, 1, 4, 16 * width)[..., : vectors.shape[0]]
        extras = links.flip(links.flip(extras, 0, links.my_core), 2, links.my_z)
        by_owner = extras.transpose(2, 0, 1, 3).reshape(links.fsdp, -1).astype(F32)
        attvec, feedvec = by_owner[:, :att_len].reshape(-1), by_owner[:, att_len:].reshape(-1)

        feed_own = jnp.concatenate([part[:size] for part in feed_z] + [part[size:] for part in feed_z], axis=0)
        feed_own, *_ = tie(feed_own, *attn_three)
        feed_one, feed_two = spread_plane(links, feed_own)
        feed_far = [links.swap(feed_own, core=1)]
    else:
        rows, attvec, feedvec = gather_plain(attention, attvector, expand, contract, feedvector)
        attn_pieces, attn_starts = [rows[0]], [0]
        expands = [(rows[1], i * quad, quad) for i in range(8)]
        contracts = [(rows[2], i * quad, quad) for i in range(8)]

    def row_of(vector, i, start=0):
        return vector[start + i * width : start + (i + 1) * width]

    project_bias = jnp.stack([row_of(attvec, 0), row_of(attvec, 1)])
    vec_rows = [row_of(attvec, i) for i in (2, 3, 4)] + [row_of(feedvec, i, hidden) for i in range(3)]
    vec_rows = jnp.stack(vec_rows + [jnp.zeros((width,), F32)] * 2)
    inner_bias = links.to_exchange(feedvec[:hidden].reshape(4, 2, 4, size)).reshape(1, hidden)

    projected, attn_rows = project(tokens, project_bias, links.table(), attn_pieces, attn_starts, size)
    context, logs = attend(projected, lengths, positions)
    if links.paired:
        context, feed_one, feed_two = tie(context, feed_one, feed_two)
        feed_three = spread_corner(links, feed_one, feed_two)
        feed_far += [links.swap(feed_one, core=1), links.swap(feed_two, core=1)]
    normed_one, inverse_one, hidden_low, sum_middle = middle(
        lengths, vec_rows, context, attn_rows, tokens, positions
    )
    if links.paired:
        hidden_low, *feed_three = tie(hidden_low, *feed_three)
        feed_near = [feed_own, feed_one, feed_two]
        far_three = [links.swap(part, core=1) for part in feed_three]
        expands = [(part, 0, quad) for part in feed_near] + [(feed_three[0], 0, quad)]
        expands += [(part, 0, quad) for part in feed_far] + [(far_three[0], 0, quad)]
        contracts = [(part, quad, quad) for part in feed_near] + [(feed_three[1], 0, quad)]
        contracts += [(part, quad, quad) for part in feed_far] + [(far_three[1], 0, quad)]
    gelu, slope = expand_call(hidden_low, inner_bias, expands)
    result, grad_two, grad_two_low, sum_two = contract_call(
        lengths, vec_rows, gelu, normed_one, cotangent, contracts, positions
    )
    inner_grad, hidden_grad, sum_inner = inner_back(grad_two_low, slope, grad_two, contracts, expands)
    feed_far_part = feed_weights(inner_grad, gelu, hidden_low, grad_two_low, 1, 4)
    feed_near_part = feed_weights(inner_grad, gelu, hidden_low, grad_two_low, 0, 4)
    grad_one, grad_one_low, context_grad, sum_one = middle_back(
        vec_rows, hidden_grad, normed_one, inverse_one, attn_rows
    )
    qkv_grad, sum_qkv = attend_back(projected, lengths, context_grad, context, logs, positions)

    def attn_part(e):
        table = jnp.stack([links.my_core ^ e, links.my_dp, links.my_z]).astype(jnp.int32)
        return attn_weights(table, qkv_grad, grad_one_low, tokens, context)

    attn_far_part, attn_near_part = attn_part(1), attn_part(0)
    input_grad = input_back(qkv_grad, attn_rows, grad_one)

    if links.paired:
        feed_sum = reduce_paired(links, feed_near_part, feed_far_part)
        feed_sum = share_plane(links, reduce_z(links, feed_sum, size))
        expand_sum = feed_sum[:, :size].reshape(quad, width).astype(F32).T
        contract_sum = feed_sum[:, size:].reshape(quad, width).astype(F32)
        attn_sum = reduce_paired(
            links, attn_near_part.reshape(-1, width), attn_far_part.reshape(-1, width)
        )
        attn_sum = share_plane(links, reduce_z(links, attn_sum, size)).reshape(quad, width).astype(F32).T
    else:
        def finish(natural):
            shard = lax.psum_scatter(natural, "fsdp", scatter_dimension=0, tiled=True)
            return lax.psum(shard, "dp").astype(F32)

        feed = jnp.concatenate([feed_near_part, feed_far_part], axis=0).reshape(8, 2, quad, width)
        expand_sum = finish(feed[:, 0].reshape(hidden, width)).T
        contract_sum = finish(feed[:, 1].reshape(hidden, width))
        both = jnp.stack([attn_near_part, attn_far_part])
        attn_sum = finish(both.transpose(2, 0, 1, 3, 4).reshape(4 * width, width)).T

    inner_sum = links.to_natural(sum_inner[0].reshape(2, 4, 4, size)).reshape(hidden // width, width)
    sum_rows = jnp.sum(sum_qkv, axis=0)
    count_row = jnp.pad(jnp.sum(lengths).astype(F32).reshape(1, 1), ((0, 0), (0, width - 1)))
    packed = jnp.concatenate(
        [sum_rows, sum_one[:3], inner_sum, sum_two[1:4], sum_middle[:2], sum_two[:1], count_row], axis=0
    )
    if links.paired:
        for step in ({"core": 1}, {"dp": 1}, {"dp": 2}, {"z": 1}, {"z": 2}):
            packed = packed + links.swap(packed, **step)
    else:
        packed = lax.psum(packed, AXES)
    flat = packed.reshape(-1)
    att_total, feed_total = att_len * links.fsdp, feed_len * links.fsdp
    att_sum = lax.dynamic_slice_in_dim(flat[:att_total], links.my_fsdp * att_len, att_len, 0)
    feed_vec_sum = lax.dynamic_slice_in_dim(
        flat[att_total : att_total + feed_total], links.my_fsdp * feed_len, feed_len, 0
    )
    squares = jnp.sum(packed[12:15], axis=1)
    root_squares = jnp.sqrt(squares / (packed[15, 0] * width))
    return (result, input_grad, attn_sum, att_sum, expand_sum, contract_sum, feed_vec_sum, root_squares)


def solution(mesh):
    return jax.shard_map(
        per_device,
        mesh=mesh,
        in_specs=(
            P(AXES, None),
            P(None, "fsdp"),
            P("fsdp"),
            P(None, "fsdp"),
            P("fsdp", None),
            P("fsdp"),
            P(AXES),
            P(AXES, None),
        ),
        out_specs=(
            P(AXES, None),
            P(AXES, None),
            P(None, "fsdp"),
            P("fsdp"),
            P(None, "fsdp"),
            P("fsdp", None),
            P("fsdp"),
            P(),
        ),
        check_vma=False,
    )
```

```python
import functools
import math

import jax
import jax.numpy as jnp
from jax import lax
from jax.experimental import pallas as pl
from jax.experimental.pallas import tpu as pltpu
from jax.sharding import PartitionSpec as P

HEAD_DIM = 64
EPSILON = 1e-12
NEGATIVE = -1000000000.0
BF = jnp.bfloat16
F32 = jnp.float32
AXES = ("dp", "fsdp")
LOG2E = 1.0 / math.log(2.0)
SCALE = 1.0 / math.sqrt(HEAD_DIM)
TILE = 256
PAIR = 2 * HEAD_DIM


def dot_nt(left, right, precision=None):
    return lax.dot_general(
        left, right, (((1,), (1,)), ((), ())), precision=precision, preferred_element_type=F32
    )


def dot_nn(left, right):
    return jnp.dot(left, right, preferred_element_type=F32)


def dot_tn(left, right):
    return lax.dot_general(left, right, (((0,), (0,)), ((), ())), preferred_element_type=F32)


def resident(shape, *index):
    index = index or (0,) * len(shape)
    return pl.BlockSpec(shape, lambda *_: index)


def call(kernel, name, flops, bytes_moved, **kwargs):
    cost = pl.CostEstimate(flops=flops, bytes_accessed=bytes_moved, transcendentals=0)
    return pl.pallas_call(kernel, name=name, cost_estimate=cost, **kwargs)


SMEM = pl.BlockSpec(memory_space=pltpu.SMEM)


def project_kernel(table_ref, bias_ref, token_ref, *refs, starts, size):
    pieces, (out_ref, rows_ref) = refs[:-2], refs[-2:]

    @pl.when(pl.program_id(0) == 0)
    def _():
        for piece, start in zip(pieces, starts):
            for i in range(piece.shape[0] // size):
                there = pl.multiple_of(table_ref[start + i] * size, size)
                rows_ref[pl.ds(there, size), :] = piece[i * size : (i + 1) * size, :]

    width = token_ref.shape[1]
    for j in range(3):
        part = dot_nt(token_ref[...], rows_ref[j * width : (j + 1) * width, :])
        if j == 0:
            part = part + bias_ref[0:1, :]
        if j == 2:
            part = part + bias_ref[1:2, :]
        out_ref[j] = part.astype(BF)


def project(tokens, bias, table, pieces, starts, size):
    count, width = tokens.shape
    total = sum(piece.shape[0] for piece in pieces)
    return call(
        functools.partial(project_kernel, starts=starts, size=size),
        "project",
        2 * count * width * 3 * width,
        2 * (4 * count * width + 2 * total * width),
        grid=(count // TILE,),
        in_specs=[SMEM, resident(bias.shape), pl.BlockSpec((TILE, width), lambda t: (t, 0))]
        + [resident(piece.shape) for piece in pieces],
        out_specs=[
            pl.BlockSpec((3, TILE, width), lambda t: (0, t, 0)),
            resident((total, width)),
        ],
        out_shape=[
            jax.ShapeDtypeStruct((3, count, width), BF),
            jax.ShapeDtypeStruct((total, width), BF),
        ],
    )(table, bias, tokens, *pieces)


def head_lanes(values, head):
    lane = lax.broadcasted_iota(jnp.int32, values.shape, 1)
    return jnp.where((lane >= HEAD_DIM) == (head == 1), values, jnp.zeros_like(values))


def scores_of(keys, queries, length, head):
    scores = dot_nt(keys, head_lanes(queries, head))
    place = lax.broadcasted_iota(jnp.int32, scores.shape, 0)
    return jnp.where(place < length, scores, NEGATIVE / SCALE)


def attend_kernel(length_ref, q_ref, k_ref, v_ref, out_ref, log_ref):
    length = length_ref[pl.program_id(0)]
    keys = k_ref[0]
    values_t = v_ref[0].T
    halves = []
    for head in range(2):
        scores = scores_of(keys, q_ref[0], length, head)
        peak = jnp.max(scores, axis=0, keepdims=True) * (SCALE * LOG2E)
        weights = jnp.exp2(scores * (SCALE * LOG2E) - peak)
        total = jnp.sum(weights, axis=0, keepdims=True)
        part = dot_nn(values_t[head * HEAD_DIM : (head + 1) * HEAD_DIM, :], weights.astype(BF))
        halves.append(part * (1.0 / total))
        log_ref[0, 0, head : head + 1, :] = peak + jnp.log2(total)
    out_ref[...] = jnp.concatenate(halves, axis=0).T.astype(BF)


def attend(projected, lengths, positions):
    _, count, width = projected.shape
    rows, pairs = count // positions, width // PAIR
    block = (1, positions, PAIR)
    flops = 4 * rows * pairs * 2 * positions * positions * HEAD_DIM
    return call(
        attend_kernel,
        "attend",
        2 * flops,
        8 * count * width,
        grid_spec=pltpu.PrefetchScalarGridSpec(
            num_scalar_prefetch=1,
            grid=(rows, pairs),
            in_specs=[pl.BlockSpec(block, lambda r, p, _, j=j: (j, r, p)) for j in range(3)],
            out_specs=[
                pl.BlockSpec((positions, PAIR), lambda r, p, _: (r, p)),
                pl.BlockSpec((1, 1, 2, positions), lambda r, p, _: (r, p, 0, 0)),
            ],
        ),
        out_shape=[
            jax.ShapeDtypeStruct((count, width), BF),
            jax.ShapeDtypeStruct((rows, pairs, 2, positions), F32),
        ],
    )(lengths, projected, projected, projected)


def attend_back_kernel(
    length_ref, _, q_ref, k_ref, v_ref, grad_ref, ctx_ref, log_ref, out_ref, sum_ref
):
    length = length_ref[pl.program_id(0)]
    queries, keys, values, grad = q_ref[0], k_ref[0], v_ref[0], grad_ref[...]
    keys_t = keys.T
    product = grad.astype(F32) * ctx_ref[...].astype(F32)
    key_grad, value_grad, query_halves = None, None, []
    for head in range(2):
        scores = scores_of(keys, queries, length, head)
        wide = jnp.exp2(scores * (SCALE * LOG2E) - log_ref[0, 0, head : head + 1, :])
        grad_head = head_lanes(grad, head)
        value_part = dot_nn(wide.astype(BF), grad_head)
        weight_grad = dot_nt(values, grad_head)
        ones = head_lanes(jnp.ones((8, PAIR), F32), head)
        row_total = dot_nt(ones, product, lax.Precision.HIGHEST)[0:1, :]
        score_grad = (wide * (weight_grad - row_total)).astype(BF)
        key_part = dot_nn(score_grad, head_lanes(queries, head))
        query_halves.append(dot_nn(keys_t[head * HEAD_DIM : (head + 1) * HEAD_DIM, :], score_grad))
        value_grad = value_part if head == 0 else value_grad + value_part
        key_grad = key_part if head == 0 else key_grad + key_part
    query_low = (jnp.concatenate(query_halves, axis=0) * SCALE).T.astype(BF)
    value_low = value_grad.astype(BF)
    out_ref[0] = query_low
    out_ref[1] = (key_grad * SCALE).astype(BF)
    out_ref[2] = value_low
    sum_ref[0, 0:1, :] = jnp.sum(query_low.astype(F32), axis=0, keepdims=True)
    sum_ref[0, 1:2, :] = jnp.sum(value_low.astype(F32), axis=0, keepdims=True)


def attend_back(projected, lengths, side, context_grad, context, logs, positions):
    _, count, width = projected.shape
    rows, pairs = count // positions, width // PAIR // 2
    block = (1, positions, PAIR)
    flat = pl.BlockSpec((positions, PAIR), lambda r, p, _, s: (r, s[0] * pairs + p))
    flops = 10 * rows * pairs * 2 * positions * positions * HEAD_DIM
    return call(
        attend_back_kernel,
        "attend_back",
        2 * flops,
        8 * count * width,
        grid_spec=pltpu.PrefetchScalarGridSpec(
            num_scalar_prefetch=2,
            grid=(rows, pairs),
            in_specs=[
                pl.BlockSpec(block, lambda r, p, _, s, j=j: (j, r, s[0] * pairs + p)) for j in range(3)
            ]
            + [
                flat,
                flat,
                pl.BlockSpec((1, 1, 2, positions), lambda r, p, _, s: (r, s[0] * pairs + p, 0, 0)),
            ],
            out_specs=[
                pl.BlockSpec((3, positions, PAIR), lambda r, p, _, s: (0, r, p)),
                pl.BlockSpec((1, 2, PAIR), lambda r, p, _, s: (r, 0, p)),
            ],
        ),
        out_shape=[
            jax.ShapeDtypeStruct((3, count, width // 2), BF),
            jax.ShapeDtypeStruct((rows, 2, width // 2), F32),
        ],
    )(lengths, side, projected, projected, projected, context_grad, context, logs)


def normalize(residual):
    centered = residual - jnp.mean(residual, axis=-1, keepdims=True)
    inverse = lax.rsqrt(jnp.mean(centered * centered, axis=-1, keepdims=True) + EPSILON)
    return centered * inverse, inverse


def norm_back(upstream, normed, inverse, gain):
    scaled = upstream * gain
    mean_plain = jnp.mean(scaled, axis=-1, keepdims=True)
    mean_normed = jnp.mean(scaled * normed, axis=-1, keepdims=True)
    return inverse * (scaled - mean_plain - normed * mean_normed)


def live_tile(length_ref, positions, shape):
    first = pl.program_id(0) * TILE
    place = lax.broadcasted_iota(jnp.int32, shape, 0) + first % positions
    return place < length_ref[first // positions]


def add_rows(ref, rows):
    @pl.when(pl.program_id(0) == 0)
    def _():
        ref[...] = jnp.zeros_like(ref)

    for i, row in enumerate(rows):
        ref[i : i + 1, :] += jnp.sum(row, axis=0, keepdims=True)


def middle_kernel(length_ref, vec_ref, ctx_ref, weight_ref, token_ref, n_ref, s_ref, low_ref, sum_ref, *, positions):
    branch = dot_nt(ctx_ref[...], weight_ref[...]) + vec_ref[0:1, :]
    tokens = token_ref[...].astype(F32)
    normed, inverse = normalize(tokens + branch)
    n_ref[...] = normed
    s_ref[...] = jnp.broadcast_to(inverse, s_ref.shape)
    low_ref[...] = (normed * vec_ref[1:2, :] + vec_ref[2:3, :]).astype(BF)
    live = live_tile(length_ref, positions, tokens.shape)
    add_rows(sum_ref, [jnp.where(live, tokens * tokens, 0.0), jnp.where(live, branch * branch, 0.0)])


def tiles(width):
    return pl.BlockSpec((TILE, width), lambda t: (t, 0))


def middle(lengths, vectors, context, attn_rows, tokens, positions):
    count, width = tokens.shape
    return call(
        functools.partial(middle_kernel, positions=positions),
        "middle",
        2 * count * width * width,
        count * width * 12,
        grid=(count // TILE,),
        in_specs=[SMEM, resident(vectors.shape), tiles(width), resident((width, width), 3, 0), tiles(width)],
        out_specs=[tiles(width), tiles(128), tiles(width), resident((8, width))],
        out_shape=[
            jax.ShapeDtypeStruct((count, width), F32),
            jax.ShapeDtypeStruct((count, 128), F32),
            jax.ShapeDtypeStruct((count, width), BF),
            jax.ShapeDtypeStruct((8, width), F32),
        ],
    )(lengths, vectors, context, attn_rows, tokens)


def gelu_parts(inner):
    cumulative = 0.5 * (1.0 + lax.erf(inner * (1.0 / math.sqrt(2.0))))
    density = jnp.exp2(inner * inner * (-0.5 * LOG2E)) * (1.0 / math.sqrt(2.0 * math.pi))
    return inner * cumulative, cumulative + inner * density


def expand_kernel(bias_ref, low_ref, *refs):
    pieces, (gelu_ref, slope_ref) = refs[:-2], refs[-2:]
    low, at = low_ref[...], 0
    for piece in pieces:
        size = piece.shape[0]
        inner = dot_nt(low, piece[...]) + bias_ref[0:1, at : at + size]
        gelu, slope = gelu_parts(inner)
        gelu_ref[:, at : at + size] = gelu.astype(BF)
        slope_ref[:, at : at + size] = slope.astype(BF)
        at += size


def picked(piece, width):
    array, start, size = piece
    return pl.BlockSpec((size, width), lambda *_, at=start // size: (at, 0))


def expand_call(low, bias, pieces):
    count, width = low.shape
    hidden = bias.shape[1]
    return call(
        expand_kernel,
        "expand_gelu",
        2 * count * width * hidden,
        count * hidden * 4,
        grid=(count // TILE,),
        in_specs=[resident(bias.shape), tiles(width)] + [picked(piece, width) for piece in pieces],
        out_specs=[tiles(hidden), tiles(hidden)],
        out_shape=[jax.ShapeDtypeStruct((count, hidden), BF)] * 2,
    )(bias, low, *[piece[0] for piece in pieces])


def contract_kernel(length_ref, vec_ref, gelu_ref, n_ref, cot_ref, *refs, positions):
    pieces, (out_ref, grad_ref, low_ref, sum_ref) = refs[:-4], refs[-4:]
    branch, at = vec_ref[3:4, :], 0
    for piece in pieces:
        size = piece.shape[0]
        branch = branch + dot_nn(gelu_ref[:, at : at + size], piece[...])
        at += size
    first = n_ref[...] * vec_ref[1:2, :] + vec_ref[2:3, :]
    normed, inverse = normalize(first + branch)
    out_ref[...] = (normed * vec_ref[4:5, :] + vec_ref[5:6, :]).astype(BF)
    upstream = cot_ref[...].astype(F32)
    grad = norm_back(upstream, normed, inverse, vec_ref[4:5, :])
    low = grad.astype(BF)
    grad_ref[...] = grad
    low_ref[...] = low
    live = live_tile(length_ref, positions, branch.shape)
    add_rows(
        sum_ref, [jnp.where(live, branch * branch, 0.0), low.astype(F32), upstream * normed, upstream]
    )


def contract_call(lengths, vectors, gelu, normed, cotangent, pieces, positions):
    count, width = cotangent.shape
    hidden = gelu.shape[1]
    return call(
        functools.partial(contract_kernel, positions=positions),
        "contract_norm",
        2 * count * width * hidden,
        count * hidden * 2 + count * width * 14,
        grid=(count // TILE,),
        in_specs=[SMEM, resident(vectors.shape), tiles(hidden), tiles(width), tiles(width)]
        + [picked(piece, width) for piece in pieces],
        out_specs=[tiles(width), tiles(width), tiles(width), resident((8, width))],
        out_shape=[
            jax.ShapeDtypeStruct((count, width), BF),
            jax.ShapeDtypeStruct((count, width), F32),
            jax.ShapeDtypeStruct((count, width), BF),
            jax.ShapeDtypeStruct((8, width), F32),
        ],
    )(lengths, vectors, gelu, normed, cotangent, *[piece[0] for piece in pieces])


def inner_kernel(low_ref, slope_ref, grad_ref, *refs, count):
    contracts, expands, (inner_ref, out_ref, sum_ref) = refs[:count], refs[count : 2 * count], refs[2 * count :]

    @pl.when(pl.program_id(0) == 0)
    def _():
        sum_ref[...] = jnp.zeros_like(sum_ref)

    low, total, at = low_ref[...], grad_ref[...], 0
    for contract, expand in zip(contracts, expands):
        span = slice(at, at + contract.shape[0])
        inner = (dot_nt(low, contract[...]) * slope_ref[:, span].astype(F32)).astype(BF)
        inner_ref[:, span] = inner
        sum_ref[0:1, span] += jnp.sum(inner.astype(F32), axis=0, keepdims=True)
        total = total + dot_nn(inner, expand[...])
        at += contract.shape[0]
    out_ref[...] = total


def inner_back(low, slope, grad, contracts, expands):
    count, width = low.shape
    hidden = slope.shape[1]
    return call(
        functools.partial(inner_kernel, count=len(contracts)),
        "inner_back",
        4 * count * width * hidden,
        count * hidden * 4 + count * width * 10,
        grid=(count // TILE,),
        in_specs=[tiles(width), tiles(hidden), tiles(width)]
        + [picked(piece, width) for piece in contracts + expands],
        out_specs=[tiles(hidden), tiles(width), resident((8, hidden))],
        out_shape=[
            jax.ShapeDtypeStruct((count, hidden), BF),
            jax.ShapeDtypeStruct((count, width), F32),
            jax.ShapeDtypeStruct((8, hidden), F32),
        ],
    )(low, slope, grad, *[piece[0] for piece in contracts + expands])


def feed_weights_kernel(inner_ref, gelu_ref, low_ref, grad_ref, out_ref):
    size = inner_ref.shape[1]
    out_ref[0:size, :] = dot_tn(inner_ref[...], low_ref[...]).astype(BF)
    out_ref[size:, :] = dot_tn(gelu_ref[...], grad_ref[...]).astype(BF)


def feed_weights(inner, gelu, low, grad, half, blocks):
    count, width = low.shape
    size = inner.shape[1] // (2 * blocks)
    columns = pl.BlockSpec((count, size), lambda i: (0, half * blocks + i))
    return call(
        feed_weights_kernel,
        "feed_weights",
        4 * count * width * size * blocks,
        count * size * blocks * 4 + blocks * size * width * 4,
        grid=(blocks,),
        in_specs=[columns, columns, resident((count, width)), resident((count, width))],
        out_specs=pl.BlockSpec((2 * size, width), lambda i: (i, 0)),
        out_shape=jax.ShapeDtypeStruct((blocks * 2 * size, width), BF),
    )(inner, gelu, low, grad)


def middle_back_kernel(vec_ref, hid_ref, n_ref, s_ref, weight_ref, grad_ref, low_ref, ctx_ref, sum_ref):
    upstream, normed = hid_ref[...], n_ref[...]
    grad = norm_back(upstream, normed, s_ref[:, 0:1], vec_ref[1:2, :])
    low = grad.astype(BF)
    grad_ref[...] = grad
    low_ref[...] = low
    ctx_ref[...] = dot_nn(low, weight_ref[...]).astype(BF)
    add_rows(sum_ref, [low.astype(F32), upstream * normed, upstream])


def middle_back(vectors, hidden_grad, normed, inverse, attn_rows):
    count, width = hidden_grad.shape
    return call(
        middle_back_kernel,
        "middle_back",
        2 * count * width * width,
        count * width * 16,
        grid=(count // TILE,),
        in_specs=[resident(vectors.shape), tiles(width), tiles(width), tiles(128), resident((width, width), 3, 0)],
        out_specs=[tiles(width), tiles(width), tiles(width), resident((8, width))],
        out_shape=[
            jax.ShapeDtypeStruct((count, width), F32),
            jax.ShapeDtypeStruct((count, width), BF),
            jax.ShapeDtypeStruct((count, width), BF),
            jax.ShapeDtypeStruct((8, width), F32),
        ],
    )(vectors, hidden_grad, normed, inverse, attn_rows)


def attn_weights_kernel(table_ref, qkv_ref, low_ref, token_ref, ctx_ref, out_ref, *, quarters):
    def put(result):
        size = result.shape[0] // quarters
        for d in range(quarters):
            out_ref[d ^ table_ref[1], 0] = result[d * size : (d + 1) * size, :]

    @pl.when(pl.program_id(0) < 3)
    def _():
        put(dot_tn(qkv_ref[0], token_ref[...]).astype(BF))

    @pl.when(pl.program_id(0) == 3)
    def _():
        put(dot_tn(low_ref[...], ctx_ref[...]).astype(BF))


def attn_weights(table, qkv_grad, out_grad, tokens, context):
    count, width = tokens.shape
    half = width // 2
    return call(
        functools.partial(attn_weights_kernel, quarters=4),
        "attn_weights",
        4 * 2 * count * width * half,
        count * width * 8 + width * width * 4,
        grid_spec=pltpu.PrefetchScalarGridSpec(
            num_scalar_prefetch=1,
            grid=(4,),
            in_specs=[
                pl.BlockSpec((1, count, half), lambda i, t: (jnp.minimum(i, 2), 0, 0)),
                pl.BlockSpec((count, half), lambda i, t: (0, t[0])),
                resident((count, width)),
                resident((count, width)),
            ],
            out_specs=pl.BlockSpec((4, 1, half // 4, width), lambda i, t: (0, i ^ t[2], 0, 0)),
        ),
        out_shape=jax.ShapeDtypeStruct((4, 4, half // 4, width), BF),
    )(table, qkv_grad, out_grad, tokens, context)


def input_kernel(core_ref, near_ref, far_ref, weight_ref, grad_ref, out_ref):
    width = out_ref.shape[1]
    near_first = core_ref[0] == 0
    total = grad_ref[...]
    for j in range(3):
        near, far = near_ref[j], far_ref[j]
        whole = jnp.concatenate([jnp.where(near_first, near, far), jnp.where(near_first, far, near)], axis=1)
        total = total + dot_nn(whole, weight_ref[j * width : (j + 1) * width, :])
    out_ref[...] = total.astype(BF)


def input_back(core, near, far, attn_rows, grad):
    count, width = grad.shape
    half = pl.BlockSpec((3, TILE, width // 2), lambda t: (0, t, 0))
    return call(
        input_kernel,
        "input_back",
        6 * count * width * width,
        count * width * 12 + width * width * 6,
        grid=(count // TILE,),
        in_specs=[SMEM, half, half, resident((3 * width, width)), tiles(width)],
        out_specs=tiles(width),
        out_shape=jax.ShapeDtypeStruct((count, width), BF),
    )(core, near, far, attn_rows, grad)


def tie(*values):
    return lax.optimization_barrier(values)


def add(*parts):
    return sum(part.astype(F32) for part in parts)


class Links:
    def __init__(self):
        self.dp, self.fsdp = lax.axis_size("dp"), lax.axis_size("fsdp")
        self.paired = (self.dp, self.fsdp) == (4, 8)
        my_dp, my_fsdp = lax.axis_index("dp"), lax.axis_index("fsdp")
        if self.paired:
            self.my_dp, self.my_core, self.my_z = my_dp, my_fsdp & 1, my_fsdp >> 1
        else:
            zero = jnp.zeros((), jnp.int32)
            self.my_dp, self.my_core, self.my_z = zero, zero, zero
        self.my_fsdp = my_fsdp

    def swap(self, values, core=0, dp=0, z=0):
        mask = core + 2 * z + self.fsdp * dp
        pairs = [(i, i ^ mask) for i in range(self.dp * self.fsdp)]
        return lax.ppermute(values, AXES, pairs)

    def table(self):
        e = jnp.arange(2, dtype=jnp.int32)[:, None, None]
        m = jnp.arange(4, dtype=jnp.int32)[None, :, None]
        k = jnp.arange(4, dtype=jnp.int32)[None, None, :]
        if not self.paired:
            return jnp.arange(32, dtype=jnp.int32)
        e, m, k = e ^ self.my_core, m ^ self.my_dp, k ^ self.my_z
        return ((k * 2 + e) * 4 + m).reshape(-1).astype(jnp.int32)

    def flip(self, values, axis, index):
        shape = values.shape
        bits = shape[axis].bit_length() - 1
        split = values.reshape(shape[:axis] + (2,) * bits + shape[axis + 1 :])
        for i in range(bits):
            bit = (index >> (bits - 1 - i)) & 1
            split = jnp.where(bit == 1, jnp.flip(split, axis + i), split)
        return split.reshape(shape)

    def to_exchange(self, natural):
        if not self.paired:
            return natural
        moved = natural.transpose(1, 2, 0, 3)
        return self.flip(self.flip(self.flip(moved, 0, self.my_core), 1, self.my_dp), 2, self.my_z)

    def to_natural(self, exchanged):
        if not self.paired:
            return exchanged
        moved = self.flip(self.flip(self.flip(exchanged, 0, self.my_core), 1, self.my_dp), 2, self.my_z)
        return moved.transpose(2, 0, 1, 3)


def spread_z(links, mine):
    return [mine] + [links.swap(mine, z=k) for k in range(1, 4)]


def spread_plane(links, own):
    one, two = links.swap(own, dp=1), links.swap(own, dp=2)
    return one, two


def spread_corner(links, one, two):
    half = one.shape[0] // 2
    return links.swap(one[:half], dp=2), links.swap(two[half:], dp=1)


def gather_plain(attention, attvector, expand, contract, feedvector):
    def whole(shard):
        return lax.all_gather(shard, "fsdp", axis=0, tiled=True)

    rows = [whole(attention.T), whole(expand.T), whole(contract)]
    return rows, whole(attvector).astype(F32), whole(feedvector).astype(F32)


def reduce_core(links, near, far_got):
    return add(near, far_got).astype(BF)


def reduce_corner(links, mine):
    block = mine.shape[0] // 4
    half = block // 2
    corner = mine[3 * block :]
    return links.swap(corner[:half], dp=2), links.swap(corner[half:], dp=1)


def reduce_sides(mine, corners):
    block = mine.shape[0] // 4
    half = block // 2
    own, one, two = (mine[m * block : (m + 1) * block] for m in range(3))
    one = jnp.concatenate([add(one[:half], corners[0]).astype(BF), one[half:]], axis=0)
    two = jnp.concatenate([two[:half], add(two[half:], corners[1]).astype(BF)], axis=0)
    return own, one, two


def reduce_z(links, summed, size):
    summed = summed.reshape(-1, 4, size, summed.shape[-1])
    pieces = [summed[:, k].reshape(-1, summed.shape[-1]) for k in range(4)]
    return pieces[0], [links.swap(pieces[k], z=k) for k in range(1, 4)]


def share_plane(links, final):
    stacked = jnp.stack([final] + [links.swap(final, dp=m) for m in range(1, 4)])
    return links.flip(stacked, 0, links.my_dp)


def per_device(tokens, attention, attvector, expand, contract, feedvector, lengths, cotangent):
    links = Links()
    width = tokens.shape[1]
    positions = tokens.shape[0] // lengths.shape[0]
    hidden = expand.shape[1] * links.fsdp
    att_len, feed_len = attvector.shape[0], feedvector.shape[0]
    size = width // 8
    quad = 4 * size

    if links.paired:
        vectors = jnp.concatenate([attvector, feedvector])
        extra = jnp.pad(vectors, (0, 16 * width - vectors.shape[0])).reshape(16, width)

        def quarter(shard):
            return lax.dynamic_slice_in_dim(shard, links.my_dp * size, size, 0)

        attn_z = spread_z(links, jnp.concatenate([quarter(attention.T), extra], axis=0))
        feed_mine = jnp.concatenate([quarter(expand.T), quarter(contract)], axis=0)
        feed_mine, *attn_z = tie(feed_mine, *attn_z)
        attn_own = jnp.concatenate([part[:size] for part in attn_z], axis=0)
        extras = jnp.concatenate([part[size:] for part in attn_z], axis=0)
        attn_one, attn_two = spread_plane(links, attn_own)
        feed_z = spread_z(links, feed_mine)
        attn_three = spread_corner(links, attn_one, attn_two)
        attn_near = [attn_own, attn_one, attn_two, *attn_three]
        attn_far = [links.swap(part, core=1) for part in attn_near]
        extras = jnp.stack([extras, links.swap(extras, core=1)])
        attn_pieces = attn_near + attn_far
        attn_starts = [0, 4, 8, 12, 14, 16, 20, 24, 28, 30]
        extras = extras.reshape(2, 1, 4, 16 * width)[..., : vectors.shape[0]]
        extras = links.flip(links.flip(extras, 0, links.my_core), 2, links.my_z)
        by_owner = extras.transpose(2, 0, 1, 3).reshape(links.fsdp, -1).astype(F32)
        attvec, feedvec = by_owner[:, :att_len].reshape(-1), by_owner[:, att_len:].reshape(-1)

        feed_own = jnp.concatenate([part[:size] for part in feed_z] + [part[size:] for part in feed_z], axis=0)
        feed_own, *_ = tie(feed_own, *attn_three)
        feed_one, feed_two = spread_plane(links, feed_own)
        feed_far = [links.swap(feed_own, core=1)]
    else:
        rows, attvec, feedvec = gather_plain(attention, attvector, expand, contract, feedvector)
        attn_pieces, attn_starts = [rows[0]], [0]
        expands = [(rows[1], i * quad, quad) for i in range(8)]
        contracts = [(rows[2], i * quad, quad) for i in range(8)]

    def row_of(vector, i, start=0):
        return vector[start + i * width : start + (i + 1) * width]

    project_bias = jnp.stack([row_of(attvec, 0), row_of(attvec, 1)])
    vec_rows = [row_of(attvec, i) for i in (2, 3, 4)] + [row_of(feedvec, i, hidden) for i in range(3)]
    vec_rows = jnp.stack(vec_rows + [jnp.zeros((width,), F32)] * 2)
    inner_bias = links.to_exchange(feedvec[:hidden].reshape(4, 2, 4, size)).reshape(1, hidden)

    projected, attn_rows = project(tokens, project_bias, links.table(), attn_pieces, attn_starts, size)
    context, logs = attend(projected, lengths, positions)
    if links.paired:
        context, feed_one, feed_two = tie(context, feed_one, feed_two)
        feed_three = spread_corner(links, feed_one, feed_two)
        feed_far += [links.swap(feed_one, core=1), links.swap(feed_two, core=1)]
    normed_one, inverse_one, hidden_low, sum_middle = middle(
        lengths, vec_rows, context, attn_rows, tokens, positions
    )
    if links.paired:
        hidden_low, *feed_three = tie(hidden_low, *feed_three)
        feed_near = [feed_own, feed_one, feed_two]
        far_three = [links.swap(part, core=1) for part in feed_three]
        expands = [(part, 0, quad) for part in feed_near] + [(feed_three[0], 0, quad)]
        expands += [(part, 0, quad) for part in feed_far] + [(far_three[0], 0, quad)]
        contracts = [(part, quad, quad) for part in feed_near] + [(feed_three[1], 0, quad)]
        contracts += [(part, quad, quad) for part in feed_far] + [(far_three[1], 0, quad)]
    gelu, slope = expand_call(hidden_low, inner_bias, expands)
    result, grad_two, grad_two_low, sum_two = contract_call(
        lengths, vec_rows, gelu, normed_one, cotangent, contracts, positions
    )
    inner_grad, hidden_grad, sum_inner = inner_back(grad_two_low, slope, grad_two, contracts, expands)
    feed_far = feed_weights(inner_grad, gelu, hidden_low, grad_two_low, 1, 4)
    inner_grad, feed_far = tie(inner_grad, feed_far)
    feed_near = feed_weights(inner_grad, gelu, hidden_low, grad_two_low, 0, 4)
    if links.paired:
        feed_far = links.swap(feed_far, core=1)
        feed_mine = reduce_core(links, feed_near, feed_far)
        hidden_grad, feed_mine = tie(hidden_grad, feed_mine)
        feed_corners = reduce_corner(links, feed_mine)
    else:
        hidden_grad, feed_near, feed_far = tie(hidden_grad, feed_near, feed_far)
    grad_one, grad_one_low, context_grad, sum_one = middle_back(
        vec_rows, hidden_grad, normed_one, inverse_one, attn_rows
    )
    if links.paired:
        context_grad, *feed_corners = tie(context_grad, *feed_corners)
        feed_own, feed_one, feed_two = reduce_sides(feed_mine, feed_corners)
        context_grad, feed_one, feed_two = tie(context_grad, feed_one, feed_two)
        feed_one, feed_two = links.swap(feed_one, dp=1), links.swap(feed_two, dp=2)

    def attn_part(e, context_grad):
        table = jnp.stack([links.my_core ^ e, links.my_dp, links.my_z]).astype(jnp.int32)
        qkv_grad, sums = attend_back(
            projected, lengths, table[:1], context_grad, context, logs, positions
        )
        return qkv_grad, attn_weights(table, qkv_grad, grad_one_low, tokens, context), sums

    qkv_far, attn_far, sum_far = attn_part(1, context_grad)
    if links.paired:
        context_grad, feed_one, feed_two, attn_far = tie(context_grad, feed_one, feed_two, attn_far)
        feed_sum = add(feed_own, feed_one, feed_two).astype(BF)
        context_grad, feed_sum = tie(context_grad, feed_sum)
        feed_piece, feed_z = reduce_z(links, feed_sum, size)
        attn_far = links.swap(attn_far.reshape(-1, width), core=1)
    else:
        context_grad, attn_far = tie(context_grad, attn_far)
    qkv_near, sum_near = attend_back(
        projected, lengths, links.my_core.reshape(1).astype(jnp.int32), context_grad, context, logs, positions
    )
    table = jnp.stack([links.my_core, links.my_dp, links.my_z]).astype(jnp.int32)
    if links.paired:
        qkv_near, *feed_z = tie(qkv_near, *feed_z)
        feed_final = add(feed_piece, *feed_z).astype(BF)
        qkv_near, feed_final = tie(qkv_near, feed_final)
        feed_shared = share_plane(links, feed_final)
    attn_near = attn_weights(table, qkv_near, grad_one_low, tokens, context)
    if links.paired:
        attn_mine = reduce_core(links, attn_near.reshape(-1, width), attn_far)
        qkv_last, attn_mine = tie(qkv_near, attn_mine)
        input_grad = input_back(table[:1], qkv_last, qkv_far, attn_rows, grad_one)
        corners = reduce_corner(links, attn_mine)
        attn_own, attn_one, attn_two = reduce_sides(attn_mine, corners)
        attn_one, attn_two = links.swap(attn_one, dp=1), links.swap(attn_two, dp=2)
        attn_sum = add(attn_own, attn_one, attn_two).astype(BF)
        attn_sum, input_grad = tie(attn_sum, input_grad)
        attn_piece, attn_z = reduce_z(links, attn_sum, size)
        attn_final = add(attn_piece, *attn_z).astype(BF)
        attn_sum = share_plane(links, attn_final).reshape(quad, width).astype(F32).T
        expand_sum = feed_shared[:, :size].reshape(quad, width).astype(F32).T
        contract_sum = feed_shared[:, size:].reshape(quad, width).astype(F32)
    else:
        input_grad = input_back(table[:1], qkv_near, qkv_far, attn_rows, grad_one)

        def finish(natural):
            shard = lax.psum_scatter(natural, "fsdp", scatter_dimension=0, tiled=True)
            return lax.psum(shard, "dp").astype(F32)

        feed = jnp.concatenate([feed_near, feed_far], axis=0).reshape(8, 2, quad, width)
        expand_sum = finish(feed[:, 0].reshape(hidden, width)).T
        contract_sum = finish(feed[:, 1].reshape(hidden, width))
        both = jnp.stack([attn_near, attn_far])
        attn_sum = finish(both.transpose(2, 0, 1, 3, 4).reshape(4 * width, width)).T

    sums = [jnp.sum(part, axis=0) for part in (sum_near, sum_far)]
    near_first = links.my_core == 0
    sum_rows = jnp.concatenate(
        [jnp.where(near_first, *sums), jnp.where(near_first, sums[1], sums[0])], axis=1
    )
    inner_sum = links.to_natural(sum_inner[0].reshape(2, 4, 4, size)).reshape(hidden // width, width)
    count_row = jnp.pad(jnp.sum(lengths).astype(F32).reshape(1, 1), ((0, 0), (0, width - 1)))
    packed = jnp.concatenate(
        [sum_rows, sum_one[:3], inner_sum, sum_two[1:4], sum_middle[:2], sum_two[:1], count_row], axis=0
    )
    if links.paired:
        packed, attn_mine = tie(packed, attn_mine)
        for step in ({"core": 1}, {"dp": 1}, {"dp": 2}, {"z": 1}, {"z": 2}):
            packed = packed + links.swap(packed, **step)
    else:
        packed = lax.psum(packed, AXES)
    flat = packed.reshape(-1)
    att_total, feed_total = att_len * links.fsdp, feed_len * links.fsdp
    att_sum = lax.dynamic_slice_in_dim(flat[:att_total], links.my_fsdp * att_len, att_len, 0)
    feed_vec_sum = lax.dynamic_slice_in_dim(
        flat[att_total : att_total + feed_total], links.my_fsdp * feed_len, feed_len, 0
    )
    squares = jnp.sum(packed[12:15], axis=1)
    root_squares = jnp.sqrt(squares / (packed[15, 0] * width))
    return (result, input_grad, attn_sum, att_sum, expand_sum, contract_sum, feed_vec_sum, root_squares)


def solution(mesh):
    return jax.shard_map(
        per_device,
        mesh=mesh,
        in_specs=(
            P(AXES, None),
            P(None, "fsdp"),
            P("fsdp"),
            P(None, "fsdp"),
            P("fsdp", None),
            P("fsdp"),
            P(AXES),
            P(AXES, None),
        ),
        out_specs=(
            P(AXES, None),
            P(AXES, None),
            P(None, "fsdp"),
            P("fsdp"),
            P(None, "fsdp"),
            P("fsdp", None),
            P("fsdp"),
            P(),
        ),
        check_vma=False,
    )
```

```python
import functools
import math

import jax
import jax.numpy as jnp
from jax import lax
from jax.experimental import pallas as pl
from jax.experimental.pallas import tpu as pltpu
from jax.sharding import PartitionSpec as P

HEAD_DIM = 64
EPSILON = 1e-12
NEGATIVE = -1000000000.0
BF = jnp.bfloat16
F32 = jnp.float32
AXES = ("dp", "fsdp")
LOG2E = 1.0 / math.log(2.0)
SCALE = 1.0 / math.sqrt(HEAD_DIM)
TILE = 256
PAIR = 2 * HEAD_DIM


def dot_nt(left, right, precision=None):
    return lax.dot_general(
        left, right, (((1,), (1,)), ((), ())), precision=precision, preferred_element_type=F32
    )


def dot_nn(left, right):
    return jnp.dot(left, right, preferred_element_type=F32)


def dot_tn(left, right):
    return lax.dot_general(left, right, (((0,), (0,)), ((), ())), preferred_element_type=F32)


def resident(shape, *index):
    index = index or (0,) * len(shape)
    return pl.BlockSpec(shape, lambda *_: index)


def call(kernel, name, flops, bytes_moved, **kwargs):
    cost = pl.CostEstimate(flops=flops, bytes_accessed=bytes_moved, transcendentals=0)
    return pl.pallas_call(kernel, name=name, cost_estimate=cost, **kwargs)


SMEM = pl.BlockSpec(memory_space=pltpu.SMEM)


def project_kernel(table_ref, bias_ref, token_ref, *refs, starts, size):
    pieces, (out_ref, rows_ref) = refs[:-2], refs[-2:]

    @pl.when(pl.program_id(0) == 0)
    def _():
        for piece, start in zip(pieces, starts):
            for i in range(piece.shape[0] // size):
                there = pl.multiple_of(table_ref[start + i] * size, size)
                rows_ref[pl.ds(there, size), :] = piece[i * size : (i + 1) * size, :]

    width = token_ref.shape[1]
    for j in range(3):
        part = dot_nt(token_ref[...], rows_ref[j * width : (j + 1) * width, :])
        if j == 0:
            part = part + bias_ref[0:1, :]
        if j == 2:
            part = part + bias_ref[1:2, :]
        out_ref[j] = part.astype(BF)


def project(tokens, bias, table, pieces, starts, size):
    count, width = tokens.shape
    total = sum(piece.shape[0] for piece in pieces)
    return call(
        functools.partial(project_kernel, starts=starts, size=size),
        "project",
        2 * count * width * 3 * width,
        2 * (4 * count * width + 2 * total * width),
        grid=(count // TILE,),
        in_specs=[SMEM, resident(bias.shape), pl.BlockSpec((TILE, width), lambda t: (t, 0))]
        + [resident(piece.shape) for piece in pieces],
        out_specs=[
            pl.BlockSpec((3, TILE, width), lambda t: (0, t, 0)),
            resident((total, width)),
        ],
        out_shape=[
            jax.ShapeDtypeStruct((3, count, width), BF),
            jax.ShapeDtypeStruct((total, width), BF),
        ],
    )(table, bias, tokens, *pieces)


def head_lanes(values, head):
    lane = lax.broadcasted_iota(jnp.int32, values.shape, 1)
    return jnp.where((lane >= HEAD_DIM) == (head == 1), values, jnp.zeros_like(values))


def scores_of(keys, queries, length, head):
    live = lax.broadcasted_iota(jnp.int32, (keys.shape[0], 1), 0) < length
    factor = jnp.where(live, SCALE * LOG2E, 0.0)
    shift = jnp.where(live, 0.0, NEGATIVE * LOG2E)
    return dot_nt(keys, head_lanes(queries, head)) * factor + shift


def pairs_per_step(pairs):
    return 3 if pairs % 3 == 0 else 1


def attend_kernel(length_ref, q_ref, k_ref, v_ref, out_ref, log_ref):
    length = length_ref[pl.program_id(0)]
    for i in range(log_ref.shape[1]):
        span = slice(i * PAIR, (i + 1) * PAIR)
        keys, values_t = k_ref[0, :, span], v_ref[0, :, span].T
        halves = []
        for head in range(2):
            scores = scores_of(keys, q_ref[0, :, span], length, head)
            peak = jnp.max(scores, axis=0, keepdims=True)
            weights = jnp.exp2(scores - peak)
            total = jnp.sum(weights, axis=0, keepdims=True)
            part = dot_nn(values_t[head * HEAD_DIM : (head + 1) * HEAD_DIM, :], weights.astype(BF))
            halves.append(part * (1.0 / total))
            log_ref[0, i, head : head + 1, :] = peak + jnp.log2(total)
        out_ref[:, span] = jnp.concatenate(halves, axis=0).T.astype(BF)


def attend(projected, lengths, positions):
    _, count, width = projected.shape
    rows, pairs = count // positions, width // PAIR
    group = pairs_per_step(pairs)
    block = (1, positions, group * PAIR)
    flops = 4 * rows * pairs * 2 * positions * positions * HEAD_DIM
    return call(
        attend_kernel,
        "attend",
        2 * flops,
        8 * count * width,
        grid_spec=pltpu.PrefetchScalarGridSpec(
            num_scalar_prefetch=1,
            grid=(rows, pairs // group),
            in_specs=[pl.BlockSpec(block, lambda r, p, _, j=j: (j, r, p)) for j in range(3)],
            out_specs=[
                pl.BlockSpec((positions, group * PAIR), lambda r, p, _: (r, p)),
                pl.BlockSpec((1, group, 2, positions), lambda r, p, _: (r, p, 0, 0)),
            ],
        ),
        out_shape=[
            jax.ShapeDtypeStruct((count, width), BF),
            jax.ShapeDtypeStruct((rows, pairs, 2, positions), F32),
        ],
    )(lengths, projected, projected, projected)


def attend_back_kernel(
    length_ref, _, q_ref, k_ref, v_ref, grad_ref, ctx_ref, log_ref, out_ref, sum_ref
):
    length = length_ref[pl.program_id(0)]
    row = lax.broadcasted_iota(jnp.int32, (8, PAIR), 0)
    lane = lax.broadcasted_iota(jnp.int32, (8, PAIR), 1)
    chosen = jnp.where((lane >= HEAD_DIM) == (row == 1), 1.0, 0.0).astype(BF)
    for i in range(log_ref.shape[1]):
        span = slice(i * PAIR, (i + 1) * PAIR)
        queries, keys, values, grad = q_ref[0, :, span], k_ref[0, :, span], v_ref[0, :, span], grad_ref[:, span]
        product = grad.astype(F32) * ctx_ref[:, span].astype(F32)
        high = product.astype(BF)
        low = (product - high.astype(F32)).astype(BF)
        row_totals = dot_nt(chosen, high) + dot_nt(chosen, low)
        query_grad, key_grad, value_grad = 0.0, 0.0, 0.0
        for head in range(2):
            scores = scores_of(keys, queries, length, head)
            wide = jnp.exp2(scores - log_ref[0, i, head : head + 1, :])
            grad_head = head_lanes(grad, head)
            value_grad += dot_nn(wide.astype(BF), grad_head)
            weight_grad = dot_nt(values, grad_head)
            score_grad = (wide * (weight_grad - row_totals[head : head + 1, :])).astype(BF)
            key_grad += dot_nn(score_grad, head_lanes(queries, head))
            query_grad += dot_tn(score_grad, head_lanes(keys, head))
        query_low = (query_grad * SCALE).astype(BF)
        value_low = value_grad.astype(BF)
        out_ref[0, :, span] = query_low
        out_ref[1, :, span] = (key_grad * SCALE).astype(BF)
        out_ref[2, :, span] = value_low
        sum_ref[0, 0:1, span] = jnp.sum(query_low.astype(F32), axis=0, keepdims=True)
        sum_ref[0, 1:2, span] = jnp.sum(value_low.astype(F32), axis=0, keepdims=True)


def attend_back(projected, lengths, side, context_grad, context, logs, positions):
    _, count, width = projected.shape
    rows, pairs = count // positions, width // PAIR // 2
    group = pairs_per_step(pairs)
    steps = pairs // group
    block = (1, positions, group * PAIR)
    flat = pl.BlockSpec((positions, group * PAIR), lambda r, p, _, s: (r, s[0] * steps + p))
    flops = 10 * rows * pairs * 2 * positions * positions * HEAD_DIM
    return call(
        attend_back_kernel,
        "attend_back",
        2 * flops,
        8 * count * width,
        grid_spec=pltpu.PrefetchScalarGridSpec(
            num_scalar_prefetch=2,
            grid=(rows, steps),
            in_specs=[
                pl.BlockSpec(block, lambda r, p, _, s, j=j: (j, r, s[0] * steps + p)) for j in range(3)
            ]
            + [
                flat,
                flat,
                pl.BlockSpec((1, group, 2, positions), lambda r, p, _, s: (r, s[0] * steps + p, 0, 0)),
            ],
            out_specs=[
                pl.BlockSpec((3, positions, group * PAIR), lambda r, p, _, s: (0, r, p)),
                pl.BlockSpec((1, 2, group * PAIR), lambda r, p, _, s: (r, 0, p)),
            ],
        ),
        out_shape=[
            jax.ShapeDtypeStruct((3, count, width // 2), BF),
            jax.ShapeDtypeStruct((rows, 2, width // 2), F32),
        ],
    )(lengths, side, projected, projected, projected, context_grad, context, logs)


def normalize(residual):
    centered = residual - jnp.mean(residual, axis=-1, keepdims=True)
    inverse = lax.rsqrt(jnp.mean(centered * centered, axis=-1, keepdims=True) + EPSILON)
    return centered * inverse, inverse


def norm_back(upstream, normed, inverse, gain):
    scaled = upstream * gain
    mean_plain = jnp.mean(scaled, axis=-1, keepdims=True)
    mean_normed = jnp.mean(scaled * normed, axis=-1, keepdims=True)
    return inverse * (scaled - mean_plain - normed * mean_normed)


def live_tile(length_ref, positions, shape):
    first = pl.program_id(0) * TILE
    place = lax.broadcasted_iota(jnp.int32, shape, 0) + first % positions
    return place < length_ref[first // positions]


def add_rows(ref, rows):
    @pl.when(pl.program_id(0) == 0)
    def _():
        ref[...] = jnp.zeros_like(ref)

    for i, row in enumerate(rows):
        ref[i : i + 1, :] += jnp.sum(row, axis=0, keepdims=True)


def middle_kernel(length_ref, vec_ref, ctx_ref, weight_ref, token_ref, n_ref, s_ref, low_ref, sum_ref, *, positions):
    branch = dot_nt(ctx_ref[...], weight_ref[...]) + vec_ref[0:1, :]
    tokens = token_ref[...].astype(F32)
    normed, inverse = normalize(tokens + branch)
    n_ref[...] = normed
    s_ref[...] = jnp.broadcast_to(inverse, s_ref.shape)
    low_ref[...] = (normed * vec_ref[1:2, :] + vec_ref[2:3, :]).astype(BF)
    live = live_tile(length_ref, positions, tokens.shape)
    add_rows(sum_ref, [jnp.where(live, tokens * tokens, 0.0), jnp.where(live, branch * branch, 0.0)])


def tiles(width):
    return pl.BlockSpec((TILE, width), lambda t: (t, 0))


def middle(lengths, vectors, context, attn_rows, tokens, positions):
    count, width = tokens.shape
    return call(
        functools.partial(middle_kernel, positions=positions),
        "middle",
        2 * count * width * width,
        count * width * 12,
        grid=(count // TILE,),
        in_specs=[SMEM, resident(vectors.shape), tiles(width), resident((width, width), 3, 0), tiles(width)],
        out_specs=[tiles(width), tiles(128), tiles(width), resident((8, width))],
        out_shape=[
            jax.ShapeDtypeStruct((count, width), F32),
            jax.ShapeDtypeStruct((count, 128), F32),
            jax.ShapeDtypeStruct((count, width), BF),
            jax.ShapeDtypeStruct((8, width), F32),
        ],
    )(lengths, vectors, context, attn_rows, tokens)


def gelu_parts(inner):
    cumulative = 0.5 * (1.0 + lax.erf(inner * (1.0 / math.sqrt(2.0))))
    density = jnp.exp2(inner * inner * (-0.5 * LOG2E)) * (1.0 / math.sqrt(2.0 * math.pi))
    return inner * cumulative, cumulative + inner * density


def two_by_two(pieces):
    for first, second in zip(pieces[::2], pieces[1::2]):
        yield jnp.concatenate([first[...], second[...]], axis=0)


def expand_kernel(bias_ref, low_ref, *refs):
    pieces, (gelu_ref, slope_ref) = refs[:-2], refs[-2:]
    low, at = low_ref[...], 0
    for piece in two_by_two(pieces):
        size = piece.shape[0]
        inner = dot_nt(low, piece) + bias_ref[0:1, at : at + size]
        gelu, slope = gelu_parts(inner)
        gelu_ref[:, at : at + size] = gelu.astype(BF)
        slope_ref[:, at : at + size] = slope.astype(BF)
        at += size


def picked(piece, width):
    array, start, size = piece
    return pl.BlockSpec((size, width), lambda *_, at=start // size: (at, 0))


def expand_call(low, bias, pieces):
    count, width = low.shape
    hidden = bias.shape[1]
    return call(
        expand_kernel,
        "expand_gelu",
        2 * count * width * hidden,
        count * hidden * 4,
        grid=(count // TILE,),
        in_specs=[resident(bias.shape), tiles(width)] + [picked(piece, width) for piece in pieces],
        out_specs=[tiles(hidden), tiles(hidden)],
        out_shape=[jax.ShapeDtypeStruct((count, hidden), BF)] * 2,
    )(bias, low, *[piece[0] for piece in pieces])


def contract_kernel(length_ref, vec_ref, gelu_ref, n_ref, cot_ref, *refs, positions):
    pieces, (out_ref, grad_ref, low_ref, sum_ref) = refs[:-4], refs[-4:]
    branch, at = vec_ref[3:4, :], 0
    for piece in two_by_two(pieces):
        size = piece.shape[0]
        branch = branch + dot_nn(gelu_ref[:, at : at + size], piece)
        at += size
    first = n_ref[...] * vec_ref[1:2, :] + vec_ref[2:3, :]
    normed, inverse = normalize(first + branch)
    out_ref[...] = (normed * vec_ref[4:5, :] + vec_ref[5:6, :]).astype(BF)
    upstream = cot_ref[...].astype(F32)
    grad = norm_back(upstream, normed, inverse, vec_ref[4:5, :])
    low = grad.astype(BF)
    grad_ref[...] = grad
    low_ref[...] = low
    live = live_tile(length_ref, positions, branch.shape)
    add_rows(
        sum_ref, [jnp.where(live, branch * branch, 0.0), low.astype(F32), upstream * normed, upstream]
    )


def contract_call(lengths, vectors, gelu, normed, cotangent, pieces, positions):
    count, width = cotangent.shape
    hidden = gelu.shape[1]
    return call(
        functools.partial(contract_kernel, positions=positions),
        "contract_norm",
        2 * count * width * hidden,
        count * hidden * 2 + count * width * 14,
        grid=(count // TILE,),
        in_specs=[SMEM, resident(vectors.shape), tiles(hidden), tiles(width), tiles(width)]
        + [picked(piece, width) for piece in pieces],
        out_specs=[tiles(width), tiles(width), tiles(width), resident((8, width))],
        out_shape=[
            jax.ShapeDtypeStruct((count, width), BF),
            jax.ShapeDtypeStruct((count, width), F32),
            jax.ShapeDtypeStruct((count, width), BF),
            jax.ShapeDtypeStruct((8, width), F32),
        ],
    )(lengths, vectors, gelu, normed, cotangent, *[piece[0] for piece in pieces])


def inner_kernel(low_ref, slope_ref, grad_ref, *refs, count):
    contracts, expands, (inner_ref, out_ref, sum_ref) = refs[:count], refs[count : 2 * count], refs[2 * count :]

    @pl.when(pl.program_id(0) == 0)
    def _():
        sum_ref[...] = jnp.zeros_like(sum_ref)

    low, total, at = low_ref[...], grad_ref[...], 0
    for contract, expand in zip(two_by_two(contracts), two_by_two(expands)):
        span = slice(at, at + contract.shape[0])
        inner = (dot_nt(low, contract) * slope_ref[:, span].astype(F32)).astype(BF)
        inner_ref[:, span] = inner
        sum_ref[0:1, span] += jnp.sum(inner.astype(F32), axis=0, keepdims=True)
        total = total + dot_nn(inner, expand)
        at += contract.shape[0]
    out_ref[...] = total


def inner_back(low, slope, grad, contracts, expands):
    count, width = low.shape
    hidden = slope.shape[1]
    return call(
        functools.partial(inner_kernel, count=len(contracts)),
        "inner_back",
        4 * count * width * hidden,
        count * hidden * 4 + count * width * 10,
        grid=(count // TILE,),
        in_specs=[tiles(width), tiles(hidden), tiles(width)]
        + [picked(piece, width) for piece in contracts + expands],
        out_specs=[tiles(hidden), tiles(width), resident((8, hidden))],
        out_shape=[
            jax.ShapeDtypeStruct((count, hidden), BF),
            jax.ShapeDtypeStruct((count, width), F32),
            jax.ShapeDtypeStruct((8, hidden), F32),
        ],
    )(low, slope, grad, *[piece[0] for piece in contracts + expands])


def feed_weights_kernel(left_ref, right_ref, out_ref):
    out_ref[...] = dot_tn(left_ref[...], right_ref[...]).astype(BF)


def feed_weights(left, right, half):
    count, width = right.shape
    rows = left.shape[1] // 2
    size = rows // 2
    return call(
        feed_weights_kernel,
        "feed_weights",
        2 * count * width * rows,
        count * rows * 2 + rows * width * 2,
        grid=(2,),
        in_specs=[pl.BlockSpec((count, size), lambda i: (0, half * 2 + i)), resident((count, width))],
        out_specs=pl.BlockSpec((size, width), lambda i: (i, 0)),
        out_shape=jax.ShapeDtypeStruct((rows, width), BF),
    )(left, right)


def middle_back_kernel(vec_ref, hid_ref, n_ref, s_ref, weight_ref, grad_ref, low_ref, ctx_ref, sum_ref):
    upstream, normed = hid_ref[...], n_ref[...]
    grad = norm_back(upstream, normed, s_ref[:, 0:1], vec_ref[1:2, :])
    low = grad.astype(BF)
    grad_ref[...] = grad
    low_ref[...] = low
    ctx_ref[...] = dot_nn(low, weight_ref[...]).astype(BF)
    add_rows(sum_ref, [low.astype(F32), upstream * normed, upstream])


def middle_back(vectors, hidden_grad, normed, inverse, attn_rows):
    count, width = hidden_grad.shape
    return call(
        middle_back_kernel,
        "middle_back",
        2 * count * width * width,
        count * width * 16,
        grid=(count // TILE,),
        in_specs=[resident(vectors.shape), tiles(width), tiles(width), tiles(128), resident((width, width), 3, 0)],
        out_specs=[tiles(width), tiles(width), tiles(width), resident((8, width))],
        out_shape=[
            jax.ShapeDtypeStruct((count, width), F32),
            jax.ShapeDtypeStruct((count, width), BF),
            jax.ShapeDtypeStruct((count, width), BF),
            jax.ShapeDtypeStruct((8, width), F32),
        ],
    )(vectors, hidden_grad, normed, inverse, attn_rows)


def attn_weights_kernel(table_ref, qkv_ref, low_ref, token_ref, ctx_ref, out_ref, *, quarters):
    def put(result):
        size = result.shape[0] // quarters
        for d in range(quarters):
            out_ref[d ^ table_ref[1], 0] = result[d * size : (d + 1) * size, :]

    @pl.when(pl.program_id(0) < 3)
    def _():
        put(dot_tn(qkv_ref[0], token_ref[...]).astype(BF))

    @pl.when(pl.program_id(0) == 3)
    def _():
        put(dot_tn(low_ref[...], ctx_ref[...]).astype(BF))


def attn_weights(table, qkv_grad, out_grad, tokens, context):
    count, width = tokens.shape
    half = width // 2
    return call(
        functools.partial(attn_weights_kernel, quarters=4),
        "attn_weights",
        4 * 2 * count * width * half,
        count * width * 8 + width * width * 4,
        grid_spec=pltpu.PrefetchScalarGridSpec(
            num_scalar_prefetch=1,
            grid=(4,),
            in_specs=[
                pl.BlockSpec((1, count, half), lambda i, t: (jnp.minimum(i, 2), 0, 0)),
                pl.BlockSpec((count, half), lambda i, t: (0, t[0])),
                resident((count, width)),
                resident((count, width)),
            ],
            out_specs=pl.BlockSpec((4, 1, half // 4, width), lambda i, t: (0, i ^ t[2], 0, 0)),
        ),
        out_shape=jax.ShapeDtypeStruct((4, 4, half // 4, width), BF),
    )(table, qkv_grad, out_grad, tokens, context)


def input_kernel(core_ref, near_ref, far_ref, weight_ref, grad_ref, out_ref):
    width = out_ref.shape[1]
    near_first = core_ref[0] == 0
    total = grad_ref[...]
    for j in range(3):
        near, far = near_ref[j], far_ref[j]
        whole = jnp.concatenate([jnp.where(near_first, near, far), jnp.where(near_first, far, near)], axis=1)
        total = total + dot_nn(whole, weight_ref[j * width : (j + 1) * width, :])
    out_ref[...] = total.astype(BF)


def input_back(core, near, far, attn_rows, grad):
    count, width = grad.shape
    half = pl.BlockSpec((3, TILE, width // 2), lambda t: (0, t, 0))
    return call(
        input_kernel,
        "input_back",
        6 * count * width * width,
        count * width * 12 + width * width * 6,
        grid=(count // TILE,),
        in_specs=[SMEM, half, half, resident((3 * width, width)), tiles(width)],
        out_specs=tiles(width),
        out_shape=jax.ShapeDtypeStruct((count, width), BF),
    )(core, near, far, attn_rows, grad)


def pack_kernel(place_ref, length_ref, near_ref, far_ref, one_ref, inner_ref, two_ref, middle_ref, out_ref):
    half = near_ref.shape[2]
    near_first = place_ref[32] == 0
    near, far = (jnp.sum(ref[...], axis=0) for ref in (near_ref, far_ref))
    first, second = jnp.where(near_first, near, far), jnp.where(near_first, far, near)
    both = jnp.concatenate([first, second], axis=1)
    rows = [both[0:1, :], both[1:2, :]] + [one_ref[i : i + 1, :] for i in range(3)]
    rows += [two_ref[i : i + 1, :] for i in (1, 2, 3)]
    at = 0
    for row in rows:
        for lane in range(0, 2 * half, 128):
            out_ref[at : at + 1, :] = row[:, lane : lane + 128]
            at += 1
    size = inner_ref.shape[1] // 32
    gap = jnp.zeros((1, 128 - size), F32)
    for i in range(32):
        part = jnp.concatenate([inner_ref[0:1, i * size : (i + 1) * size], gap], axis=1)
        out_ref[pl.ds(at + place_ref[i], 1), :] = part
    at += 32
    for row in (middle_ref[0:1, :], middle_ref[1:2, :], two_ref[0:1, :]):
        out_ref[at : at + 1, :] = sum(row[:, lane : lane + 128] for lane in range(0, 2 * half, 128))
        at += 1
    live = length_ref[0]
    for i in range(1, length_ref.shape[0]):
        live = live + length_ref[i]
    out_ref[at : at + 1, :] = jnp.full((1, 128), live).astype(F32)
    out_ref[at + 1 :, :] = jnp.zeros((out_ref.shape[0] - at - 1, 128), F32)


def pack(places, lengths, parts):
    width = parts[2].shape[1]
    rows = 8 * width // 128 + 32 + 8
    return call(
        pack_kernel,
        "pack",
        0,
        rows * 1024,
        in_specs=[SMEM, SMEM] + [resident(part.shape) for part in parts],
        out_specs=resident((rows, 128)),
        out_shape=jax.ShapeDtypeStruct((rows, 128), F32),
        grid=(1,),
    )(places, lengths, *parts)


def tie(*values):
    return lax.optimization_barrier(values)


def add(*parts):
    return sum(part.astype(F32) for part in parts)


class Links:
    def __init__(self):
        self.dp, self.fsdp = lax.axis_size("dp"), lax.axis_size("fsdp")
        self.paired = (self.dp, self.fsdp) == (4, 8)
        my_dp, my_fsdp = lax.axis_index("dp"), lax.axis_index("fsdp")
        if self.paired:
            self.my_dp, self.my_core, self.my_z = my_dp, my_fsdp & 1, my_fsdp >> 1
        else:
            zero = jnp.zeros((), jnp.int32)
            self.my_dp, self.my_core, self.my_z = zero, zero, zero
        self.my_fsdp = my_fsdp

    def swap(self, values, core=0, dp=0, z=0):
        mask = core + 2 * z + self.fsdp * dp
        pairs = [(i, i ^ mask) for i in range(self.dp * self.fsdp)]
        return lax.ppermute(values, AXES, pairs)

    def table(self):
        e = jnp.arange(2, dtype=jnp.int32)[:, None, None]
        m = jnp.arange(4, dtype=jnp.int32)[None, :, None]
        k = jnp.arange(4, dtype=jnp.int32)[None, None, :]
        if not self.paired:
            return jnp.arange(32, dtype=jnp.int32)
        e, m, k = e ^ self.my_core, m ^ self.my_dp, k ^ self.my_z
        return ((k * 2 + e) * 4 + m).reshape(-1).astype(jnp.int32)

    def flip(self, values, axis, index):
        shape = values.shape
        bits = shape[axis].bit_length() - 1
        split = values.reshape(shape[:axis] + (2,) * bits + shape[axis + 1 :])
        for i in range(bits):
            bit = (index >> (bits - 1 - i)) & 1
            split = jnp.where(bit == 1, jnp.flip(split, axis + i), split)
        return split.reshape(shape)

    def to_exchange(self, natural):
        if not self.paired:
            return natural
        moved = natural.transpose(1, 2, 0, 3)
        return self.flip(self.flip(self.flip(moved, 0, self.my_core), 1, self.my_dp), 2, self.my_z)

    def to_natural(self, exchanged):
        if not self.paired:
            return exchanged
        moved = self.flip(self.flip(self.flip(exchanged, 0, self.my_core), 1, self.my_dp), 2, self.my_z)
        return moved.transpose(2, 0, 1, 3)


def spread_z(links, mine):
    return [mine] + [links.swap(mine, z=k) for k in range(1, 4)]


def spread_plane(links, own):
    one, two = links.swap(own, dp=1), links.swap(own, dp=2)
    return one, two


def spread_corner(links, one, two):
    half = one.shape[0] // 2
    return links.swap(one[:half], dp=2), links.swap(two[half:], dp=1)


def gather_plain(attention, attvector, expand, contract, feedvector):
    def whole(shard):
        return lax.all_gather(shard, "fsdp", axis=0, tiled=True)

    rows = [whole(attention.T), whole(expand.T), whole(contract)]
    return rows, whole(attvector).astype(F32), whole(feedvector).astype(F32)


def corner_sum(near, got):
    start = near.shape[0] // 4 * 3
    return add(near[start:], got[start:]).astype(BF)


def send_corner(links, corner):
    half = corner.shape[0] // 2
    return links.swap(corner[:half], dp=2), links.swap(corner[half:], dp=1)


def side_sums(near, got, corners):
    block = near.shape[0] // 4
    half = block // 2
    one = add(near[block : 2 * block], got[block : 2 * block])
    two = add(near[2 * block : 3 * block], got[2 * block : 3 * block])
    one = jnp.concatenate([one[:half] + corners[0].astype(F32), one[half:]], axis=0)
    two = jnp.concatenate([two[:half], two[half:] + corners[1].astype(F32)], axis=0)
    return one.astype(BF), two.astype(BF)


def send_sides(links, sides):
    return links.swap(sides[0], dp=1), links.swap(sides[1], dp=2)


def own_sum(near, got, sides):
    block = near.shape[0] // 4
    return add(near[:block], got[:block], *sides).astype(BF)


def send_z(links, summed):
    size = summed.shape[0] // 4
    return summed[:size], [links.swap(summed[k * size : (k + 1) * size], z=k) for k in range(1, 4)]


def send_share(links, final):
    return [final] + [links.swap(final, dp=m) for m in range(1, 4)]


def quarters(links, shares):
    return links.flip(jnp.stack(shares), 0, links.my_dp).reshape(-1, shares[0].shape[1]).astype(F32)


def per_device(tokens, attention, attvector, expand, contract, feedvector, lengths, cotangent):
    links = Links()
    width = tokens.shape[1]
    positions = tokens.shape[0] // lengths.shape[0]
    hidden = expand.shape[1] * links.fsdp
    att_len, feed_len = attvector.shape[0], feedvector.shape[0]
    size = width // 8
    quad = 4 * size

    if links.paired:
        vectors = jnp.concatenate([attvector, feedvector])
        extra = jnp.pad(vectors, (0, 16 * width - vectors.shape[0])).reshape(16, width)

        def quarter(shard):
            return lax.dynamic_slice_in_dim(shard, links.my_dp * size, size, 0)

        attn_z = spread_z(links, jnp.concatenate([quarter(attention.T), extra], axis=0))
        feed_mine = jnp.concatenate([quarter(expand.T), quarter(contract)], axis=0)
        feed_mine, *attn_z = tie(feed_mine, *attn_z)
        attn_own = jnp.concatenate([part[:size] for part in attn_z], axis=0)
        extras = jnp.concatenate([part[size:] for part in attn_z], axis=0)
        attn_one, attn_two = spread_plane(links, attn_own)
        feed_z = spread_z(links, feed_mine)
        extras = jnp.stack([extras, links.swap(extras, core=1)])
        extras = extras.reshape(2, 1, 4, 16 * width)[..., : vectors.shape[0]]
        extras = links.flip(links.flip(extras, 0, links.my_core), 2, links.my_z)
        by_owner = extras.transpose(2, 0, 1, 3).reshape(links.fsdp, -1).astype(F32)
        attvec, feedvec = by_owner[:, :att_len].reshape(-1), by_owner[:, att_len:].reshape(-1)
    else:
        rows, attvec, feedvec = gather_plain(attention, attvector, expand, contract, feedvector)
        attn_pieces, attn_starts = [rows[0]], [0]
        expands = [(rows[1], i * quad, quad) for i in range(8)]
        contracts = [(rows[2], i * quad, quad) for i in range(8)]

    def row_of(vector, i, start=0):
        return vector[start + i * width : start + (i + 1) * width]

    project_bias = jnp.stack([row_of(attvec, 0), row_of(attvec, 1)])
    vec_rows = [row_of(attvec, i) for i in (2, 3, 4)] + [row_of(feedvec, i, hidden) for i in range(3)]
    vec_rows = jnp.stack(vec_rows + [jnp.zeros((width,), F32)] * 2)
    inner_bias = links.to_exchange(feedvec[:hidden].reshape(4, 2, 4, size)).reshape(1, hidden)

    if links.paired:
        attn_one, attn_two, project_bias, vec_rows, inner_bias = tie(
            attn_one, attn_two, project_bias, vec_rows, inner_bias
        )
        attn_three = spread_corner(links, attn_one, attn_two)
        attn_near = [attn_own, attn_one, attn_two, *attn_three]
        attn_far = [links.swap(part, core=1) for part in attn_near]
        attn_pieces = attn_near + attn_far
        attn_starts = [0, 4, 8, 12, 14, 16, 20, 24, 28, 30]
        feed_own = jnp.concatenate([part[:size] for part in feed_z] + [part[size:] for part in feed_z], axis=0)
        feed_own, *_ = tie(feed_own, *attn_three)
        feed_one, feed_two = spread_plane(links, feed_own)
        feed_far = [links.swap(feed_own, core=1)]

    projected, attn_rows = project(tokens, project_bias, links.table(), attn_pieces, attn_starts, size)
    context, logs = attend(projected, lengths, positions)
    if links.paired:
        context, feed_one, feed_two = tie(context, feed_one, feed_two)
        feed_three = spread_corner(links, feed_one, feed_two)
        feed_far += [links.swap(feed_one, core=1), links.swap(feed_two, core=1)]
    normed_one, inverse_one, hidden_low, sum_middle = middle(
        lengths, vec_rows, context, attn_rows, tokens, positions
    )
    if links.paired:
        hidden_low, *feed_three = tie(hidden_low, *feed_three)
        feed_near = [feed_own, feed_one, feed_two]
        far_three = [links.swap(part, core=1) for part in feed_three]
        expands = [(part, 0, quad) for part in feed_near] + [(feed_three[0], 0, quad)]
        expands += [(part, 0, quad) for part in feed_far] + [(far_three[0], 0, quad)]
        contracts = [(part, quad, quad) for part in feed_near] + [(feed_three[1], 0, quad)]
        contracts += [(part, quad, quad) for part in feed_far] + [(far_three[1], 0, quad)]
    gelu, slope = expand_call(hidden_low, inner_bias, expands)
    result, grad_two, grad_two_low, sum_two = contract_call(
        lengths, vec_rows, gelu, normed_one, cotangent, contracts, positions
    )
    tables = [
        jnp.stack([links.my_core ^ e, links.my_dp, links.my_z]).astype(jnp.int32) for e in range(2)
    ]
    places = jnp.concatenate([links.table(), tables[0]])

    cf = feed_weights(gelu, grad_two_low, 1)
    gelu, cf = tie(gelu, cf)
    cn = feed_weights(gelu, grad_two_low, 0)
    if links.paired:
        cg = links.swap(cf, core=1)
        corner = corner_sum(cn, cg)
        slope, corner = tie(slope, corner)
        c_in = send_corner(links, corner)
    else:
        slope, cn = tie(slope, cn)
    inner_grad, hidden_grad, sum_inner = inner_back(grad_two_low, slope, grad_two, contracts, expands)
    if links.paired:
        inner_grad, *c_in = tie(inner_grad, *c_in)
        inner_grad, *c_in = tie(inner_grad, *side_sums(cn, cg, c_in))
        c_in = send_sides(links, c_in)
    ef = feed_weights(inner_grad, hidden_low, 1)
    inner_grad, ef = tie(inner_grad, ef)
    en = feed_weights(inner_grad, hidden_low, 0)
    if links.paired:
        eg = links.swap(ef, core=1)
        hidden_grad, corner = tie(hidden_grad, corner_sum(en, eg))
        e_in = send_corner(links, corner)
    else:
        hidden_grad, en = tie(hidden_grad, en)
    grad_one, grad_one_low, context_grad, sum_one = middle_back(
        vec_rows, hidden_grad, normed_one, inverse_one, attn_rows
    )
    if links.paired:
        context_grad, *got = tie(context_grad, *e_in, *c_in)
        context_grad, c_own, *e_in = tie(
            context_grad, own_sum(cn, cg, got[2:]), *side_sums(en, eg, got[:2])
        )
        e_in = send_sides(links, e_in)
        c_own, c_in = send_z(links, c_own)
    qkv_far, sum_far = attend_back(projected, lengths, tables[1][:1], context_grad, context, logs, positions)
    if links.paired:
        qkv_far, *got = tie(qkv_far, *e_in, *c_in)
        qkv_far, e_own, c_own = tie(
            qkv_far, own_sum(en, eg, got[:2]), add(c_own, *got[2:]).astype(BF)
        )
        c_in = send_share(links, c_own)
        e_own, e_in = send_z(links, e_own)
    af = attn_weights(tables[1], qkv_far, grad_one_low, tokens, context)
    context_grad, af = tie(context_grad, af)
    qkv_near, sum_near = attend_back(
        projected, lengths, tables[0][:1], context_grad, context, logs, positions
    )
    packed = pack(places, lengths, [sum_near, sum_far, sum_one, sum_inner, sum_two, sum_middle])
    if links.paired:
        qkv_near, *e_in = tie(qkv_near, *e_in)
        qkv_near, e_own, packed = tie(qkv_near, add(e_own, *e_in).astype(BF), packed)
        e_in = send_share(links, e_own)
        packed_in = links.swap(packed, core=1)
    an = attn_weights(tables[0], qkv_near, grad_one_low, tokens, context)
    if links.paired:
        an, af = an.reshape(-1, width), af.reshape(-1, width)
        ag = links.swap(af, core=1)
        an, packed_in = tie(an, packed_in)
        qkv_near, corner, packed = tie(qkv_near, corner_sum(an, ag), packed + packed_in)
        a_in, packed_in = send_corner(links, corner), links.swap(packed, dp=1)
        qkv_near, packed, *a_in = tie(qkv_near, packed + packed_in, *side_sums(an, ag, a_in))
        a_in, packed_in = send_sides(links, a_in), links.swap(packed, dp=2)
        input_grad = input_back(tables[0][:1], qkv_near, qkv_far, attn_rows, grad_one)
        input_grad, packed_in, *a_in = tie(input_grad, packed_in, *a_in)
        input_grad, packed, a_own = tie(input_grad, packed + packed_in, own_sum(an, ag, a_in))
        packed_in = links.swap(packed, z=1)
        a_own, a_in = send_z(links, a_own)
        packed, a_own = tie(packed + packed_in, add(a_own, *a_in).astype(BF))
        packed = packed + links.swap(packed, z=2)
        attn_sum = quarters(links, send_share(links, a_own)).T
        expand_sum, contract_sum = quarters(links, e_in).T, quarters(links, c_in)
    else:
        input_grad = input_back(tables[0][:1], qkv_near, qkv_far, attn_rows, grad_one)

        def finish(natural):
            shard = lax.psum_scatter(natural, "fsdp", scatter_dimension=0, tiled=True)
            return lax.psum(shard, "dp").astype(F32)

        expand_sum = finish(jnp.concatenate([en, ef], axis=0)).T
        contract_sum = finish(jnp.concatenate([cn, cf], axis=0))
        attn_sum = finish(jnp.stack([an, af]).transpose(2, 0, 1, 3, 4).reshape(4 * width, width)).T
        packed = lax.psum(packed, AXES)

    att_rows = att_len * links.fsdp // 128
    inner_at = att_rows + (feed_len * links.fsdp - hidden) // 128
    att_sum = lax.dynamic_slice_in_dim(packed[:att_rows].reshape(-1), links.my_fsdp * att_len, att_len, 0)
    feed_flat = jnp.concatenate(
        [packed[inner_at : inner_at + 32, : hidden // 32].reshape(-1), packed[att_rows:inner_at].reshape(-1)]
    )
    feed_vec_sum = lax.dynamic_slice_in_dim(feed_flat, links.my_fsdp * feed_len, feed_len, 0)
    squares = jnp.sum(packed[inner_at + 32 : inner_at + 35], axis=1)
    root_squares = jnp.sqrt(squares / (packed[inner_at + 35, 0] * width))
    return (result, input_grad, attn_sum, att_sum, expand_sum, contract_sum, feed_vec_sum, root_squares)


def solution(mesh):
    return jax.shard_map(
        per_device,
        mesh=mesh,
        in_specs=(
            P(AXES, None),
            P(None, "fsdp"),
            P("fsdp"),
            P(None, "fsdp"),
            P("fsdp", None),
            P("fsdp"),
            P(AXES),
            P(AXES, None),
        ),
        out_specs=(
            P(AXES, None),
            P(AXES, None),
            P(None, "fsdp"),
            P("fsdp"),
            P(None, "fsdp"),
            P("fsdp", None),
            P("fsdp"),
            P(),
        ),
        check_vma=False,
    )
```

```python
import functools
import math

import jax
import jax.numpy as jnp
from jax import lax
from jax.experimental import pallas as pl
from jax.experimental.pallas import tpu as pltpu
from jax.sharding import PartitionSpec as P

HEAD_DIM = 64
EPSILON = 1e-12
NEGATIVE = -1000000000.0
BF = jnp.bfloat16
F32 = jnp.float32
AXES = ("dp", "fsdp")
LOG2E = 1.0 / math.log(2.0)
SCALE = 1.0 / math.sqrt(HEAD_DIM)
TILE = 256
PAIR = 2 * HEAD_DIM


def dot_nt(left, right, precision=None):
    return lax.dot_general(
        left, right, (((1,), (1,)), ((), ())), precision=precision, preferred_element_type=F32
    )


def dot_nn(left, right):
    return jnp.dot(left, right, preferred_element_type=F32)


def dot_tn(left, right):
    return lax.dot_general(left, right, (((0,), (0,)), ((), ())), preferred_element_type=F32)


def resident(shape, *index):
    index = index or (0,) * len(shape)
    return pl.BlockSpec(shape, lambda *_: index)


def call(kernel, name, flops, bytes_moved, **kwargs):
    cost = pl.CostEstimate(flops=flops, bytes_accessed=bytes_moved, transcendentals=0)
    return pl.pallas_call(kernel, name=name, cost_estimate=cost, **kwargs)


SMEM = pl.BlockSpec(memory_space=pltpu.SMEM)


def project_kernel(table_ref, bias_ref, token_ref, *refs, starts, size):
    pieces, (out_ref, rows_ref) = refs[:-2], refs[-2:]

    @pl.when(pl.program_id(0) == 0)
    def _():
        for piece, start in zip(pieces, starts):
            for i in range(piece.shape[0] // size):
                there = pl.multiple_of(table_ref[start + i] * size, size)
                rows_ref[pl.ds(there, size), :] = piece[i * size : (i + 1) * size, :]

    width = token_ref.shape[1]
    for j in range(3):
        part = dot_nt(token_ref[...], rows_ref[j * width : (j + 1) * width, :])
        if j == 0:
            part = part + bias_ref[0:1, :]
        if j == 2:
            part = part + bias_ref[1:2, :]
        out_ref[j] = part.astype(BF)


def project(tokens, bias, table, pieces, starts, size):
    count, width = tokens.shape
    total = sum(piece.shape[0] for piece in pieces)
    return call(
        functools.partial(project_kernel, starts=starts, size=size),
        "project",
        2 * count * width * 3 * width,
        2 * (4 * count * width + 2 * total * width),
        grid=(count // TILE,),
        in_specs=[SMEM, resident(bias.shape), pl.BlockSpec((TILE, width), lambda t: (t, 0))]
        + [resident(piece.shape) for piece in pieces],
        out_specs=[
            pl.BlockSpec((3, TILE, width), lambda t: (0, t, 0)),
            resident((total, width)),
        ],
        out_shape=[
            jax.ShapeDtypeStruct((3, count, width), BF),
            jax.ShapeDtypeStruct((total, width), BF),
        ],
    )(table, bias, tokens, *pieces)


def head_lanes(values, head):
    lane = lax.broadcasted_iota(jnp.int32, values.shape, 1)
    return jnp.where((lane >= HEAD_DIM) == (head == 1), values, jnp.zeros_like(values))


def scores_of(keys, queries, length, head):
    live = lax.broadcasted_iota(jnp.int32, (keys.shape[0], 1), 0) < length
    factor = jnp.where(live, SCALE * LOG2E, 0.0)
    shift = jnp.where(live, 0.0, NEGATIVE * LOG2E)
    return dot_nt(keys, head_lanes(queries, head)) * factor + shift


def pairs_per_step(pairs):
    return 2 if pairs % 2 == 0 else 1


def attend_kernel(length_ref, q_ref, k_ref, v_ref, out_ref, log_ref):
    length = length_ref[pl.program_id(0)]
    for i in range(log_ref.shape[1]):
        span = slice(i * PAIR, (i + 1) * PAIR)
        keys, values_t = k_ref[0, :, span], v_ref[0, :, span].T
        halves = []
        for head in range(2):
            scores = scores_of(keys, q_ref[0, :, span], length, head)
            peak = jnp.max(scores, axis=0, keepdims=True)
            weights = jnp.exp2(scores - peak)
            total = jnp.sum(weights, axis=0, keepdims=True)
            part = dot_nn(values_t[head * HEAD_DIM : (head + 1) * HEAD_DIM, :], weights.astype(BF))
            halves.append(part * (1.0 / total))
            log_ref[0, i, head : head + 1, :] = peak + jnp.log2(total)
        out_ref[:, span] = jnp.concatenate(halves, axis=0).T.astype(BF)


def attend(projected, lengths, positions):
    _, count, width = projected.shape
    rows, pairs = count // positions, width // PAIR
    group = pairs_per_step(pairs)
    block = (1, positions, group * PAIR)
    flops = 4 * rows * pairs * 2 * positions * positions * HEAD_DIM
    return call(
        attend_kernel,
        "attend",
        2 * flops,
        8 * count * width,
        grid_spec=pltpu.PrefetchScalarGridSpec(
            num_scalar_prefetch=1,
            grid=(rows, pairs // group),
            in_specs=[pl.BlockSpec(block, lambda r, p, _, j=j: (j, r, p)) for j in range(3)],
            out_specs=[
                pl.BlockSpec((positions, group * PAIR), lambda r, p, _: (r, p)),
                pl.BlockSpec((1, group, 2, positions), lambda r, p, _: (r, p, 0, 0)),
            ],
        ),
        out_shape=[
            jax.ShapeDtypeStruct((count, width), BF),
            jax.ShapeDtypeStruct((rows, pairs, 2, positions), F32),
        ],
    )(lengths, projected, projected, projected)


def attend_back_kernel(
    length_ref, q_ref, k_ref, v_ref, grad_ref, ctx_ref, log_ref, out_ref, sum_ref
):
    length = length_ref[pl.program_id(0)]
    row = lax.broadcasted_iota(jnp.int32, (8, PAIR), 0)
    lane = lax.broadcasted_iota(jnp.int32, (8, PAIR), 1)
    chosen = jnp.where((lane >= HEAD_DIM) == (row == 1), 1.0, 0.0).astype(BF)
    for i in range(log_ref.shape[1]):
        span = slice(i * PAIR, (i + 1) * PAIR)
        queries, keys, values, grad = q_ref[0, :, span], k_ref[0, :, span], v_ref[0, :, span], grad_ref[:, span]
        product = grad.astype(F32) * ctx_ref[:, span].astype(F32)
        high = product.astype(BF)
        low = (product - high.astype(F32)).astype(BF)
        row_totals = dot_nt(chosen, high) + dot_nt(chosen, low)
        query_grad, key_grad, value_grad = 0.0, 0.0, 0.0
        for head in range(2):
            scores = scores_of(keys, queries, length, head)
            wide = jnp.exp2(scores - log_ref[0, i, head : head + 1, :])
            grad_head = head_lanes(grad, head)
            value_grad += dot_nn(wide.astype(BF), grad_head)
            weight_grad = dot_nt(values, grad_head)
            score_grad = (wide * (weight_grad - row_totals[head : head + 1, :])).astype(BF)
            key_grad += dot_nn(score_grad, head_lanes(queries, head))
            query_grad += dot_tn(score_grad, head_lanes(keys, head))
        query_low = (query_grad * SCALE).astype(BF)
        value_low = value_grad.astype(BF)
        out_ref[0, :, span] = query_low
        out_ref[1, :, span] = (key_grad * SCALE).astype(BF)
        out_ref[2, :, span] = value_low
        sum_ref[0, 0:1, span] = jnp.sum(query_low.astype(F32), axis=0, keepdims=True)
        sum_ref[0, 1:2, span] = jnp.sum(value_low.astype(F32), axis=0, keepdims=True)


def attend_back(projected, lengths, context_grad, context, logs, positions):
    _, count, width = projected.shape
    rows, pairs = count // positions, width // PAIR
    group = pairs_per_step(pairs)
    block = (1, positions, group * PAIR)
    flat = pl.BlockSpec((positions, group * PAIR), lambda r, p, _: (r, p))
    flops = 10 * rows * pairs * 2 * positions * positions * HEAD_DIM
    return call(
        attend_back_kernel,
        "attend_back",
        2 * flops,
        16 * count * width,
        grid_spec=pltpu.PrefetchScalarGridSpec(
            num_scalar_prefetch=1,
            grid=(rows, pairs // group),
            in_specs=[pl.BlockSpec(block, lambda r, p, _, j=j: (j, r, p)) for j in range(3)]
            + [flat, flat, pl.BlockSpec((1, group, 2, positions), lambda r, p, _: (r, p, 0, 0))],
            out_specs=[
                pl.BlockSpec((3, positions, group * PAIR), lambda r, p, _: (0, r, p)),
                pl.BlockSpec((1, 2, group * PAIR), lambda r, p, _: (r, 0, p)),
            ],
        ),
        out_shape=[
            jax.ShapeDtypeStruct((3, count, width), BF),
            jax.ShapeDtypeStruct((rows, 2, width), F32),
        ],
    )(lengths, projected, projected, projected, context_grad, context, logs)


def normalize(residual):
    centered = residual - jnp.mean(residual, axis=-1, keepdims=True)
    inverse = lax.rsqrt(jnp.mean(centered * centered, axis=-1, keepdims=True) + EPSILON)
    return centered * inverse, inverse


def norm_back(upstream, normed, inverse, gain):
    scaled = upstream * gain
    mean_plain = jnp.mean(scaled, axis=-1, keepdims=True)
    mean_normed = jnp.mean(scaled * normed, axis=-1, keepdims=True)
    return inverse * (scaled - mean_plain - normed * mean_normed)


def live_tile(length_ref, positions, shape):
    first = pl.program_id(0) * TILE
    place = lax.broadcasted_iota(jnp.int32, shape, 0) + first % positions
    return place < length_ref[first // positions]


def add_rows(ref, rows):
    @pl.when(pl.program_id(0) == 0)
    def _():
        ref[...] = jnp.zeros_like(ref)

    for i, row in enumerate(rows):
        ref[i : i + 1, :] += jnp.sum(row, axis=0, keepdims=True)


def middle_kernel(length_ref, vec_ref, ctx_ref, weight_ref, token_ref, n_ref, s_ref, low_ref, sum_ref, *, positions):
    branch = dot_nt(ctx_ref[...], weight_ref[...]) + vec_ref[0:1, :]
    tokens = token_ref[...].astype(F32)
    normed, inverse = normalize(tokens + branch)
    n_ref[...] = normed
    s_ref[...] = jnp.broadcast_to(inverse, s_ref.shape)
    low_ref[...] = (normed * vec_ref[1:2, :] + vec_ref[2:3, :]).astype(BF)
    live = live_tile(length_ref, positions, tokens.shape)
    add_rows(sum_ref, [jnp.where(live, tokens * tokens, 0.0), jnp.where(live, branch * branch, 0.0)])


def tiles(width):
    return pl.BlockSpec((TILE, width), lambda t: (t, 0))


def middle(lengths, vectors, context, attn_rows, tokens, positions):
    count, width = tokens.shape
    return call(
        functools.partial(middle_kernel, positions=positions),
        "middle",
        2 * count * width * width,
        count * width * 12,
        grid=(count // TILE,),
        in_specs=[SMEM, resident(vectors.shape), tiles(width), resident((width, width), 3, 0), tiles(width)],
        out_specs=[tiles(width), tiles(128), tiles(width), resident((8, width))],
        out_shape=[
            jax.ShapeDtypeStruct((count, width), F32),
            jax.ShapeDtypeStruct((count, 128), F32),
            jax.ShapeDtypeStruct((count, width), BF),
            jax.ShapeDtypeStruct((8, width), F32),
        ],
    )(lengths, vectors, context, attn_rows, tokens)


def gelu_parts(inner):
    cumulative = 0.5 * (1.0 + lax.erf(inner * (1.0 / math.sqrt(2.0))))
    density = jnp.exp2(inner * inner * (-0.5 * LOG2E)) * (1.0 / math.sqrt(2.0 * math.pi))
    return inner * cumulative, cumulative + inner * density


def two_by_two(pieces):
    for first, second in zip(pieces[::2], pieces[1::2]):
        yield jnp.concatenate([first[...], second[...]], axis=0)


def expand_kernel(bias_ref, low_ref, *refs, groups):
    pieces, (gelu_ref, slope_ref) = refs[:-2], refs[-2:]
    low = low_ref[...]
    for first, last, at in groups:
        weights = jnp.concatenate([piece[...] for piece in pieces[first:last]], axis=0)
        span = slice(at, at + weights.shape[0])
        gelu, slope = gelu_parts(dot_nt(low, weights) + bias_ref[0:1, span])
        gelu_ref[:, span] = gelu.astype(BF)
        slope_ref[:, span] = slope.astype(BF)


def expand_last_kernel(bias_ref, low_ref, near_ref, far_ref, _, __, gelu_ref, slope_ref):
    weights = jnp.where(pl.program_id(1) == 0, near_ref[...], far_ref[...])
    gelu, slope = gelu_parts(dot_nt(low_ref[...], weights) + bias_ref[...])
    gelu_ref[...] = gelu.astype(BF)
    slope_ref[...] = slope.astype(BF)


def picked(piece, width):
    array, start, size = piece
    return pl.BlockSpec((size, width), lambda *_, at=start // size: (at, 0))


def expand_call(low, bias, pieces, groups):
    count, width = low.shape
    hidden = bias.shape[1]
    done = sum(piece[2] for piece in pieces)
    return call(
        functools.partial(expand_kernel, groups=groups),
        "expand_gelu",
        2 * count * width * done,
        count * hidden * 4,
        grid=(count // TILE,),
        in_specs=[resident(bias.shape), tiles(width)] + [picked(piece, width) for piece in pieces],
        out_specs=[tiles(hidden), tiles(hidden)],
        out_shape=[jax.ShapeDtypeStruct((count, hidden), BF)] * 2,
    )(bias, low, *[piece[0] for piece in pieces])


def expand_last(low, bias, pieces, gelu, slope):
    count, width = low.shape
    size = pieces[0][2]
    tall = count // 2
    spot = pl.BlockSpec((tall, size), lambda t, e: (t, 4 * e + 3))
    anywhere = pl.BlockSpec(memory_space=pl.ANY)
    return call(
        expand_last_kernel,
        "expand_last",
        4 * count * width * size,
        count * size * 8,
        grid=(2, 2),
        in_specs=[
            pl.BlockSpec((1, size), lambda t, e: (0, 4 * e + 3)),
            pl.BlockSpec((tall, width), lambda t, e: (t, 0)),
        ]
        + [picked(piece, width) for piece in pieces]
        + [anywhere, anywhere],
        out_specs=[spot, spot],
        out_shape=[jax.ShapeDtypeStruct(gelu.shape, BF)] * 2,
        input_output_aliases={4: 0, 5: 1},
    )(bias, low, *[piece[0] for piece in pieces], gelu, slope)


def contract_kernel(length_ref, vec_ref, gelu_ref, n_ref, cot_ref, *refs, positions):
    pieces, (out_ref, grad_ref, low_ref, sum_ref) = refs[:-4], refs[-4:]
    branch, at = vec_ref[3:4, :], 0
    for piece in two_by_two(pieces):
        size = piece.shape[0]
        branch = branch + dot_nn(gelu_ref[:, at : at + size], piece)
        at += size
    first = n_ref[...] * vec_ref[1:2, :] + vec_ref[2:3, :]
    normed, inverse = normalize(first + branch)
    out_ref[...] = (normed * vec_ref[4:5, :] + vec_ref[5:6, :]).astype(BF)
    upstream = cot_ref[...].astype(F32)
    grad = norm_back(upstream, normed, inverse, vec_ref[4:5, :])
    low = grad.astype(BF)
    grad_ref[...] = grad
    low_ref[...] = low
    live = live_tile(length_ref, positions, branch.shape)
    add_rows(
        sum_ref, [jnp.where(live, branch * branch, 0.0), low.astype(F32), upstream * normed, upstream]
    )


def contract_call(lengths, vectors, gelu, normed, cotangent, pieces, positions):
    count, width = cotangent.shape
    hidden = gelu.shape[1]
    return call(
        functools.partial(contract_kernel, positions=positions),
        "contract_norm",
        2 * count * width * hidden,
        count * hidden * 2 + count * width * 14,
        grid=(count // TILE,),
        in_specs=[SMEM, resident(vectors.shape), tiles(hidden), tiles(width), tiles(width)]
        + [picked(piece, width) for piece in pieces],
        out_specs=[tiles(width), tiles(width), tiles(width), resident((8, width))],
        out_shape=[
            jax.ShapeDtypeStruct((count, width), BF),
            jax.ShapeDtypeStruct((count, width), F32),
            jax.ShapeDtypeStruct((count, width), BF),
            jax.ShapeDtypeStruct((8, width), F32),
        ],
    )(lengths, vectors, gelu, normed, cotangent, *[piece[0] for piece in pieces])


def inner_kernel(low_ref, slope_ref, grad_ref, *refs, count):
    contracts, expands, (inner_ref, out_ref, sum_ref) = refs[:count], refs[count : 2 * count], refs[2 * count :]

    @pl.when(pl.program_id(0) == 0)
    def _():
        sum_ref[...] = jnp.zeros_like(sum_ref)

    low, total, at = low_ref[...], grad_ref[...], 0
    for contract, expand in zip(two_by_two(contracts), two_by_two(expands)):
        span = slice(at, at + contract.shape[0])
        inner = (dot_nt(low, contract) * slope_ref[:, span].astype(F32)).astype(BF)
        inner_ref[:, span] = inner
        sum_ref[0:1, span] += jnp.sum(inner.astype(F32), axis=0, keepdims=True)
        total = total + dot_nn(inner, expand)
        at += contract.shape[0]
    out_ref[...] = total


def inner_back(low, slope, grad, contracts, expands):
    count, width = low.shape
    hidden = slope.shape[1]
    return call(
        functools.partial(inner_kernel, count=len(contracts)),
        "inner_back",
        4 * count * width * hidden,
        count * hidden * 4 + count * width * 10,
        grid=(count // TILE,),
        in_specs=[tiles(width), tiles(hidden), tiles(width)]
        + [picked(piece, width) for piece in contracts + expands],
        out_specs=[tiles(hidden), tiles(width), resident((8, hidden))],
        out_shape=[
            jax.ShapeDtypeStruct((count, hidden), BF),
            jax.ShapeDtypeStruct((count, width), F32),
            jax.ShapeDtypeStruct((8, hidden), F32),
        ],
    )(low, slope, grad, *[piece[0] for piece in contracts + expands])


def feed_weights_kernel(left_ref, right_ref, out_ref):
    out_ref[...] = dot_tn(left_ref[...], right_ref[...]).astype(BF)


def feed_weights(left, right, half):
    count, width = right.shape
    rows = left.shape[1] // 2
    size = rows // 2
    return call(
        feed_weights_kernel,
        "feed_weights",
        2 * count * width * rows,
        count * rows * 2 + rows * width * 2,
        grid=(2,),
        in_specs=[pl.BlockSpec((count, size), lambda i: (0, half * 2 + i)), resident((count, width))],
        out_specs=pl.BlockSpec((size, width), lambda i: (i, 0)),
        out_shape=jax.ShapeDtypeStruct((rows, width), BF),
    )(left, right)


def middle_back_kernel(vec_ref, hid_ref, n_ref, s_ref, weight_ref, grad_ref, low_ref, ctx_ref, sum_ref):
    upstream, normed = hid_ref[...], n_ref[...]
    grad = norm_back(upstream, normed, s_ref[:, 0:1], vec_ref[1:2, :])
    low = grad.astype(BF)
    grad_ref[...] = grad
    low_ref[...] = low
    ctx_ref[...] = dot_nn(low, weight_ref[...]).astype(BF)
    add_rows(sum_ref, [low.astype(F32), upstream * normed, upstream])


def middle_back(vectors, hidden_grad, normed, inverse, attn_rows):
    count, width = hidden_grad.shape
    return call(
        middle_back_kernel,
        "middle_back",
        2 * count * width * width,
        count * width * 16,
        grid=(count // TILE,),
        in_specs=[resident(vectors.shape), tiles(width), tiles(width), tiles(128), resident((width, width), 3, 0)],
        out_specs=[tiles(width), tiles(width), tiles(width), resident((8, width))],
        out_shape=[
            jax.ShapeDtypeStruct((count, width), F32),
            jax.ShapeDtypeStruct((count, width), BF),
            jax.ShapeDtypeStruct((count, width), BF),
            jax.ShapeDtypeStruct((8, width), F32),
        ],
    )(vectors, hidden_grad, normed, inverse, attn_rows)


def attn_weights_kernel(table_ref, qkv_ref, low_ref, token_ref, ctx_ref, far_ref, near_ref, sum_ref):
    step = pl.program_id(0)

    @pl.when(step % 4 < 3)
    def _():
        sum_ref[...] = dot_tn(qkv_ref[0], token_ref[...]).astype(BF)

    @pl.when(step % 4 == 3)
    def _():
        sum_ref[...] = dot_tn(low_ref[...], ctx_ref[...]).astype(BF)

    def put(out_ref):
        size = out_ref.shape[2]
        for d in range(4):
            out_ref[d ^ table_ref[1], 0] = sum_ref[d * size : (d + 1) * size, :]

    pl.when(step < 4)(lambda: put(far_ref))
    pl.when(step >= 4)(lambda: put(near_ref))


def attn_weights(table, qkv_grad, out_grad, tokens, context):
    count, width = tokens.shape
    half = width // 2
    block = (4, 1, half // 4, width)

    def column(i, t):
        return jnp.where(i < 4, 1 - t[0], t[0])

    return call(
        attn_weights_kernel,
        "attn_weights",
        8 * 2 * count * width * half,
        count * width * 8 + width * width * 8,
        grid_spec=pltpu.PrefetchScalarGridSpec(
            num_scalar_prefetch=1,
            grid=(8,),
            in_specs=[
                pl.BlockSpec((1, count, half), lambda i, t: (jnp.minimum(i % 4, 2), 0, column(i, t))),
                pl.BlockSpec((count, half), lambda i, t: (0, column(i, t))),
                resident((count, width)),
                resident((count, width)),
            ],
            out_specs=[
                pl.BlockSpec(block, lambda i, t: (0, jnp.minimum(i, 3) ^ t[2], 0, 0)),
                pl.BlockSpec(block, lambda i, t: (0, jnp.maximum(i - 4, 0) ^ t[2], 0, 0)),
            ],
            scratch_shapes=[pltpu.VMEM((half, width), BF)],
        ),
        out_shape=[jax.ShapeDtypeStruct((4, 4, half // 4, width), BF)] * 2,
    )(table, qkv_grad, out_grad, tokens, context)


def input_kernel(qkv_ref, weight_ref, grad_ref, out_ref):
    width = out_ref.shape[1]
    total = grad_ref[...]
    for j in range(3):
        total = total + dot_nn(qkv_ref[j], weight_ref[j * width : (j + 1) * width, :])
    out_ref[...] = total.astype(BF)


def input_back(qkv_grad, attn_rows, grad):
    count, width = grad.shape
    return call(
        input_kernel,
        "input_back",
        6 * count * width * width,
        count * width * 12 + width * width * 6,
        grid=(count // TILE,),
        in_specs=[
            pl.BlockSpec((3, TILE, width), lambda t: (0, t, 0)),
            resident((3 * width, width)),
            tiles(width),
        ],
        out_specs=tiles(width),
        out_shape=jax.ShapeDtypeStruct((count, width), BF),
    )(qkv_grad, attn_rows, grad)


def pack_kernel(place_ref, length_ref, qkv_ref, one_ref, inner_ref, two_ref, middle_ref, out_ref):
    width = qkv_ref.shape[2]
    both = jnp.sum(qkv_ref[...], axis=0)
    rows = [both[0:1, :], both[1:2, :]] + [one_ref[i : i + 1, :] for i in range(3)]
    rows += [two_ref[i : i + 1, :] for i in (1, 2, 3)]
    at = 0
    for row in rows:
        for lane in range(0, width, 128):
            out_ref[at : at + 1, :] = row[:, lane : lane + 128]
            at += 1
    size = inner_ref.shape[1] // 32
    gap = jnp.zeros((1, 128 - size), F32)
    for i in range(32):
        part = jnp.concatenate([inner_ref[0:1, i * size : (i + 1) * size], gap], axis=1)
        out_ref[pl.ds(at + place_ref[i], 1), :] = part
    at += 32
    for row in (middle_ref[0:1, :], middle_ref[1:2, :], two_ref[0:1, :]):
        out_ref[at : at + 1, :] = sum(row[:, lane : lane + 128] for lane in range(0, width, 128))
        at += 1
    live = length_ref[0]
    for i in range(1, length_ref.shape[0]):
        live = live + length_ref[i]
    out_ref[at : at + 1, :] = jnp.full((1, 128), live).astype(F32)
    out_ref[at + 1 :, :] = jnp.zeros((out_ref.shape[0] - at - 1, 128), F32)


def pack(places, lengths, parts):
    width = parts[1].shape[1]
    rows = 8 * width // 128 + 32 + 8
    return call(
        pack_kernel,
        "pack",
        0,
        rows * 1024,
        in_specs=[SMEM, SMEM] + [resident(part.shape) for part in parts],
        out_specs=resident((rows, 128)),
        out_shape=jax.ShapeDtypeStruct((rows, 128), F32),
        grid=(1,),
    )(places, lengths, *parts)


def tie(*values):
    return lax.optimization_barrier(values)


def add(*parts):
    return sum(part.astype(F32) for part in parts)


class Links:
    def __init__(self):
        self.dp, self.fsdp = lax.axis_size("dp"), lax.axis_size("fsdp")
        self.paired = (self.dp, self.fsdp) == (4, 8)
        my_dp, my_fsdp = lax.axis_index("dp"), lax.axis_index("fsdp")
        if self.paired:
            self.my_dp, self.my_core, self.my_z = my_dp, my_fsdp & 1, my_fsdp >> 1
        else:
            zero = jnp.zeros((), jnp.int32)
            self.my_dp, self.my_core, self.my_z = zero, zero, zero
        self.my_fsdp = my_fsdp

    def swap(self, values, core=0, dp=0, z=0):
        mask = core + 2 * z + self.fsdp * dp
        pairs = [(i, i ^ mask) for i in range(self.dp * self.fsdp)]
        return lax.ppermute(values, AXES, pairs)

    def table(self):
        e = jnp.arange(2, dtype=jnp.int32)[:, None, None]
        m = jnp.arange(4, dtype=jnp.int32)[None, :, None]
        k = jnp.arange(4, dtype=jnp.int32)[None, None, :]
        if not self.paired:
            return jnp.arange(32, dtype=jnp.int32)
        e, m, k = e ^ self.my_core, m ^ self.my_dp, k ^ self.my_z
        return ((k * 2 + e) * 4 + m).reshape(-1).astype(jnp.int32)

    def flip(self, values, axis, index):
        shape = values.shape
        bits = shape[axis].bit_length() - 1
        split = values.reshape(shape[:axis] + (2,) * bits + shape[axis + 1 :])
        for i in range(bits):
            bit = (index >> (bits - 1 - i)) & 1
            split = jnp.where(bit == 1, jnp.flip(split, axis + i), split)
        return split.reshape(shape)

    def to_exchange(self, natural):
        if not self.paired:
            return natural
        moved = natural.transpose(1, 2, 0, 3)
        return self.flip(self.flip(self.flip(moved, 0, self.my_core), 1, self.my_dp), 2, self.my_z)

    def to_natural(self, exchanged):
        if not self.paired:
            return exchanged
        moved = self.flip(self.flip(self.flip(exchanged, 0, self.my_core), 1, self.my_dp), 2, self.my_z)
        return moved.transpose(2, 0, 1, 3)


def spread_z(links, mine):
    return [mine] + [links.swap(mine, z=k) for k in range(1, 4)]


def spread_plane(links, own):
    one, two = links.swap(own, dp=1), links.swap(own, dp=2)
    return one, two


def spread_corner(links, one, two):
    half = one.shape[0] // 2
    return links.swap(one[:half], dp=2), links.swap(two[half:], dp=1)


def gather_plain(attention, attvector, expand, contract, feedvector):
    def whole(shard):
        return lax.all_gather(shard, "fsdp", axis=0, tiled=True)

    rows = [whole(attention.T), whole(expand.T), whole(contract)]
    return rows, whole(attvector).astype(F32), whole(feedvector).astype(F32)


def corner_sum(near, got):
    half = near.shape[0] // 8
    parts = (slice(6 * half, 7 * half), slice(7 * half, 8 * half))
    return [add(near[part], got[part]).astype(BF) for part in parts]


def send_corner(links, corner):
    return links.swap(corner[0], dp=2), links.swap(corner[1], dp=1)


def side_sums(near, got, corners):
    block = near.shape[0] // 4
    half = block // 2
    one = add(near[block : 2 * block], got[block : 2 * block])
    two = add(near[2 * block : 3 * block], got[2 * block : 3 * block])
    one = jnp.concatenate([one[:half] + corners[0].astype(F32), one[half:]], axis=0)
    two = jnp.concatenate([two[:half], two[half:] + corners[1].astype(F32)], axis=0)
    return one.astype(BF), two.astype(BF)


def send_sides(links, sides):
    return links.swap(sides[0], dp=1), links.swap(sides[1], dp=2)


def own_sum(near, got, sides):
    block = near.shape[0] // 4
    return add(near[:block], got[:block], *sides).astype(BF)


def send_z_far(links, summed):
    half = summed.shape[0] // 2
    return summed[:half], links.swap(summed[half:], z=2)


def send_z(links, summed):
    size = summed.shape[0] // 4
    return summed[:size], [links.swap(summed[k * size : (k + 1) * size], z=k) for k in range(1, 4)]


def send_share(links, final):
    return [final] + [links.swap(final, dp=m) for m in range(1, 4)]


def quarters(links, shares):
    return links.flip(jnp.stack(shares), 0, links.my_dp).reshape(-1, shares[0].shape[1]).astype(F32)


def per_device(tokens, attention, attvector, expand, contract, feedvector, lengths, cotangent):
    links = Links()
    width = tokens.shape[1]
    positions = tokens.shape[0] // lengths.shape[0]
    hidden = expand.shape[1] * links.fsdp
    att_len, feed_len = attvector.shape[0], feedvector.shape[0]
    size = width // 8
    quad = 4 * size

    if links.paired:
        vectors = jnp.concatenate([attvector, feedvector])
        extra = jnp.pad(vectors, (0, 8 * width - vectors.shape[0])).reshape(8, width)

        def quarter(shard):
            return lax.dynamic_slice_in_dim(shard, links.my_dp * size, size, 0)

        attn_z = spread_z(links, jnp.concatenate([quarter(attention.T), extra], axis=0))
        feed_mine = jnp.concatenate([quarter(expand.T), quarter(contract)], axis=0)
        feed_mine, *attn_z = tie(feed_mine, *attn_z)
        attn_own = jnp.concatenate([part[:size] for part in attn_z], axis=0)
        extras = jnp.concatenate([part[size:] for part in attn_z], axis=0)
        attn_one, attn_two = spread_plane(links, attn_own)
        attn_far, extras_far = links.swap(attn_own, core=1), links.swap(extras, core=1)
        feed_mine, attn_far, extras_far = tie(feed_mine, attn_far, extras_far)
        feed_z = spread_z(links, feed_mine)
        extras = jnp.stack([extras, extras_far])
        extras = extras.reshape(2, 1, 4, 8 * width)[..., : vectors.shape[0]]
        extras = links.flip(links.flip(extras, 0, links.my_core), 2, links.my_z)
        by_owner = extras.transpose(2, 0, 1, 3).reshape(links.fsdp, -1).astype(F32)
        attvec, feedvec = by_owner[:, :att_len].reshape(-1), by_owner[:, att_len:].reshape(-1)
    else:
        rows, attvec, feedvec = gather_plain(attention, attvector, expand, contract, feedvector)
        attn_pieces, attn_starts = [rows[0]], [0]
        expands = [(rows[1], i * quad, quad) for i in range(8)]
        contracts = [(rows[2], i * quad, quad) for i in range(8)]

    def row_of(vector, i, start=0):
        return vector[start + i * width : start + (i + 1) * width]

    project_bias = jnp.stack([row_of(attvec, 0), row_of(attvec, 1)])
    vec_rows = [row_of(attvec, i) for i in (2, 3, 4)] + [row_of(feedvec, i, hidden) for i in range(3)]
    vec_rows = jnp.stack(vec_rows + [jnp.zeros((width,), F32)] * 2)
    inner_bias = links.to_exchange(feedvec[:hidden].reshape(4, 2, 4, size)).reshape(1, hidden)

    if links.paired:
        attn_one, attn_two, project_bias, vec_rows, inner_bias = tie(
            attn_one, attn_two, project_bias, vec_rows, inner_bias
        )
        *feed_z, _ = tie(*feed_z, attn_one)
        attn_three = spread_corner(links, attn_one, attn_two)
        attn_near = [attn_own, attn_one, attn_two, *attn_three]
        attn_far = [attn_far] + [links.swap(part, core=1) for part in attn_near[1:]]
        attn_pieces = attn_near + attn_far
        attn_starts = [0, 4, 8, 12, 14, 16, 20, 24, 28, 30]
        feed_own = jnp.concatenate([part[:size] for part in feed_z] + [part[size:] for part in feed_z], axis=0)
        feed_own, *_ = tie(feed_own, *attn_three)
        feed_one, feed_two = spread_plane(links, feed_own)
        feed_far = [links.swap(feed_own, core=1)]

    places = links.table()
    projected, attn_rows = project(tokens, project_bias, places, attn_pieces, attn_starts, size)
    context, logs = attend(projected, lengths, positions)
    if links.paired:
        context, feed_one, feed_two = tie(context, feed_one, feed_two)
        feed_three = spread_corner(links, feed_one, feed_two)
        feed_far += [links.swap(feed_one, core=1), links.swap(feed_two, core=1)]
    normed_one, inverse_one, hidden_low, sum_middle = middle(
        lengths, vec_rows, context, attn_rows, tokens, positions
    )
    if links.paired:
        feed_near = [feed_own, feed_one, feed_two]
        expands = [(part, 0, quad) for part in feed_near + feed_far]
        gelu, slope = expand_call(hidden_low, inner_bias, expands, [(0, 3, 0), (3, 6, 4 * quad)])
        gelu, *feed_three = tie(gelu, *feed_three)
        far_three = [links.swap(part, core=1) for part in feed_three]
        last = [(feed_three[0], 0, quad), (far_three[0], 0, quad)]
        gelu, slope = expand_last(hidden_low, inner_bias, last, gelu, slope)
        expands = expands[:3] + last[:1] + expands[3:] + last[1:]
        contracts = [(part, quad, quad) for part in feed_near] + [(feed_three[1], 0, quad)]
        contracts += [(part, quad, quad) for part in feed_far] + [(far_three[1], 0, quad)]
    else:
        groups = [(i, i + 2, i * quad) for i in range(0, 8, 2)]
        gelu, slope = expand_call(hidden_low, inner_bias, expands, groups)
    result, grad_two, grad_two_low, sum_two = contract_call(
        lengths, vec_rows, gelu, normed_one, cotangent, contracts, positions
    )
    table = jnp.stack([links.my_core, links.my_dp, links.my_z]).astype(jnp.int32)

    cf = feed_weights(gelu, grad_two_low, 1)
    gelu, cf = tie(gelu, cf)
    cn = feed_weights(gelu, grad_two_low, 0)
    if links.paired:
        cg = links.swap(cf, core=1)
        slope, *corner = tie(slope, *corner_sum(cn, cg))
        c_in = send_corner(links, corner)
    else:
        slope, cn = tie(slope, cn)
    inner_grad, hidden_grad, sum_inner = inner_back(grad_two_low, slope, grad_two, contracts, expands)
    if links.paired:
        inner_grad, cn, cg, *c_in = tie(inner_grad, cn, cg, *c_in)
        inner_grad, *c_in = tie(inner_grad, *side_sums(cn, cg, c_in))
        c_in = send_sides(links, c_in)
    ef = feed_weights(inner_grad, hidden_low, 1)
    inner_grad, ef = tie(inner_grad, ef)
    en = feed_weights(inner_grad, hidden_low, 0)
    if links.paired:
        eg = links.swap(ef, core=1)
        hidden_grad, *corner = tie(hidden_grad, *corner_sum(en, eg))
        e_in = send_corner(links, corner)
    else:
        hidden_grad, en = tie(hidden_grad, en)
    grad_one, grad_one_low, context_grad, sum_one = middle_back(
        vec_rows, hidden_grad, normed_one, inverse_one, attn_rows
    )
    if links.paired:
        context_grad, cn, cg, en, eg, *got = tie(context_grad, cn, cg, en, eg, *e_in, *c_in)
        context_grad, c_own, *e_in = tie(
            context_grad, own_sum(cn, cg, got[2:]), *side_sums(en, eg, got[:2])
        )
        e_in = send_sides(links, e_in)
        c_own, c_in = send_z(links, c_own)
    qkv_grad, sum_qkv = attend_back(projected, lengths, context_grad, context, logs, positions)
    packed = pack(places, lengths, [sum_qkv, sum_one, sum_inner, sum_two, sum_middle])
    if links.paired:
        qkv_grad, c_own, packed, *got = tie(qkv_grad, c_own, packed, *e_in, *c_in)
        c_own = add(c_own, *got[2:]).astype(BF)
        qkv_grad, e_own, c_own = tie(qkv_grad, own_sum(en, eg, got[:2]), c_own)
        c_in, packed_in = send_share(links, c_own), links.swap(packed, core=1)
        e_own, e_in = send_z_far(links, e_own)
    af, an = attn_weights(table, qkv_grad, grad_one_low, tokens, context)
    if links.paired:
        an, af = an.reshape(-1, width), af.reshape(-1, width)
        an, af, packed_in, e_own, e_in, *c_in = tie(an, af, packed_in, e_own, e_in, *c_in)
        ag = links.swap(af, core=1)
        packed = packed + packed_in
        packed_in = links.swap(packed, dp=1)
        e_own = add(e_own, e_in)
        e_in = e_own[size:].astype(BF)
        qkv_grad, packed, packed_in, e_in, *got = tie(
            qkv_grad, packed, packed_in, e_in, *corner_sum(an, ag), *c_in
        )
        corner, c_in = got[:2], got[2:]
        packed = packed + packed_in
        a_in = send_corner(links, corner)
        packed_in, e_in = links.swap(packed, dp=2), links.swap(e_in, z=1)
        an, ag, packed, packed_in, e_in, *a_in = tie(an, ag, packed, packed_in, e_in, *a_in)
        e_own = add(e_own[:size], e_in).astype(BF)
        qkv_grad, packed, e_own, *a_in = tie(qkv_grad, packed + packed_in, e_own, *side_sums(an, ag, a_in))
        a_in, packed_in = send_sides(links, a_in), links.swap(packed, z=1)
        e_in = links.swap(e_own, dp=1)
        input_grad = input_back(qkv_grad, attn_rows, grad_one)
        input_grad, packed_in, e_in, *a_in = tie(input_grad, packed_in, e_in, *a_in)
        e_near = jnp.concatenate([e_own, e_in], axis=0)
        packed, a_own, e_near = tie(packed + packed_in, own_sum(an, ag, a_in), e_near)
        a_own, a_in = send_z(links, a_own)
        packed_in, e_far = links.swap(packed, z=2), links.swap(e_near, dp=2)
        packed, packed_in, e_far, *a_in = tie(packed, packed_in, e_far, *a_in)
        a_own, packed, e_far = tie(add(a_own, *a_in).astype(BF), packed + packed_in, e_far)
        a_in = send_share(links, a_own)
        attn_sum = quarters(links, a_in).T
        expand_sum, contract_sum = quarters(links, [e_near[:size], e_near[size:], e_far[:size], e_far[size:]]).T, quarters(links, c_in)
    else:
        input_grad = input_back(qkv_grad, attn_rows, grad_one)

        def finish(natural):
            shard = lax.psum_scatter(natural, "fsdp", scatter_dimension=0, tiled=True)
            return lax.psum(shard, "dp").astype(F32)

        expand_sum = finish(jnp.concatenate([en, ef], axis=0)).T
        contract_sum = finish(jnp.concatenate([cn, cf], axis=0))
        attn_sum = finish(jnp.stack([an, af]).transpose(2, 0, 1, 3, 4).reshape(4 * width, width)).T
        packed = lax.psum(packed, AXES)

    att_rows = att_len * links.fsdp // 128
    inner_at = att_rows + (feed_len * links.fsdp - hidden) // 128
    att_sum = lax.dynamic_slice_in_dim(packed[:att_rows].reshape(-1), links.my_fsdp * att_len, att_len, 0)
    feed_flat = jnp.concatenate(
        [packed[inner_at : inner_at + 32, : hidden // 32].reshape(-1), packed[att_rows:inner_at].reshape(-1)]
    )
    feed_vec_sum = lax.dynamic_slice_in_dim(feed_flat, links.my_fsdp * feed_len, feed_len, 0)
    squares = jnp.sum(packed[inner_at + 32 : inner_at + 35], axis=1)
    root_squares = jnp.sqrt(squares / (packed[inner_at + 35, 0] * width))
    return (result, input_grad, attn_sum, att_sum, expand_sum, contract_sum, feed_vec_sum, root_squares)


def solution(mesh):
    return jax.shard_map(
        per_device,
        mesh=mesh,
        in_specs=(
            P(AXES, None),
            P(None, "fsdp"),
            P("fsdp"),
            P(None, "fsdp"),
            P("fsdp", None),
            P("fsdp"),
            P(AXES),
            P(AXES, None),
        ),
        out_specs=(
            P(AXES, None),
            P(AXES, None),
            P(None, "fsdp"),
            P("fsdp"),
            P(None, "fsdp"),
            P("fsdp", None),
            P("fsdp"),
            P(),
        ),
        check_vma=False,
    )
```

```python
import functools
import math

import jax
import jax.numpy as jnp
from jax import lax
from jax.experimental import pallas as pl
from jax.experimental.pallas import tpu as pltpu
from jax.sharding import PartitionSpec as P

HEAD_DIM = 64
EPSILON = 1e-12
NEGATIVE = -1000000000.0
BF = jnp.bfloat16
F32 = jnp.float32
AXES = ("dp", "fsdp")
LOG2E = 1.0 / math.log(2.0)
SCALE = 1.0 / math.sqrt(HEAD_DIM)
TILE = 256
PAIR = 2 * HEAD_DIM


def dot_nt(left, right, precision=None):
    return lax.dot_general(
        left, right, (((1,), (1,)), ((), ())), precision=precision, preferred_element_type=F32
    )


def dot_nn(left, right):
    return jnp.dot(left, right, preferred_element_type=F32)


def dot_tn(left, right):
    return lax.dot_general(left, right, (((0,), (0,)), ((), ())), preferred_element_type=F32)


def resident(shape, *index):
    index = index or (0,) * len(shape)
    return pl.BlockSpec(shape, lambda *_: index)


def call(kernel, name, flops, bytes_moved, **kwargs):
    cost = pl.CostEstimate(flops=flops, bytes_accessed=bytes_moved, transcendentals=0)
    return pl.pallas_call(kernel, name=name, cost_estimate=cost, **kwargs)


SMEM = pl.BlockSpec(memory_space=pltpu.SMEM)


def project_kernel(table_ref, bias_ref, token_ref, *refs, starts, size):
    pieces, (out_ref, rows_ref) = refs[:-2], refs[-2:]

    @pl.when(pl.program_id(0) == 0)
    def _():
        for piece, start in zip(pieces, starts):
            for i in range(piece.shape[0] // size):
                there = pl.multiple_of(table_ref[start + i] * size, size)
                rows_ref[pl.ds(there, size), :] = piece[i * size : (i + 1) * size, :]

    width = token_ref.shape[1]
    for j in range(3):
        part = dot_nt(token_ref[...], rows_ref[j * width : (j + 1) * width, :])
        if j == 0:
            part = part + bias_ref[0:1, :]
        if j == 2:
            part = part + bias_ref[1:2, :]
        out_ref[j] = part.astype(BF)


def project(tokens, bias, table, pieces, starts, size):
    count, width = tokens.shape
    total = sum(piece.shape[0] for piece in pieces)
    return call(
        functools.partial(project_kernel, starts=starts, size=size),
        "project",
        2 * count * width * 3 * width,
        2 * (4 * count * width + 2 * total * width),
        grid=(count // TILE,),
        in_specs=[SMEM, resident(bias.shape), pl.BlockSpec((TILE, width), lambda t: (t, 0))]
        + [resident(piece.shape) for piece in pieces],
        out_specs=[
            pl.BlockSpec((3, TILE, width), lambda t: (0, t, 0)),
            resident((total, width)),
        ],
        out_shape=[
            jax.ShapeDtypeStruct((3, count, width), BF),
            jax.ShapeDtypeStruct((total, width), BF),
        ],
    )(table, bias, tokens, *pieces)


def head_lanes(values, head):
    lane = lax.broadcasted_iota(jnp.int32, values.shape, 1)
    return jnp.where((lane >= HEAD_DIM) == (head == 1), values, jnp.zeros_like(values))


def scores_of(keys, queries, length, head):
    live = lax.broadcasted_iota(jnp.int32, (keys.shape[0], 1), 0) < length
    factor = jnp.where(live, SCALE * LOG2E, 0.0)
    shift = jnp.where(live, 0.0, NEGATIVE * LOG2E)
    return dot_nt(keys, head_lanes(queries, head)) * factor + shift


def pairs_per_step(pairs):
    return 2 if pairs % 2 == 0 else 1


def attend_kernel(length_ref, q_ref, k_ref, v_ref, out_ref, log_ref):
    length = length_ref[pl.program_id(0)]
    for i in range(log_ref.shape[1]):
        span = slice(i * PAIR, (i + 1) * PAIR)
        keys, values_t = k_ref[0, :, span], v_ref[0, :, span].T
        halves = []
        for head in range(2):
            scores = scores_of(keys, q_ref[0, :, span], length, head)
            peak = jnp.max(scores, axis=0, keepdims=True)
            weights = jnp.exp2(scores - peak)
            total = jnp.sum(weights, axis=0, keepdims=True)
            part = dot_nn(values_t[head * HEAD_DIM : (head + 1) * HEAD_DIM, :], weights.astype(BF))
            halves.append(part * (1.0 / total))
            log_ref[0, i, head : head + 1, :] = peak + jnp.log2(total)
        out_ref[:, span] = jnp.concatenate(halves, axis=0).T.astype(BF)


def attend(projected, lengths, positions):
    _, count, width = projected.shape
    rows, pairs = count // positions, width // PAIR
    group = pairs_per_step(pairs)
    block = (1, positions, group * PAIR)
    flops = 4 * rows * pairs * 2 * positions * positions * HEAD_DIM
    return call(
        attend_kernel,
        "attend",
        2 * flops,
        8 * count * width,
        grid_spec=pltpu.PrefetchScalarGridSpec(
            num_scalar_prefetch=1,
            grid=(rows, pairs // group),
            in_specs=[pl.BlockSpec(block, lambda r, p, _, j=j: (j, r, p)) for j in range(3)],
            out_specs=[
                pl.BlockSpec((positions, group * PAIR), lambda r, p, _: (r, p)),
                pl.BlockSpec((1, group, 2, positions), lambda r, p, _: (r, p, 0, 0)),
            ],
        ),
        out_shape=[
            jax.ShapeDtypeStruct((count, width), BF),
            jax.ShapeDtypeStruct((rows, pairs, 2, positions), F32),
        ],
    )(lengths, projected, projected, projected)


def attend_back_kernel(
    length_ref, q_ref, k_ref, v_ref, grad_ref, ctx_ref, log_ref, out_ref, sum_ref
):
    length = length_ref[pl.program_id(0)]
    row = lax.broadcasted_iota(jnp.int32, (8, PAIR), 0)
    lane = lax.broadcasted_iota(jnp.int32, (8, PAIR), 1)
    chosen = jnp.where((lane >= HEAD_DIM) == (row == 1), 1.0, 0.0).astype(BF)
    for i in range(log_ref.shape[1]):
        span = slice(i * PAIR, (i + 1) * PAIR)
        queries, keys, values, grad = q_ref[0, :, span], k_ref[0, :, span], v_ref[0, :, span], grad_ref[:, span]
        product = grad.astype(F32) * ctx_ref[:, span].astype(F32)
        high = product.astype(BF)
        low = (product - high.astype(F32)).astype(BF)
        row_totals = dot_nt(chosen, high) + dot_nt(chosen, low)
        query_grad, key_grad, value_grad = 0.0, 0.0, 0.0
        for head in range(2):
            scores = scores_of(keys, queries, length, head)
            wide = jnp.exp2(scores - log_ref[0, i, head : head + 1, :])
            grad_head = head_lanes(grad, head)
            value_grad += dot_nn(wide.astype(BF), grad_head)
            weight_grad = dot_nt(values, grad_head)
            score_grad = (wide * (weight_grad - row_totals[head : head + 1, :])).astype(BF)
            key_grad += dot_nn(score_grad, head_lanes(queries, head))
            query_grad += dot_tn(score_grad, head_lanes(keys, head))
        query_low = (query_grad * SCALE).astype(BF)
        value_low = value_grad.astype(BF)
        out_ref[0, :, span] = query_low
        out_ref[1, :, span] = (key_grad * SCALE).astype(BF)
        out_ref[2, :, span] = value_low
        sum_ref[0, 0:1, span] = jnp.sum(query_low.astype(F32), axis=0, keepdims=True)
        sum_ref[0, 1:2, span] = jnp.sum(value_low.astype(F32), axis=0, keepdims=True)


def attend_back(projected, lengths, context_grad, context, logs, positions):
    _, count, width = projected.shape
    rows, pairs = count // positions, width // PAIR
    group = pairs_per_step(pairs)
    block = (1, positions, group * PAIR)
    flat = pl.BlockSpec((positions, group * PAIR), lambda r, p, _: (r, p))
    flops = 10 * rows * pairs * 2 * positions * positions * HEAD_DIM
    return call(
        attend_back_kernel,
        "attend_back",
        2 * flops,
        16 * count * width,
        grid_spec=pltpu.PrefetchScalarGridSpec(
            num_scalar_prefetch=1,
            grid=(rows, pairs // group),
            in_specs=[pl.BlockSpec(block, lambda r, p, _, j=j: (j, r, p)) for j in range(3)]
            + [flat, flat, pl.BlockSpec((1, group, 2, positions), lambda r, p, _: (r, p, 0, 0))],
            out_specs=[
                pl.BlockSpec((3, positions, group * PAIR), lambda r, p, _: (0, r, p)),
                pl.BlockSpec((1, 2, group * PAIR), lambda r, p, _: (r, 0, p)),
            ],
        ),
        out_shape=[
            jax.ShapeDtypeStruct((3, count, width), BF),
            jax.ShapeDtypeStruct((rows, 2, width), F32),
        ],
    )(lengths, projected, projected, projected, context_grad, context, logs)


def normalize(residual):
    centered = residual - jnp.mean(residual, axis=-1, keepdims=True)
    inverse = lax.rsqrt(jnp.mean(centered * centered, axis=-1, keepdims=True) + EPSILON)
    return centered * inverse, inverse


def norm_back(upstream, normed, inverse, gain):
    scaled = upstream * gain
    mean_plain = jnp.mean(scaled, axis=-1, keepdims=True)
    mean_normed = jnp.mean(scaled * normed, axis=-1, keepdims=True)
    return inverse * (scaled - mean_plain - normed * mean_normed)


def live_tile(length_ref, positions, shape):
    first = pl.program_id(0) * TILE
    place = lax.broadcasted_iota(jnp.int32, shape, 0) + first % positions
    return place < length_ref[first // positions]


def add_rows(ref, rows):
    @pl.when(pl.program_id(0) == 0)
    def _():
        ref[...] = jnp.zeros_like(ref)

    for i, row in enumerate(rows):
        ref[i : i + 1, :] += jnp.sum(row, axis=0, keepdims=True)


def middle_kernel(length_ref, vec_ref, ctx_ref, weight_ref, token_ref, n_ref, s_ref, low_ref, sum_ref, *, positions):
    branch = dot_nt(ctx_ref[...], weight_ref[...]) + vec_ref[0:1, :]
    tokens = token_ref[...].astype(F32)
    normed, inverse = normalize(tokens + branch)
    n_ref[...] = normed
    s_ref[...] = jnp.broadcast_to(inverse, s_ref.shape)
    low_ref[...] = (normed * vec_ref[1:2, :] + vec_ref[2:3, :]).astype(BF)
    live = live_tile(length_ref, positions, tokens.shape)
    add_rows(sum_ref, [jnp.where(live, tokens * tokens, 0.0), jnp.where(live, branch * branch, 0.0)])


def tiles(width):
    return pl.BlockSpec((TILE, width), lambda t: (t, 0))


def middle(lengths, vectors, context, attn_rows, tokens, positions):
    count, width = tokens.shape
    return call(
        functools.partial(middle_kernel, positions=positions),
        "middle",
        2 * count * width * width,
        count * width * 12,
        grid=(count // TILE,),
        in_specs=[SMEM, resident(vectors.shape), tiles(width), resident((width, width), 3, 0), tiles(width)],
        out_specs=[tiles(width), tiles(128), tiles(width), resident((8, width))],
        out_shape=[
            jax.ShapeDtypeStruct((count, width), F32),
            jax.ShapeDtypeStruct((count, 128), F32),
            jax.ShapeDtypeStruct((count, width), BF),
            jax.ShapeDtypeStruct((8, width), F32),
        ],
    )(lengths, vectors, context, attn_rows, tokens)


def gelu_parts(inner):
    cumulative = 0.5 * (1.0 + lax.erf(inner * (1.0 / math.sqrt(2.0))))
    density = jnp.exp2(inner * inner * (-0.5 * LOG2E)) * (1.0 / math.sqrt(2.0 * math.pi))
    return inner * cumulative, cumulative + inner * density


def two_by_two(pieces):
    for first, second in zip(pieces[::2], pieces[1::2]):
        yield jnp.concatenate([rows_of(first), rows_of(second)], axis=0)


def expand_kernel(bias_ref, low_ref, *refs, groups):
    pieces, (gelu_ref, slope_ref) = refs[:-2], refs[-2:]
    low = low_ref[...]
    for first, last, at in groups:
        weights = jnp.concatenate([rows_of(piece) for piece in pieces[first:last]], axis=0)
        span = slice(at, at + weights.shape[0])
        gelu, slope = gelu_parts(dot_nt(low, weights) + bias_ref[0:1, span])
        gelu_ref[:, span] = gelu.astype(BF)
        slope_ref[:, span] = slope.astype(BF)


def expand_last_kernel(bias_ref, low_ref, near_ref, far_ref, _, __, gelu_ref, slope_ref):
    weights = jnp.where(pl.program_id(1) == 0, rows_of(near_ref), rows_of(far_ref))
    gelu, slope = gelu_parts(dot_nt(low_ref[...], weights) + bias_ref[...])
    gelu_ref[...] = gelu.astype(BF)
    slope_ref[...] = slope.astype(BF)


def picked(piece, width):
    array, at, rows = piece
    if array.ndim == 3:
        return pl.BlockSpec((4, rows // 4, width), lambda *_: (0, at, 0))
    return pl.BlockSpec((rows, width), lambda *_: (at, 0))


def rows_of(piece):
    return piece[...].reshape(-1, piece.shape[-1])


def expand_call(low, bias, pieces, groups):
    count, width = low.shape
    hidden = bias.shape[1]
    done = sum(piece[2] for piece in pieces)
    return call(
        functools.partial(expand_kernel, groups=groups),
        "expand_gelu",
        2 * count * width * done,
        count * hidden * 4,
        grid=(count // TILE,),
        in_specs=[resident(bias.shape), tiles(width)] + [picked(piece, width) for piece in pieces],
        out_specs=[tiles(hidden), tiles(hidden)],
        out_shape=[jax.ShapeDtypeStruct((count, hidden), BF)] * 2,
    )(bias, low, *[piece[0] for piece in pieces])


def expand_last(low, bias, pieces, gelu, slope):
    count, width = low.shape
    size = pieces[0][2]
    tall = count // 2
    spot = pl.BlockSpec((tall, size), lambda t, e: (t, 4 * e + 3))
    anywhere = pl.BlockSpec(memory_space=pl.ANY)
    return call(
        expand_last_kernel,
        "expand_last",
        4 * count * width * size,
        count * size * 8,
        grid=(2, 2),
        in_specs=[
            pl.BlockSpec((1, size), lambda t, e: (0, 4 * e + 3)),
            pl.BlockSpec((tall, width), lambda t, e: (t, 0)),
        ]
        + [picked(piece, width) for piece in pieces]
        + [anywhere, anywhere],
        out_specs=[spot, spot],
        out_shape=[jax.ShapeDtypeStruct(gelu.shape, BF)] * 2,
        input_output_aliases={4: 0, 5: 1},
    )(bias, low, *[piece[0] for piece in pieces], gelu, slope)


def contract_kernel(length_ref, vec_ref, gelu_ref, n_ref, cot_ref, *refs, positions):
    pieces, (out_ref, grad_ref, low_ref, sum_ref) = refs[:-4], refs[-4:]
    branch, at = vec_ref[3:4, :], 0
    for piece in two_by_two(pieces):
        size = piece.shape[0]
        branch = branch + dot_nn(gelu_ref[:, at : at + size], piece)
        at += size
    first = n_ref[...] * vec_ref[1:2, :] + vec_ref[2:3, :]
    normed, inverse = normalize(first + branch)
    out_ref[...] = (normed * vec_ref[4:5, :] + vec_ref[5:6, :]).astype(BF)
    upstream = cot_ref[...].astype(F32)
    grad = norm_back(upstream, normed, inverse, vec_ref[4:5, :])
    low = grad.astype(BF)
    grad_ref[...] = grad
    low_ref[...] = low
    live = live_tile(length_ref, positions, branch.shape)
    add_rows(
        sum_ref, [jnp.where(live, branch * branch, 0.0), low.astype(F32), upstream * normed, upstream]
    )


def contract_call(lengths, vectors, gelu, normed, cotangent, pieces, positions):
    count, width = cotangent.shape
    hidden = gelu.shape[1]
    return call(
        functools.partial(contract_kernel, positions=positions),
        "contract_norm",
        2 * count * width * hidden,
        count * hidden * 2 + count * width * 14,
        grid=(count // TILE,),
        in_specs=[SMEM, resident(vectors.shape), tiles(hidden), tiles(width), tiles(width)]
        + [picked(piece, width) for piece in pieces],
        out_specs=[tiles(width), tiles(width), tiles(width), resident((8, width))],
        out_shape=[
            jax.ShapeDtypeStruct((count, width), BF),
            jax.ShapeDtypeStruct((count, width), F32),
            jax.ShapeDtypeStruct((count, width), BF),
            jax.ShapeDtypeStruct((8, width), F32),
        ],
    )(lengths, vectors, gelu, normed, cotangent, *[piece[0] for piece in pieces])


def inner_kernel(low_ref, slope_ref, grad_ref, *refs, count):
    contracts, expands, (inner_ref, out_ref, sum_ref) = refs[:count], refs[count : 2 * count], refs[2 * count :]

    @pl.when(pl.program_id(0) == 0)
    def _():
        sum_ref[...] = jnp.zeros_like(sum_ref)

    low, total, at = low_ref[...], grad_ref[...], 0
    for contract, expand in zip(two_by_two(contracts), two_by_two(expands)):
        span = slice(at, at + contract.shape[0])
        inner = (dot_nt(low, contract) * slope_ref[:, span].astype(F32)).astype(BF)
        inner_ref[:, span] = inner
        sum_ref[0:1, span] += jnp.sum(inner.astype(F32), axis=0, keepdims=True)
        total = total + dot_nn(inner, expand)
        at += contract.shape[0]
    out_ref[...] = total


def inner_back(low, slope, grad, contracts, expands):
    count, width = low.shape
    hidden = slope.shape[1]
    return call(
        functools.partial(inner_kernel, count=len(contracts)),
        "inner_back",
        4 * count * width * hidden,
        count * hidden * 4 + count * width * 10,
        grid=(count // TILE,),
        in_specs=[tiles(width), tiles(hidden), tiles(width)]
        + [picked(piece, width) for piece in contracts + expands],
        out_specs=[tiles(hidden), tiles(width), resident((8, hidden))],
        out_shape=[
            jax.ShapeDtypeStruct((count, hidden), BF),
            jax.ShapeDtypeStruct((count, width), F32),
            jax.ShapeDtypeStruct((8, hidden), F32),
        ],
    )(low, slope, grad, *[piece[0] for piece in contracts + expands])


def feed_weights_kernel(left_ref, right_ref, out_ref):
    out_ref[...] = dot_tn(left_ref[...], right_ref[...]).astype(BF)


def feed_weights(left, right, half):
    count, width = right.shape
    rows = left.shape[1] // 2
    size = rows // 2
    return call(
        feed_weights_kernel,
        "feed_weights",
        2 * count * width * rows,
        count * rows * 2 + rows * width * 2,
        grid=(2,),
        in_specs=[pl.BlockSpec((count, size), lambda i: (0, half * 2 + i)), resident((count, width))],
        out_specs=pl.BlockSpec((size, width), lambda i: (i, 0)),
        out_shape=jax.ShapeDtypeStruct((rows, width), BF),
    )(left, right)


def middle_back_kernel(vec_ref, hid_ref, n_ref, s_ref, weight_ref, grad_ref, low_ref, ctx_ref, sum_ref):
    upstream, normed = hid_ref[...], n_ref[...]
    grad = norm_back(upstream, normed, s_ref[:, 0:1], vec_ref[1:2, :])
    low = grad.astype(BF)
    grad_ref[...] = grad
    low_ref[...] = low
    ctx_ref[...] = dot_nn(low, weight_ref[...]).astype(BF)
    add_rows(sum_ref, [low.astype(F32), upstream * normed, upstream])


def middle_back(vectors, hidden_grad, normed, inverse, attn_rows):
    count, width = hidden_grad.shape
    return call(
        middle_back_kernel,
        "middle_back",
        2 * count * width * width,
        count * width * 16,
        grid=(count // TILE,),
        in_specs=[resident(vectors.shape), tiles(width), tiles(width), tiles(128), resident((width, width), 3, 0)],
        out_specs=[tiles(width), tiles(width), tiles(width), resident((8, width))],
        out_shape=[
            jax.ShapeDtypeStruct((count, width), F32),
            jax.ShapeDtypeStruct((count, width), BF),
            jax.ShapeDtypeStruct((count, width), BF),
            jax.ShapeDtypeStruct((8, width), F32),
        ],
    )(vectors, hidden_grad, normed, inverse, attn_rows)


def attn_weights_kernel(table_ref, qkv_ref, low_ref, token_ref, ctx_ref, far_ref, near_ref, sum_ref):
    step = pl.program_id(0)

    @pl.when(step % 4 < 3)
    def _():
        sum_ref[...] = dot_tn(qkv_ref[0], token_ref[...]).astype(BF)

    @pl.when(step % 4 == 3)
    def _():
        sum_ref[...] = dot_tn(low_ref[...], ctx_ref[...]).astype(BF)

    def put(out_ref):
        size = out_ref.shape[2]
        for d in range(4):
            out_ref[d ^ table_ref[1], 0] = sum_ref[d * size : (d + 1) * size, :]

    pl.when(step < 4)(lambda: put(far_ref))
    pl.when(step >= 4)(lambda: put(near_ref))


def attn_weights(table, qkv_grad, out_grad, tokens, context):
    count, width = tokens.shape
    half = width // 2
    block = (4, 1, half // 4, width)

    def column(i, t):
        return jnp.where(i < 4, 1 - t[0], t[0])

    return call(
        attn_weights_kernel,
        "attn_weights",
        8 * 2 * count * width * half,
        count * width * 8 + width * width * 8,
        grid_spec=pltpu.PrefetchScalarGridSpec(
            num_scalar_prefetch=1,
            grid=(8,),
            in_specs=[
                pl.BlockSpec((1, count, half), lambda i, t: (jnp.minimum(i % 4, 2), 0, column(i, t))),
                pl.BlockSpec((count, half), lambda i, t: (0, column(i, t))),
                resident((count, width)),
                resident((count, width)),
            ],
            out_specs=[
                pl.BlockSpec(block, lambda i, t: (0, jnp.minimum(i, 3) ^ t[2], 0, 0)),
                pl.BlockSpec(block, lambda i, t: (0, jnp.maximum(i - 4, 0) ^ t[2], 0, 0)),
            ],
            scratch_shapes=[pltpu.VMEM((half, width), BF)],
        ),
        out_shape=[jax.ShapeDtypeStruct((4, 4, half // 4, width), BF)] * 2,
    )(table, qkv_grad, out_grad, tokens, context)


def input_kernel(qkv_ref, weight_ref, grad_ref, out_ref):
    width = out_ref.shape[1]
    total = grad_ref[...]
    for j in range(3):
        total = total + dot_nn(qkv_ref[j], weight_ref[j * width : (j + 1) * width, :])
    out_ref[...] = total.astype(BF)


def input_back(qkv_grad, attn_rows, grad):
    count, width = grad.shape
    return call(
        input_kernel,
        "input_back",
        6 * count * width * width,
        count * width * 12 + width * width * 6,
        grid=(count // TILE,),
        in_specs=[
            pl.BlockSpec((3, TILE, width), lambda t: (0, t, 0)),
            resident((3 * width, width)),
            tiles(width),
        ],
        out_specs=tiles(width),
        out_shape=jax.ShapeDtypeStruct((count, width), BF),
    )(qkv_grad, attn_rows, grad)


def pack_kernel(place_ref, length_ref, qkv_ref, one_ref, inner_ref, two_ref, middle_ref, out_ref):
    width = qkv_ref.shape[2]
    both = jnp.sum(qkv_ref[...], axis=0)
    rows = [both[0:1, :], both[1:2, :]] + [one_ref[i : i + 1, :] for i in range(3)]
    rows += [two_ref[i : i + 1, :] for i in (1, 2, 3)]
    at = 0
    for row in rows:
        for lane in range(0, width, 128):
            out_ref[at : at + 1, :] = row[:, lane : lane + 128]
            at += 1
    size = inner_ref.shape[1] // 32
    gap = jnp.zeros((1, 128 - size), F32)
    for i in range(32):
        part = jnp.concatenate([inner_ref[0:1, i * size : (i + 1) * size], gap], axis=1)
        out_ref[pl.ds(at + place_ref[i], 1), :] = part
    at += 32
    for row in (middle_ref[0:1, :], middle_ref[1:2, :], two_ref[0:1, :]):
        out_ref[at : at + 1, :] = sum(row[:, lane : lane + 128] for lane in range(0, width, 128))
        at += 1
    live = length_ref[0]
    for i in range(1, length_ref.shape[0]):
        live = live + length_ref[i]
    out_ref[at : at + 1, :] = jnp.full((1, 128), live).astype(F32)
    out_ref[at + 1 :, :] = jnp.zeros((out_ref.shape[0] - at - 1, 128), F32)


def pack(places, lengths, parts):
    width = parts[1].shape[1]
    rows = 8 * width // 128 + 32 + 8
    return call(
        pack_kernel,
        "pack",
        0,
        rows * 1024,
        in_specs=[SMEM, SMEM] + [resident(part.shape) for part in parts],
        out_specs=resident((rows, 128)),
        out_shape=jax.ShapeDtypeStruct((rows, 128), F32),
        grid=(1,),
    )(places, lengths, *parts)


def tie(*values):
    return lax.optimization_barrier(values)


def add(*parts):
    return sum(part.astype(F32) for part in parts)


class Links:
    def __init__(self):
        self.dp, self.fsdp = lax.axis_size("dp"), lax.axis_size("fsdp")
        self.paired = (self.dp, self.fsdp) == (4, 8)
        my_dp, my_fsdp = lax.axis_index("dp"), lax.axis_index("fsdp")
        if self.paired:
            self.my_dp, self.my_core, self.my_z = my_dp, my_fsdp & 1, my_fsdp >> 1
        else:
            zero = jnp.zeros((), jnp.int32)
            self.my_dp, self.my_core, self.my_z = zero, zero, zero
        self.my_fsdp = my_fsdp

    def swap(self, values, core=0, dp=0, z=0):
        mask = core + 2 * z + self.fsdp * dp
        pairs = [(i, i ^ mask) for i in range(self.dp * self.fsdp)]
        return lax.ppermute(values, AXES, pairs)

    def table(self):
        e = jnp.arange(2, dtype=jnp.int32)[:, None, None]
        m = jnp.arange(4, dtype=jnp.int32)[None, :, None]
        k = jnp.arange(4, dtype=jnp.int32)[None, None, :]
        if not self.paired:
            return jnp.arange(32, dtype=jnp.int32)
        e, m, k = e ^ self.my_core, m ^ self.my_dp, k ^ self.my_z
        return ((k * 2 + e) * 4 + m).reshape(-1).astype(jnp.int32)

    def flip(self, values, axis, index):
        shape = values.shape
        bits = shape[axis].bit_length() - 1
        split = values.reshape(shape[:axis] + (2,) * bits + shape[axis + 1 :])
        for i in range(bits):
            bit = (index >> (bits - 1 - i)) & 1
            split = jnp.where(bit == 1, jnp.flip(split, axis + i), split)
        return split.reshape(shape)

    def to_exchange(self, natural):
        if not self.paired:
            return natural
        moved = natural.transpose(1, 2, 0, 3)
        return self.flip(self.flip(self.flip(moved, 0, self.my_core), 1, self.my_dp), 2, self.my_z)

    def to_natural(self, exchanged):
        if not self.paired:
            return exchanged
        moved = self.flip(self.flip(self.flip(exchanged, 0, self.my_core), 1, self.my_dp), 2, self.my_z)
        return moved.transpose(2, 0, 1, 3)


def spread_z(links, mine):
    return [mine] + [links.swap(mine, z=k) for k in range(1, 4)]


def spread_plane(links, own):
    one, two = links.swap(own, dp=1), links.swap(own, dp=2)
    return one, two


def spread_corner(links, one, two):
    half = one.shape[0] // 2
    return links.swap(one[:half], dp=2), links.swap(two[half:], dp=1)


def gather_plain(attention, attvector, expand, contract, feedvector):
    def whole(shard):
        return lax.all_gather(shard, "fsdp", axis=0, tiled=True)

    rows = [whole(attention.T), whole(expand.T), whole(contract)]
    return rows, whole(attvector).astype(F32), whole(feedvector).astype(F32)


def corner_sum(near, got):
    half = near.shape[0] // 8
    parts = (slice(6 * half, 7 * half), slice(7 * half, 8 * half))
    return [add(near[part], got[part]).astype(BF) for part in parts]


def send_corner(links, corner):
    return links.swap(corner[0], dp=2), links.swap(corner[1], dp=1)


def side_sums(near, got, corners):
    block = near.shape[0] // 4
    half = block // 2
    one = add(near[block : 2 * block], got[block : 2 * block])
    two = add(near[2 * block : 3 * block], got[2 * block : 3 * block])
    one = jnp.concatenate([one[:half] + corners[0].astype(F32), one[half:]], axis=0)
    two = jnp.concatenate([two[:half], two[half:] + corners[1].astype(F32)], axis=0)
    return one.astype(BF), two.astype(BF)


def send_sides(links, sides):
    return links.swap(sides[0], dp=1), links.swap(sides[1], dp=2)


def own_sum(near, got, sides):
    block = near.shape[0] // 4
    return add(near[:block], got[:block], *sides).astype(BF)


def send_z_far(links, summed):
    half = summed.shape[0] // 2
    return summed[:half], links.swap(summed[half:], z=2)


def send_z(links, summed):
    size = summed.shape[0] // 4
    return summed[:size], [links.swap(summed[k * size : (k + 1) * size], z=k) for k in range(1, 4)]


def send_share(links, final):
    return [final] + [links.swap(final, dp=m) for m in range(1, 4)]


def quarters(links, shares):
    return links.flip(jnp.stack(shares), 0, links.my_dp).reshape(-1, shares[0].shape[1]).astype(F32)


def per_device(tokens, attention, attvector, expand, contract, feedvector, lengths, cotangent):
    links = Links()
    width = tokens.shape[1]
    positions = tokens.shape[0] // lengths.shape[0]
    hidden = expand.shape[1] * links.fsdp
    att_len, feed_len = attvector.shape[0], feedvector.shape[0]
    size = width // 8
    quad = 4 * size

    if links.paired:
        vectors = jnp.concatenate([attvector, feedvector])
        extra = jnp.pad(vectors, (0, 8 * width - vectors.shape[0])).reshape(8, width)

        def quarter(shard):
            return lax.dynamic_slice_in_dim(shard, links.my_dp * size, size, 0)

        attn_z = spread_z(links, jnp.concatenate([quarter(attention.T), extra], axis=0))
        feed_mine = jnp.concatenate([quarter(expand.T), quarter(contract)], axis=0)
        feed_mine, *attn_z = tie(feed_mine, *attn_z)
        attn_own = jnp.concatenate([part[:size] for part in attn_z], axis=0)
        extras = jnp.concatenate([part[size:] for part in attn_z], axis=0)
        attn_one, attn_two = spread_plane(links, attn_own)
        attn_far, extras_far = links.swap(attn_own, core=1), links.swap(extras, core=1)
        feed_mine, attn_far, extras_far = tie(feed_mine, attn_far, extras_far)
        feed_z = spread_z(links, feed_mine)
        extras = jnp.stack([extras, extras_far])
        extras = extras.reshape(2, 1, 4, 8 * width)[..., : vectors.shape[0]]
        extras = links.flip(links.flip(extras, 0, links.my_core), 2, links.my_z)
        by_owner = extras.transpose(2, 0, 1, 3).reshape(links.fsdp, -1).astype(F32)
        attvec, feedvec = by_owner[:, :att_len].reshape(-1), by_owner[:, att_len:].reshape(-1)
    else:
        rows, attvec, feedvec = gather_plain(attention, attvector, expand, contract, feedvector)
        attn_pieces, attn_starts = [rows[0]], [0]
        expands = [(rows[1], i, quad) for i in range(8)]
        contracts = [(rows[2], i, quad) for i in range(8)]

    def row_of(vector, i, start=0):
        return vector[start + i * width : start + (i + 1) * width]

    project_bias = jnp.stack([row_of(attvec, 0), row_of(attvec, 1)])
    vec_rows = [row_of(attvec, i) for i in (2, 3, 4)] + [row_of(feedvec, i, hidden) for i in range(3)]
    vec_rows = jnp.stack(vec_rows + [jnp.zeros((width,), F32)] * 2)
    inner_bias = links.to_exchange(feedvec[:hidden].reshape(4, 2, 4, size)).reshape(1, hidden)

    if links.paired:
        attn_one, attn_two, project_bias, vec_rows, inner_bias = tie(
            attn_one, attn_two, project_bias, vec_rows, inner_bias
        )
        *feed_z, _ = tie(*feed_z, attn_one)
        attn_three = spread_corner(links, attn_one, attn_two)
        attn_near = [attn_own, attn_one, attn_two, *attn_three]
        attn_far = [attn_far] + [links.swap(part, core=1) for part in attn_near[1:]]
        attn_pieces = attn_near + attn_far
        attn_starts = [0, 4, 8, 12, 14, 16, 20, 24, 28, 30]
        feed_own = jnp.stack(feed_z)
        feed_own, *_ = tie(feed_own, *attn_three)
        feed_one, feed_two = spread_plane(links, feed_own)
        feed_far = [links.swap(feed_own, core=1)]

    places = links.table()
    projected, attn_rows = project(tokens, project_bias, places, attn_pieces, attn_starts, size)
    context, logs = attend(projected, lengths, positions)
    if links.paired:
        context, feed_one, feed_two = tie(context, feed_one, feed_two)
        feed_three = links.swap(feed_one[:, :size], dp=2), links.swap(feed_two[:, size:], dp=1)
        feed_far += [links.swap(feed_one, core=1), links.swap(feed_two, core=1)]
    normed_one, inverse_one, hidden_low, sum_middle = middle(
        lengths, vec_rows, context, attn_rows, tokens, positions
    )
    if links.paired:
        feed_near = [feed_own, feed_one, feed_two]
        expands = [(part, 0, quad) for part in feed_near + feed_far]
        gelu, slope = expand_call(hidden_low, inner_bias, expands, [(0, 3, 0), (3, 6, 4 * quad)])
        gelu, *feed_three = tie(gelu, *feed_three)
        far_three = [links.swap(part, core=1) for part in feed_three]
        last = [(feed_three[0], 0, quad), (far_three[0], 0, quad)]
        gelu, slope = expand_last(hidden_low, inner_bias, last, gelu, slope)
        expands = expands[:3] + last[:1] + expands[3:] + last[1:]
        contracts = [(part, 1, quad) for part in feed_near] + [(feed_three[1], 0, quad)]
        contracts += [(part, 1, quad) for part in feed_far] + [(far_three[1], 0, quad)]
    else:
        groups = [(i, i + 2, i * quad) for i in range(0, 8, 2)]
        gelu, slope = expand_call(hidden_low, inner_bias, expands, groups)
    result, grad_two, grad_two_low, sum_two = contract_call(
        lengths, vec_rows, gelu, normed_one, cotangent, contracts, positions
    )
    table = jnp.stack([links.my_core, links.my_dp, links.my_z]).astype(jnp.int32)

    cf = feed_weights(gelu, grad_two_low, 1)
    gelu, cf = tie(gelu, cf)
    cn = feed_weights(gelu, grad_two_low, 0)
    if links.paired:
        cg = links.swap(cf, core=1)
        slope, *corner = tie(slope, *corner_sum(cn, cg))
        c_in = send_corner(links, corner)
    else:
        slope, cn = tie(slope, cn)
    inner_grad, hidden_grad, sum_inner = inner_back(grad_two_low, slope, grad_two, contracts, expands)
    if links.paired:
        inner_grad, cn, cg, *c_in = tie(inner_grad, cn, cg, *c_in)
        inner_grad, *c_in = tie(inner_grad, *side_sums(cn, cg, c_in))
        c_in = send_sides(links, c_in)
    ef = feed_weights(inner_grad, hidden_low, 1)
    inner_grad, ef = tie(inner_grad, ef)
    en = feed_weights(inner_grad, hidden_low, 0)
    if links.paired:
        eg = links.swap(ef, core=1)
        hidden_grad, *corner = tie(hidden_grad, *corner_sum(en, eg))
        e_in = send_corner(links, corner)
    else:
        hidden_grad, en = tie(hidden_grad, en)
    grad_one, grad_one_low, context_grad, sum_one = middle_back(
        vec_rows, hidden_grad, normed_one, inverse_one, attn_rows
    )
    if links.paired:
        context_grad, cn, cg, en, eg, *got = tie(context_grad, cn, cg, en, eg, *e_in, *c_in)
        context_grad, c_own, *e_in = tie(
            context_grad, own_sum(cn, cg, got[2:]), *side_sums(en, eg, got[:2])
        )
        e_in = send_sides(links, e_in)
        c_own, c_in = send_z(links, c_own)
    qkv_grad, sum_qkv = attend_back(projected, lengths, context_grad, context, logs, positions)
    packed = pack(places, lengths, [sum_qkv, sum_one, sum_inner, sum_two, sum_middle])
    if links.paired:
        qkv_grad, c_own, packed, *got = tie(qkv_grad, c_own, packed, *e_in, *c_in)
        c_own = add(c_own, *got[2:]).astype(BF)
        qkv_grad, e_own, c_own = tie(qkv_grad, own_sum(en, eg, got[:2]), c_own)
        c_in, packed_in = send_share(links, c_own), links.swap(packed, core=1)
        e_own, e_in = send_z_far(links, e_own)
    af, an = attn_weights(table, qkv_grad, grad_one_low, tokens, context)
    if links.paired:
        an, af = an.reshape(-1, width), af.reshape(-1, width)
        an, af, packed_in, e_own, e_in, *c_in = tie(an, af, packed_in, e_own, e_in, *c_in)
        ag = links.swap(af, core=1)
        packed = packed + packed_in
        packed_in = links.swap(packed, dp=1)
        e_own = add(e_own, e_in)
        e_in = e_own[size:].astype(BF)
        qkv_grad, packed, packed_in, e_in, *got = tie(
            qkv_grad, packed, packed_in, e_in, *corner_sum(an, ag), *c_in
        )
        corner, c_in = got[:2], got[2:]
        packed = packed + packed_in
        a_in = send_corner(links, corner)
        packed_in, e_in = links.swap(packed, dp=2), links.swap(e_in, z=1)
        an, ag, packed, packed_in, e_in, *a_in = tie(an, ag, packed, packed_in, e_in, *a_in)
        e_own = add(e_own[:size], e_in).astype(BF)
        qkv_grad, packed, e_own, *a_in = tie(qkv_grad, packed + packed_in, e_own, *side_sums(an, ag, a_in))
        a_in, packed_in = send_sides(links, a_in), links.swap(packed, z=1)
        e_in = links.swap(e_own, dp=1)
        input_grad = input_back(qkv_grad, attn_rows, grad_one)
        input_grad, packed_in, e_in, *a_in = tie(input_grad, packed_in, e_in, *a_in)
        e_near = jnp.concatenate([e_own, e_in], axis=0)
        packed, a_own, e_near = tie(packed + packed_in, own_sum(an, ag, a_in), e_near)
        a_own, a_in = send_z(links, a_own)
        packed_in, e_far = links.swap(packed, z=2), links.swap(e_near, dp=2)
        packed, packed_in, e_far, *a_in = tie(packed, packed_in, e_far, *a_in)
        a_own, packed, e_far = tie(add(a_own, *a_in).astype(BF), packed + packed_in, e_far)
        a_in = send_share(links, a_own)
        attn_sum = quarters(links, a_in).T
        expand_sum, contract_sum = quarters(links, [e_near[:size], e_near[size:], e_far[:size], e_far[size:]]).T, quarters(links, c_in)
    else:
        input_grad = input_back(qkv_grad, attn_rows, grad_one)

        def finish(natural):
            shard = lax.psum_scatter(natural, "fsdp", scatter_dimension=0, tiled=True)
            return lax.psum(shard, "dp").astype(F32)

        expand_sum = finish(jnp.concatenate([en, ef], axis=0)).T
        contract_sum = finish(jnp.concatenate([cn, cf], axis=0))
        attn_sum = finish(jnp.stack([an, af]).transpose(2, 0, 1, 3, 4).reshape(4 * width, width)).T
        packed = lax.psum(packed, AXES)

    att_rows = att_len * links.fsdp // 128
    inner_at = att_rows + (feed_len * links.fsdp - hidden) // 128
    att_sum = lax.dynamic_slice_in_dim(packed[:att_rows].reshape(-1), links.my_fsdp * att_len, att_len, 0)
    feed_flat = jnp.concatenate(
        [packed[inner_at : inner_at + 32, : hidden // 32].reshape(-1), packed[att_rows:inner_at].reshape(-1)]
    )
    feed_vec_sum = lax.dynamic_slice_in_dim(feed_flat, links.my_fsdp * feed_len, feed_len, 0)
    squares = jnp.sum(packed[inner_at + 32 : inner_at + 35], axis=1)
    root_squares = jnp.sqrt(squares / (packed[inner_at + 35, 0] * width))
    return (result, input_grad, attn_sum, att_sum, expand_sum, contract_sum, feed_vec_sum, root_squares)


def solution(mesh):
    return jax.shard_map(
        per_device,
        mesh=mesh,
        in_specs=(
            P(AXES, None),
            P(None, "fsdp"),
            P("fsdp"),
            P(None, "fsdp"),
            P("fsdp", None),
            P("fsdp"),
            P(AXES),
            P(AXES, None),
        ),
        out_specs=(
            P(AXES, None),
            P(AXES, None),
            P(None, "fsdp"),
            P("fsdp"),
            P(None, "fsdp"),
            P("fsdp", None),
            P("fsdp"),
            P(),
        ),
        check_vma=False,
    )
```
